256 devices in a mesh: seq: 8 (over z), head: 16 (over y, x), batch: 2 (over core).
Axes of the slice: x: 4, y: 4, z: 8, core: 2. Of those that a mesh axis runs over, the one named last changes fastest.
Arguments:
- ssm_input: bfloat16 [32768, 5120], P(('batch', 'seq'), 'head'), parts along dimension 0, may hold values from -500 to 500
- gate_input: bfloat16 [32768, 5120], P(('batch', 'seq'), 'head'), parts along dimension 0, may hold values from -6 to 6
- b_proj: bfloat16 [32768, 1024], P(('batch', 'seq')), parts along dimension 0, may hold values from -2 to 2
- c_proj: bfloat16 [32768, 1024], P(('batch', 'seq')), parts along dimension 0, may hold values from -2 to 2
- step_size: float32 [80, 32768], P('head', ('batch', 'seq')), parts along dimension 1, may hold values from 0.02 to 0.2
- log_decay: float32 [80, 32768], P('head', ('batch', 'seq')), parts along dimension 1, may hold values from -1.5 to 0, as said below
- skip_gain: float32 [80], P('head'), may hold values from 0.5 to 1.5
- norm_gain: float32 [5120], replicated, may hold values from 0.1 to 1.9
- out_weight: bfloat16 [5120, 2560], P('head'), may hold values from -0.078125 to 0.078125
Outputs:
- layer_out: bfloat16 [32768, 2560], P(('batch', 'seq', 'head')), parts along dimension 0
The draws below stay inside these ranges and needn't reach their ends.
There are 2 independent parts, one for each index of `batch`. The reference program is written for one: setup_inputs(seed, part) draws one part's arguments, and reference() takes and returns one part's arrays. A program takes and returns all parts, laid end to end along the dimension named above; an argument that names none is the same for every part. Nothing has to cross between parts.
Inputs may be any that keep to these rules, and one draw needn't show every extreme that they name: `log_decay`: negative.
All inputs are finite; a program needn't handle non-finite values.
Results may differ from the reference program's by a relative error of at most 0.018.
Values may be sent and summed in bfloat16 or wider, within the bound.
No kernel may reach another device: no remote copies, remote signals or barrier semaphores. Data moves between devices by JAX's collectives and lax.ppermute only.
A program may use at most 128 MiB of HBM per device.

```python
import math
import jax
import jax.numpy as jnp
from jax import lax

D = 2560
HEAD_COUNT = 80
HEAD_DIM = 64
STATE = 128
GROUPS = 8
BLOCK = 256
SEQUENCE_LENGTH = 16384


def draw_ssm_input(key, part):
    random_keys = jax.random.split(key, 3)
    total_width = HEAD_COUNT * HEAD_DIM
    columns = 10.0 ** (jnp.arange(total_width, dtype=jnp.float32) / total_width)
    row_scale = 10.0 ** jax.random.uniform(random_keys[0], (SEQUENCE_LENGTH, 1), jnp.float32)
    values = jnp.clip(jax.random.normal(random_keys[2], (SEQUENCE_LENGTH, total_width), jnp.float32), -4.0, 4.0)
    return (values * columns[None, :] * row_scale).astype(jnp.bfloat16)


def draw_log_decay(key, part):
    random_keys = jax.random.split(key, 6)
    fast_share = 0.5
    is_fast = jax.random.uniform(random_keys[0], (HEAD_COUNT, 1), jnp.float32) < fast_share
    fast_rate = 10.0 ** jax.random.uniform(random_keys[1], (HEAD_COUNT, 1), jnp.float32, -1.699, -1.347)
    slow_rate = 10.0 ** jax.random.uniform(random_keys[2], (HEAD_COUNT, 1), jnp.float32, -1.0, 0.0) / SEQUENCE_LENGTH
    per_head_decay = jnp.where(is_fast, fast_rate, slow_rate)
    jitter_level = jax.random.uniform(random_keys[3], (HEAD_COUNT, SEQUENCE_LENGTH), jnp.float32, 0.2, 1.6)
    spike_position = jax.random.randint(random_keys[4], (2, 1), 0, SEQUENCE_LENGTH)
    spike_decay = jax.random.uniform(random_keys[5], (HEAD_COUNT, 2), jnp.float32, 0.22, 0.69)
    spike_count = (jnp.arange(SEQUENCE_LENGTH)[None, :] == spike_position).astype(jnp.float32)
    return -per_head_decay * jitter_level - jnp.dot(spike_decay, spike_count)


def shard_levels(key, dims, shards, smallest, high):
    def one(dim, shards_of):
        steps = jax.random.uniform(jax.random.fold_in(jax.random.fold_in(key, 6), dim), (shards_of,), jnp.float32, smallest / len(shards), high / len(shards))
        return jnp.repeat(jnp.exp(steps), dims[dim] // shards_of).reshape((-1,) + (1,) * (len(dims) - dim - 1))

    loudness = one(*shards[0])
    for cut in shards[1:]:
        loudness = loudness * one(*cut)
    return loudness


def gaussian(key, dims, deviation, bound, shards=(), held_as=jnp.bfloat16):
    drawn = jax.random.normal(key, dims, jnp.float32) * deviation
    if len(shards) > 0:
        drawn = shard_levels(key, dims, shards, -0.22, 0.18) * drawn
    return jnp.clip(drawn, min=-bound, max=bound).astype(held_as)


def setup_inputs(seed: int = 0, part: int = 0) -> dict:
    key_list = jax.random.split(jax.random.key(seed), 10)
    part_keys = jax.random.split(jax.random.fold_in(key_list[9], part), 10)
    return {
        "ssm_input": draw_ssm_input(jax.random.fold_in(jax.random.fold_in(key_list[9], part), 71), part),
        "gate_input": gaussian(part_keys[1], (SEQUENCE_LENGTH, HEAD_COUNT * HEAD_DIM), 1.5, 6.0, ((0, 8), (1, 16))),
        "b_proj": gaussian(part_keys[2], (SEQUENCE_LENGTH, GROUPS * STATE), 0.3, 2.0, ((0, 8),)),
        "c_proj": gaussian(part_keys[3], (SEQUENCE_LENGTH, GROUPS * STATE), 0.3, 2.0, ((0, 8),)),
        "step_size": jnp.clip(jnp.exp(math.log(0.2) - 2.3025851 * jax.random.uniform(part_keys[4], (HEAD_COUNT, SEQUENCE_LENGTH), jnp.float32) ** shard_levels(part_keys[4], (HEAD_COUNT, SEQUENCE_LENGTH), ((0, 16), (1, 8)), -0.2, 0.2)), 0.02, 0.2),
        "log_decay": draw_log_decay(jax.random.fold_in(jax.random.fold_in(key_list[9], part), 71), part),
        "skip_gain": jnp.clip(0.5 + 1.0 * jax.random.uniform(key_list[6], (HEAD_COUNT,), jnp.float32) ** shard_levels(key_list[6], (HEAD_COUNT,), ((0, 16),), -0.2, 0.2), 0.5, 1.5),
        "norm_gain": jnp.clip(1.0 + 0.18 * jax.random.normal(key_list[7], (HEAD_COUNT * HEAD_DIM,), jnp.float32), 0.1, 1.9),
        "out_weight": gaussian(key_list[8], (HEAD_COUNT * HEAD_DIM, D), (HEAD_COUNT * HEAD_DIM) ** -0.5, 0.078125, ((0, 16),)),
    }


epsilon = 1e-05

def reference(ssm_input, gate_input, b_proj, c_proj, step_size, log_decay, skip_gain, norm_gain, out_weight):
    nblocks = SEQUENCE_LENGTH // BLOCK
    group_of = jnp.arange(HEAD_COUNT) // (HEAD_COUNT // GROUPS)
    lower_mask = jnp.tril(jnp.ones((BLOCK, BLOCK), dtype=bool))

    def block_step(carried, inputs_now):
        x_block, b_block, c_block, step_block, decay_block = inputs_now
        cumulative = jnp.cumsum(decay_block, axis=1)
        b_heads = b_block.reshape(BLOCK, GROUPS, STATE)[:, group_of, :].astype(jnp.float32)
        c_heads = c_block.reshape(BLOCK, GROUPS, STATE)[:, group_of, :].astype(jnp.float32)
        scores = jnp.einsum('thn,shn->hts', c_heads, b_heads)
        differ = cumulative[:, :, None] - cumulative[:, None, :]
        weights = scores * jnp.exp(jnp.where(lower_mask, differ, -jnp.inf)) * step_block[:, None, :]
        weights = lax.optimization_barrier(weights.astype(jnp.bfloat16)).astype(jnp.float32)
        x_heads = x_block.reshape(BLOCK, HEAD_COUNT, HEAD_DIM).astype(jnp.float32)
        within = jnp.einsum('hts,shp->thp', weights, x_heads)
        entering_b = lax.optimization_barrier(carried.astype(jnp.bfloat16)).astype(jnp.float32)
        across = jnp.einsum('thn,hpn->thp', c_heads, entering_b) * jnp.exp(cumulative).T[:, :, None]
        to_end = (jnp.exp(cumulative[:, -1:] - cumulative) * step_block).T
        scaled = lax.optimization_barrier((b_heads * to_end[:, :, None]).astype(jnp.bfloat16)).astype(jnp.float32)
        block_state = jnp.einsum('shp,shn->hpn', x_heads, scaled)
        renewed = jnp.exp(cumulative[:, -1])[:, None, None] * carried + block_state
        output = within + across + skip_gain[None, :, None] * x_heads
        return (renewed, output)
    x_blocks = ssm_input.reshape(nblocks, BLOCK, HEAD_COUNT * HEAD_DIM)
    b_blocks = b_proj.reshape(nblocks, BLOCK, GROUPS * STATE)
    c_blocks = c_proj.reshape(nblocks, BLOCK, GROUPS * STATE)
    step_blocks = step_size.reshape(HEAD_COUNT, nblocks, BLOCK).transpose(1, 0, 2)
    decay_blocks = log_decay.reshape(HEAD_COUNT, nblocks, BLOCK).transpose(1, 0, 2)
    start_state = jnp.zeros((HEAD_COUNT, HEAD_DIM, STATE), jnp.float32)
    unused, outputs = lax.scan(block_step, start_state, (x_blocks, b_blocks, c_blocks, step_blocks, decay_blocks))
    output = outputs.reshape(SEQUENCE_LENGTH, HEAD_COUNT * HEAD_DIM)
    gated_rows = output * jax.nn.silu(gate_input.astype(jnp.float32))
    squares = lax.optimization_barrier(jnp.sum(gated_rows * gated_rows, axis=1, keepdims=True))
    normed = (gated_rows * lax.rsqrt(squares / (HEAD_COUNT * HEAD_DIM) + epsilon) * norm_gain).astype(jnp.bfloat16)
    return jnp.dot(normed, out_weight, preferred_element_type=jnp.float32).astype(jnp.bfloat16)
```

```python
import jax
import jax.numpy as jnp
from jax import lax
from jax.experimental import pallas as pl
from jax.experimental.pallas import tpu as pltpu
from jax.sharding import PartitionSpec as P

HEAD_COUNT = 80
HEAD_DIM = 64
STATE = 128
GROUPS = 8
BLOCK = 256
RING = 4
SUB = 128
EXTRA = 8

epsilon = 1e-05


f32 = jnp.float32
bf16 = jnp.bfloat16
HIGH = lax.Precision.HIGHEST
CC = (((0,), (0,)), ((), ()))
TT = (((1,), (1,)), ((), ()))


def triangle(size):
    rows = lax.broadcasted_iota(jnp.int32, (size, size), 0)
    columns = lax.broadcasted_iota(jnp.int32, (size, size), 1)
    return rows <= columns


def spread_matrix(heads):
    rows = lax.broadcasted_iota(jnp.int32, (heads, heads * HEAD_DIM), 0)
    columns = lax.broadcasted_iota(jnp.int32, (heads, heads * HEAD_DIM), 1)
    return (rows == columns // HEAD_DIM).astype(f32)


def spread_rows(values, spread):
    return lax.dot_general(values, spread, CC, precision=HIGH, preferred_element_type=f32)


def split3(value):
    high = value.astype(bf16)
    rest = value - high.astype(f32)
    middle = rest.astype(bf16)
    return high, middle, (rest - middle.astype(f32)).astype(bf16)


def state_kernel(scalars, x_ref, b_ref, step_ref, decay_ref, prefix_ref, total_ref, cum_ref):
    heads, tokens = step_ref.shape
    blocks = tokens // BLOCK
    spread = spread_matrix(heads)
    sums = triangle(BLOCK).astype(f32)
    state = jnp.zeros((STATE, heads * HEAD_DIM), f32)
    offset = jnp.zeros((heads, 1), f32)
    for c in range(blocks):
        span = slice(c * BLOCK, (c + 1) * BLOCK)
        cumulative = jnp.dot(decay_ref[:, span], sums, precision=HIGH, preferred_element_type=f32)
        cum_ref[:, span] = cumulative + offset
        end = cumulative[:, BLOCK - 1 :]
        offset = offset + end
        prefix_ref[c] = state.astype(bf16)
        to_end = jnp.exp(end - cumulative) * step_ref[:, span]
        scaled = (x_ref[span, :].astype(f32) * spread_rows(to_end, spread)).astype(bf16)
        block_state = lax.dot_general(b_ref[span, :], scaled, CC, preferred_element_type=f32)
        state = spread_rows(jnp.exp(end), spread) * state + block_state
    total_ref[0:STATE, :] = state.astype(bf16)
    parts = split3(spread_rows(offset, spread))
    rows = jnp.concatenate([part.astype(f32) for part in parts] + [jnp.zeros((EXTRA - 3, heads * HEAD_DIM), f32)], axis=0)
    total_ref[STATE:, :] = rows.astype(bf16)


def within_kernel(scalars, x_ref, b_ref, c_ref, step_ref, decay_ref, skip_ref, prefix_ref, out_ref):
    heads = step_ref.shape[0]
    spread = spread_matrix(heads)
    lower = triangle(BLOCK)
    cumulative = jnp.dot(decay_ref[...], lower.astype(f32), precision=HIGH, preferred_element_type=f32)
    x_block = x_ref[...]
    c_block = c_ref[...]
    scores = lax.dot_general(c_block, b_ref[...], TT, preferred_element_type=f32)
    causal = jnp.logical_not(lower) | (
        lax.broadcasted_iota(jnp.int32, (BLOCK, BLOCK), 0) == lax.broadcasted_iota(jnp.int32, (BLOCK, BLOCK), 1)
    )
    columns = cumulative.T
    pieces = []
    for h in range(heads):
        differ = columns[:, h : h + 1] - cumulative[h : h + 1, :]
        weights = scores * jnp.exp(jnp.where(causal, differ, -jnp.inf)) * step_ref[h : h + 1, :]
        pieces.append(
            jnp.dot(weights.astype(bf16), x_block[:, h * HEAD_DIM : (h + 1) * HEAD_DIM], preferred_element_type=f32)
        )
    across = jnp.dot(c_block, prefix_ref[0], preferred_element_type=f32)
    across = across * spread_rows(jnp.exp(cumulative), spread)
    skip = lax.dot_general(skip_ref[...], spread, (((1,), (0,)), ((), ())), precision=HIGH, preferred_element_type=f32)
    out_ref[...] = jnp.concatenate(pieces, axis=1) + across + skip * x_block.astype(f32)


def gate_kernel(scalars, out_ref, gate_ref, c_ref, cum_ref, *refs):
    totals, results = refs[:-RING], refs[-RING:]
    heads = cum_ref.shape[0]
    spread = spread_matrix(heads)
    incoming = jnp.zeros((STATE, heads * HEAD_DIM), f32)
    log_sum = jnp.zeros((1, heads * HEAD_DIM), f32)
    for total in totals:
        incoming = incoming + jnp.exp(log_sum) * total[0:STATE, :].astype(f32)
        log_sum = log_sum + jnp.sum(total[STATE:, :].astype(f32), axis=0, keepdims=True)
    incoming = incoming.astype(bf16)
    for su in range(RING):
        for sv in range(RING):
            start = pl.multiple_of(scalars[1 + su * RING + sv] * SUB, SUB)
            rows = pl.ds(start, SUB)
            across = jnp.dot(c_ref[rows, :], incoming, preferred_element_type=f32)
            across = across * spread_rows(jnp.exp(cum_ref[:, rows]), spread)
            gate = gate_ref[rows, :].astype(f32)
            gated = (out_ref[rows, :] + across) * (gate / (1.0 + jnp.exp(-gate)))
            results[su][sv * SUB : (sv + 1) * SUB, :] = gated.astype(bf16)


def project_kernel(scalars, gain_ref, *refs):
    rows = refs[:RING]
    weights = refs[RING : 2 * RING]
    results = refs[2 * RING : 3 * RING]
    left, squares = refs[3 * RING :]

    @pl.when(pl.program_id(0) == 0)
    def prepare():
        pieces = []
        total = None
        for s in range(RING):
            values = rows[s][...].astype(f32)
            gain = gain_ref[pl.ds(scalars[17 + s], 1), :]
            pieces.append((values * gain).astype(bf16))
            part = jnp.sum(values * values, axis=1, keepdims=True)
            total = part if total is None else total + part
        left[...] = jnp.concatenate(pieces, axis=1)
        squares[...] = jnp.broadcast_to(total, squares.shape)

    right = jnp.concatenate([w[...] for w in weights], axis=0)
    product = jnp.dot(left[...], right, preferred_element_type=f32)
    for s in range(RING):
        results[s][0:SUB, :] = product[s * SUB : (s + 1) * SUB, :].astype(bf16)
        row = squares[s * SUB : (s + 1) * SUB, :].T[0:1, :]
        parts = split3(row)
        tail = jnp.concatenate([part.astype(f32) for part in parts] + [jnp.zeros((EXTRA - 3, SUB), f32)], axis=0)
        width = results[s].shape[1]
        results[s][SUB:, :] = jnp.concatenate([tail] * (width // SUB), axis=1).astype(bf16)


def finish_kernel(channels, *refs):
    parts, out_ref = refs[:-1], refs[-1]
    total = parts[0][0:SUB, :].astype(f32)
    squares = parts[0][SUB:, 0:SUB].astype(f32)
    for part in parts[1:]:
        total = total + part[0:SUB, :].astype(f32)
        squares = squares + part[SUB:, 0:SUB].astype(f32)
    squares = jnp.sum(squares, axis=0, keepdims=True)
    scale = lax.rsqrt(squares / channels + epsilon)
    column = jnp.broadcast_to(scale, (SUB, SUB)).T[:, 0:1]
    out_ref[...] = (total * column).astype(bf16)


def ring_pairs(shift, gather):
    pairs = []
    for y in range(RING):
        for x in range(RING):
            for core in range(2):
                if (core == 0) == gather:
                    there = y * RING + (x + shift) % RING
                else:
                    there = ((y + shift) % RING) * RING + x
                pairs.append(((y * RING + x) * 2 + core, there * 2 + core))
    return pairs


def ring(value, shift, gather):
    return lax.ppermute(value, ("head", "batch"), ring_pairs(shift, gather))


def body(
    ssm_input, gate_input, b_proj, c_proj, step_size, log_decay, skip_gain, norm_gain, out_weight
):
    tokens, channels = ssm_input.shape
    heads = step_size.shape[0]
    width = out_weight.shape[1]
    blocks = tokens // BLOCK
    seq_count = lax.axis_size("seq")
    head_index = lax.axis_index("head")
    core = lax.axis_index("batch")
    group = head_index * heads * GROUPS // HEAD_COUNT
    y, x = head_index // RING, head_index % RING
    u = jnp.where(core == 0, x, y)
    v = jnp.where(core == 0, y, x)

    def head_at(u_there, v_there):
        return jnp.where(core == 0, v_there * RING + u_there, u_there * RING + v_there)

    shifts = jnp.arange(RING)
    positions = head_at((u + shifts[:, None]) % RING, (v + shifts[None, :]) % RING).reshape(-1)
    sources = head_at((u - shifts) % RING, v)
    scalars = jnp.concatenate([group[None], positions, sources]).astype(jnp.int32)

    weights = [out_weight] + [ring(out_weight, s, True) for s in range(1, RING)]

    params = pltpu.CompilerParams(vmem_limit_bytes=60000 * 1024)
    prefix, total, cum = pl.pallas_call(
        state_kernel,
        grid_spec=pltpu.PrefetchScalarGridSpec(
            num_scalar_prefetch=1,
            grid=(1,),
            in_specs=[
                pl.BlockSpec((tokens, channels), lambda i, s: (0, 0)),
                pl.BlockSpec((tokens, STATE), lambda i, s: (0, s[0])),
                pl.BlockSpec((heads, tokens), lambda i, s: (0, 0)),
                pl.BlockSpec((heads, tokens), lambda i, s: (0, 0)),
            ],
            out_specs=[
                pl.BlockSpec((blocks, STATE, channels), lambda i, s: (0, 0, 0)),
                pl.BlockSpec((STATE + EXTRA, channels), lambda i, s: (0, 0)),
                pl.BlockSpec((heads, tokens), lambda i, s: (0, 0)),
            ],
        ),
        out_shape=[
            jax.ShapeDtypeStruct((blocks, STATE, channels), bf16),
            jax.ShapeDtypeStruct((STATE + EXTRA, channels), bf16),
            jax.ShapeDtypeStruct((heads, tokens), f32),
        ],
        compiler_params=params,
        name="state",
    )(scalars, ssm_input, b_proj, step_size, log_decay)

    totals = [
        lax.ppermute(total, "seq", [(k, k + s) for k in range(seq_count - s)]) for s in range(1, seq_count)
    ]

    local = pl.pallas_call(
        within_kernel,
        grid_spec=pltpu.PrefetchScalarGridSpec(
            num_scalar_prefetch=1,
            grid=(blocks,),
            in_specs=[
                pl.BlockSpec((BLOCK, channels), lambda i, s: (i, 0)),
                pl.BlockSpec((BLOCK, STATE), lambda i, s: (i, s[0])),
                pl.BlockSpec((BLOCK, STATE), lambda i, s: (i, s[0])),
                pl.BlockSpec((heads, BLOCK), lambda i, s: (0, i)),
                pl.BlockSpec((heads, BLOCK), lambda i, s: (0, i)),
                pl.BlockSpec((1, heads), lambda i, s: (0, 0)),
                pl.BlockSpec((1, STATE, channels), lambda i, s: (i, 0, 0)),
            ],
            out_specs=pl.BlockSpec((BLOCK, channels), lambda i, s: (i, 0)),
        ),
        out_shape=jax.ShapeDtypeStruct((tokens, channels), f32),
        compiler_params=params,
        name="within",
    )(scalars, ssm_input, b_proj, c_proj, step_size, log_decay, skip_gain.reshape(1, heads), prefix)

    quarter = tokens // RING
    gated = pl.pallas_call(
        gate_kernel,
        grid_spec=pltpu.PrefetchScalarGridSpec(
            num_scalar_prefetch=1,
            grid=(1,),
            in_specs=[
                pl.BlockSpec((tokens, channels), lambda i, s: (0, 0)),
                pl.BlockSpec((tokens, channels), lambda i, s: (0, 0)),
                pl.BlockSpec((tokens, STATE), lambda i, s: (0, s[0])),
                pl.BlockSpec((heads, tokens), lambda i, s: (0, 0)),
            ]
            + [pl.BlockSpec((STATE + EXTRA, channels), lambda i, s: (0, 0))] * (seq_count - 1),
            out_specs=[pl.BlockSpec((quarter, channels), lambda i, s: (0, 0))] * RING,
        ),
        out_shape=[jax.ShapeDtypeStruct((quarter, channels), bf16)] * RING,
        compiler_params=params,
        name="gate",
    )(scalars, local, gate_input, c_proj, cum, *totals)

    rows = [gated[0]] + [ring(gated[s], s, True) for s in range(1, RING)]

    tile = 512
    parts = pl.pallas_call(
        project_kernel,
        grid_spec=pltpu.PrefetchScalarGridSpec(
            num_scalar_prefetch=1,
            grid=(width // tile,),
            in_specs=[pl.BlockSpec((RING * RING, channels), lambda i, s: (0, 0))]
            + [pl.BlockSpec((quarter, channels), lambda i, s: (0, 0))] * RING
            + [pl.BlockSpec((channels, tile), lambda i, s: (0, i))] * RING,
            out_specs=[pl.BlockSpec((SUB + EXTRA, tile), lambda i, s: (0, i))] * RING,
            scratch_shapes=[
                pltpu.VMEM((quarter, RING * channels), bf16),
                pltpu.VMEM((quarter, SUB), f32),
            ],
        ),
        out_shape=[jax.ShapeDtypeStruct((SUB + EXTRA, width), bf16)] * RING,
        compiler_params=params,
        name="project",
    )(scalars, norm_gain.reshape(RING * RING, channels), *rows, *weights)

    sums = [parts[0]] + [ring(parts[s], s, False) for s in range(1, RING)]

    return pl.pallas_call(
        lambda *refs: finish_kernel(HEAD_COUNT * HEAD_DIM, *refs),
        grid=(2,),
        in_specs=[pl.BlockSpec((SUB + EXTRA, width // 2), lambda i: (0, i))] * RING,
        out_specs=pl.BlockSpec((SUB, width // 2), lambda i: (0, i)),
        out_shape=jax.ShapeDtypeStruct((SUB, width), bf16),
        compiler_params=params,
        name="finish",
    )(*sums)


def solution(mesh):
    in_specs = (
        P(("batch", "seq"), "head"),
        P(("batch", "seq"), "head"),
        P(("batch", "seq"), None),
        P(("batch", "seq"), None),
        P("head", ("batch", "seq")),
        P("head", ("batch", "seq")),
        P("head"),
        P(),
        P("head", None),
    )
    out_specs = P(("batch", "seq", "head"), None)
    return jax.shard_map(body, mesh=mesh, in_specs=in_specs, out_specs=out_specs, check_vma=False)
```

```python
import jax
import jax.numpy as jnp
from jax import lax
from jax.experimental import pallas as pl
from jax.experimental.pallas import tpu as pltpu
from jax.sharding import PartitionSpec as P

HEAD_COUNT = 80
HEAD_DIM = 64
STATE = 128
GROUPS = 8
BLOCK = 256
RING = 4
SUB = 128
EXTRA = 8
PAD = 8

epsilon = 1e-05


f32 = jnp.float32
bf16 = jnp.bfloat16
TT = (((1,), (1,)), ((), ()))


def triangle(size, dtype):
    rows = lax.broadcasted_iota(jnp.int32, (size, size), 0)
    columns = lax.broadcasted_iota(jnp.int32, (size, size), 1)
    return (rows <= columns).astype(dtype)


def split3(value):
    high = value.astype(bf16)
    rest = value - high.astype(f32)
    middle = rest.astype(bf16)
    return high, middle, (rest - middle.astype(f32)).astype(bf16)


def join3(stacked, rows):
    return stacked[0:rows].astype(f32) + stacked[rows : 2 * rows].astype(f32) + stacked[2 * rows : 3 * rows].astype(f32)


def per_head(column, heads, lanes):
    return jnp.concatenate(
        [jnp.broadcast_to(column[h : h + 1, 0:1], (HEAD_DIM, lanes)) for h in range(heads)], axis=0
    )


def state_kernel(scalars, x_ref, b_ref, step_ref, decay_ref, prefix_ref, total_ref, cum_ref, factor_ref):
    heads, tokens = step_ref.shape
    blocks = tokens // BLOCK
    fill = jnp.zeros((PAD - heads, BLOCK), f32)
    decay = jnp.concatenate(
        [piece for c in range(blocks) for piece in (decay_ref[:, c * BLOCK : (c + 1) * BLOCK], fill)], axis=0
    )
    sums = jnp.dot(
        jnp.concatenate(split3(decay), axis=0), triangle(BLOCK, bf16), preferred_element_type=f32
    )
    sums = join3(sums, blocks * PAD)
    state = jnp.zeros((heads * HEAD_DIM, STATE), f32)
    offset = jnp.zeros((PAD, 1), f32)
    for c in range(blocks):
        span = slice(c * BLOCK, (c + 1) * BLOCK)
        cumulative = sums[c * PAD : (c + 1) * PAD]
        cum_ref[:, span] = cumulative
        factor_ref[:, span] = jnp.exp(cumulative + offset)
        end = cumulative[:, BLOCK - 1 :]
        offset = offset + end
        prefix_ref[c] = state.astype(bf16)
        to_end = jnp.exp(end - cumulative)[0:heads] * step_ref[:, span]
        scaled = jnp.concatenate(
            [
                (x_ref[h * HEAD_DIM : (h + 1) * HEAD_DIM, span].astype(f32) * to_end[h : h + 1]).astype(bf16)
                for h in range(heads)
            ],
            axis=0,
        )
        block_state = jnp.dot(scaled, b_ref[span, :], preferred_element_type=f32)
        state = per_head(jnp.exp(end), heads, STATE) * state + block_state
    total_ref[0 : heads * HEAD_DIM, :] = state.astype(bf16)
    parts = split3(jnp.broadcast_to(offset, (PAD, STATE)))
    total_ref[heads * HEAD_DIM :, :] = jnp.concatenate(parts, axis=0)


def within_kernel(scalars, skip_ref, x_ref, b_ref, c_ref, cum_ref, step_ref, prefix_ref, out_ref):
    heads = step_ref.shape[0]
    half = BLOCK // 2
    causal = triangle(half, f32).T > 0
    for k in range(step_ref.shape[1] // BLOCK):
        span = slice(k * BLOCK, (k + 1) * BLOCK)
        c_block = c_ref[span, :]
        b_block = b_ref[span, :]
        scores_first = lax.dot_general(c_block[:half], b_block[:half], TT, preferred_element_type=f32)
        scores_second = lax.dot_general(c_block[half:], b_block, TT, preferred_element_type=f32)
        across = lax.dot_general(prefix_ref[k], c_block, TT, preferred_element_type=f32)
        cumulative = cum_ref[:, span]
        factor = jnp.exp(cumulative)
        columns = cumulative.T
        for h in range(heads):
            channels = slice(h * HEAD_DIM, (h + 1) * HEAD_DIM)
            x_head = x_ref[channels, span]
            row = cumulative[h : h + 1]
            step = step_ref[h : h + 1, span]
            differ = columns[:half, h : h + 1] - row[:, :half]
            first = scores_first * jnp.exp(jnp.where(causal, differ, -jnp.inf)) * step[:, :half]
            column = columns[half:, h : h + 1]
            full = scores_second[:, :half] * jnp.exp(column - row[:, :half]) * step[:, :half]
            differ = column - row[:, half:]
            last = scores_second[:, half:] * jnp.exp(jnp.where(causal, differ, -jnp.inf)) * step[:, half:]
            second = jnp.concatenate([full, last], axis=1)
            within = jnp.concatenate(
                [
                    lax.dot_general(x_head[:, :half], first.astype(bf16), TT, preferred_element_type=f32),
                    lax.dot_general(x_head, second.astype(bf16), TT, preferred_element_type=f32),
                ],
                axis=1,
            )
            out_ref[channels, span] = (
                within + across[channels] * factor[h : h + 1] + skip_ref[h] * x_head.astype(f32)
            )


def gate_kernel(scalars, out_ref, gate_ref, c_ref, factor_ref, *refs):
    totals, results = refs[:-RING], refs[-RING:]
    channels = out_ref.shape[0]
    heads = channels // HEAD_DIM
    incoming = jnp.zeros((channels, STATE), f32)
    log_sum = jnp.zeros((PAD, STATE), f32)
    for total in totals:
        incoming = incoming + per_head(jnp.exp(log_sum), heads, STATE) * total[0:channels, :].astype(f32)
        log_sum = log_sum + join3(total[channels:, :], PAD)
    incoming = incoming.astype(bf16)
    for su in range(RING):
        for sv in range(RING):
            span = pl.ds(pl.multiple_of(scalars[1 + su * RING + sv] * SUB, SUB), SUB)
            across = lax.dot_general(incoming, c_ref[span, :], TT, preferred_element_type=f32)
            factor = factor_ref[:, span]
            for h in range(heads):
                rows = slice(h * HEAD_DIM, (h + 1) * HEAD_DIM)
                gate = gate_ref[rows, span].astype(f32)
                output = out_ref[rows, span] + across[rows] * factor[h : h + 1]
                gated = output * (gate / (1.0 + jnp.exp(-gate)))
                results[su][rows, sv * SUB : (sv + 1) * SUB] = gated.astype(bf16)


def project_kernel(gain_ref, *refs):
    rows = refs[:RING]
    weights = refs[RING : 2 * RING]
    results = refs[2 * RING : 3 * RING]
    left, squares = refs[3 * RING :]
    channels = rows[0].shape[0]

    @pl.when(pl.program_id(0) == 0)
    def prepare():
        total = None
        pieces = []
        for s in range(RING):
            values = rows[s][...].astype(f32)
            gain = gain_ref[s * channels : (s + 1) * channels, :]
            pieces.append((values * gain).astype(bf16))
            part = jnp.sum(values * values, axis=0, keepdims=True)
            total = part if total is None else total + part
        left[...] = jnp.concatenate(pieces, axis=0).T
        squares[...] = jnp.broadcast_to(total, squares.shape)

    right = jnp.concatenate([w[...] for w in weights], axis=0)
    product = jnp.dot(left[...], right, preferred_element_type=f32)
    zeros = jnp.zeros((EXTRA - 3, SUB), f32)
    for s in range(RING):
        results[s][0:SUB, :] = product[s * SUB : (s + 1) * SUB, :].astype(bf16)
        parts = split3(squares[0:1, s * SUB : (s + 1) * SUB])
        tail = jnp.concatenate([part.astype(f32) for part in parts] + [zeros], axis=0)
        results[s][SUB:, :] = jnp.concatenate([tail] * (results[s].shape[1] // SUB), axis=1).astype(bf16)


def finish_kernel(channels, *refs):
    parts, out_ref = refs[:-1], refs[-1]
    total = parts[0][0:SUB, :].astype(f32)
    squares = parts[0][SUB:, 0:SUB].astype(f32)
    for part in parts[1:]:
        total = total + part[0:SUB, :].astype(f32)
        squares = squares + part[SUB:, 0:SUB].astype(f32)
    squares = jnp.sum(squares, axis=0, keepdims=True)
    scale = lax.rsqrt(squares / channels + epsilon)
    column = jnp.broadcast_to(scale, (SUB, SUB)).T[:, 0:1]
    out_ref[...] = (total * column).astype(bf16)


def ring_pairs(shift, gather):
    pairs = []
    for y in range(RING):
        for x in range(RING):
            for core in range(2):
                if (core == 0) == gather:
                    there = y * RING + (x + shift) % RING
                else:
                    there = ((y + shift) % RING) * RING + x
                pairs.append(((y * RING + x) * 2 + core, there * 2 + core))
    return pairs


def ring(value, shift, gather):
    return lax.ppermute(value, ("head", "batch"), ring_pairs(shift, gather))


def body(
    ssm_input, gate_input, b_proj, c_proj, step_size, log_decay, skip_gain, norm_gain, out_weight
):
    tokens, channels = ssm_input.shape
    heads = step_size.shape[0]
    width = out_weight.shape[1]
    blocks = tokens // BLOCK
    seq_count = lax.axis_size("seq")
    head_index = lax.axis_index("head")
    core = lax.axis_index("batch")
    group = head_index * heads * GROUPS // HEAD_COUNT
    y, x = head_index // RING, head_index % RING
    u = jnp.where(core == 0, x, y)
    v = jnp.where(core == 0, y, x)

    def head_at(u_there, v_there):
        return jnp.where(core == 0, v_there * RING + u_there, u_there * RING + v_there)

    shifts = jnp.arange(RING)
    positions = head_at((u + shifts[:, None]) % RING, (v + shifts[None, :]) % RING).reshape(-1)
    sources = head_at((u - shifts) % RING, v)
    scalars = jnp.concatenate([group[None], positions]).astype(jnp.int32)

    weights = [out_weight] + [ring(out_weight, s, True) for s in range(1, RING)]

    params = pltpu.CompilerParams(vmem_limit_bytes=60000 * 1024)
    ssm_columns = ssm_input.T
    gate_columns = gate_input.T
    payload = channels + 3 * PAD
    prefix, total, cum, factor = pl.pallas_call(
        state_kernel,
        grid_spec=pltpu.PrefetchScalarGridSpec(
            num_scalar_prefetch=1,
            grid=(1,),
            in_specs=[
                pl.BlockSpec((channels, tokens), lambda i, s: (0, 0)),
                pl.BlockSpec((tokens, STATE), lambda i, s: (0, s[0])),
                pl.BlockSpec((heads, tokens), lambda i, s: (0, 0)),
                pl.BlockSpec((heads, tokens), lambda i, s: (0, 0)),
            ],
            out_specs=[
                pl.BlockSpec((blocks, channels, STATE), lambda i, s: (0, 0, 0)),
                pl.BlockSpec((payload, STATE), lambda i, s: (0, 0)),
                pl.BlockSpec((PAD, tokens), lambda i, s: (0, 0)),
                pl.BlockSpec((PAD, tokens), lambda i, s: (0, 0)),
            ],
        ),
        out_shape=[
            jax.ShapeDtypeStruct((blocks, channels, STATE), bf16),
            jax.ShapeDtypeStruct((payload, STATE), bf16),
            jax.ShapeDtypeStruct((PAD, tokens), f32),
            jax.ShapeDtypeStruct((PAD, tokens), f32),
        ],
        compiler_params=params,
        name="state",
    )(scalars, ssm_columns, b_proj, step_size, log_decay)

    totals = [
        lax.ppermute(total, "seq", [(k, k + s) for k in range(seq_count - s)]) for s in range(1, seq_count)
    ]

    per_step = 2
    local = pl.pallas_call(
        within_kernel,
        grid_spec=pltpu.PrefetchScalarGridSpec(
            num_scalar_prefetch=1,
            grid=(blocks // per_step,),
            in_specs=[
                pl.BlockSpec(memory_space=pltpu.SMEM),
                pl.BlockSpec((channels, per_step * BLOCK), lambda i, s: (0, i)),
                pl.BlockSpec((per_step * BLOCK, STATE), lambda i, s: (i, s[0])),
                pl.BlockSpec((per_step * BLOCK, STATE), lambda i, s: (i, s[0])),
                pl.BlockSpec((PAD, per_step * BLOCK), lambda i, s: (0, i)),
                pl.BlockSpec((heads, per_step * BLOCK), lambda i, s: (0, i)),
                pl.BlockSpec((per_step, channels, STATE), lambda i, s: (i, 0, 0)),
            ],
            out_specs=pl.BlockSpec((channels, per_step * BLOCK), lambda i, s: (0, i)),
        ),
        out_shape=jax.ShapeDtypeStruct((channels, tokens), f32),
        compiler_params=params,
        name="within",
    )(scalars, skip_gain, ssm_columns, b_proj, c_proj, cum, step_size, prefix)

    quarter = tokens // RING
    gated = pl.pallas_call(
        gate_kernel,
        grid_spec=pltpu.PrefetchScalarGridSpec(
            num_scalar_prefetch=1,
            grid=(1,),
            in_specs=[
                pl.BlockSpec((channels, tokens), lambda i, s: (0, 0)),
                pl.BlockSpec((channels, tokens), lambda i, s: (0, 0)),
                pl.BlockSpec((tokens, STATE), lambda i, s: (0, s[0])),
                pl.BlockSpec((PAD, tokens), lambda i, s: (0, 0)),
            ]
            + [pl.BlockSpec((payload, STATE), lambda i, s: (0, 0))] * (seq_count - 1),
            out_specs=[pl.BlockSpec((channels, quarter), lambda i, s: (0, 0))] * RING,
        ),
        out_shape=[jax.ShapeDtypeStruct((channels, quarter), bf16)] * RING,
        compiler_params=params,
        name="gate",
    )(scalars, local, gate_columns, c_proj, factor, *totals)

    rows = [gated[0]] + [ring(gated[s], s, True) for s in range(1, RING)]

    gains = norm_gain.reshape(RING * RING, channels)[sources].reshape(RING * channels, 1)
    tile = 512
    parts = pl.pallas_call(
        project_kernel,
        grid=(width // tile,),
        in_specs=[pl.BlockSpec((RING * channels, 1), lambda i: (0, 0))]
        + [pl.BlockSpec((channels, quarter), lambda i: (0, 0))] * RING
        + [pl.BlockSpec((channels, tile), lambda i: (0, i))] * RING,
        out_specs=[pl.BlockSpec((SUB + EXTRA, tile), lambda i: (0, i))] * RING,
        scratch_shapes=[
            pltpu.VMEM((quarter, RING * channels), bf16),
            pltpu.VMEM((PAD, quarter), f32),
        ],
        out_shape=[jax.ShapeDtypeStruct((SUB + EXTRA, width), bf16)] * RING,
        compiler_params=params,
        name="project",
    )(gains, *rows, *weights)

    sums = [parts[0]] + [ring(parts[s], s, False) for s in range(1, RING)]

    return pl.pallas_call(
        lambda *refs: finish_kernel(HEAD_COUNT * HEAD_DIM, *refs),
        grid=(2,),
        in_specs=[pl.BlockSpec((SUB + EXTRA, width // 2), lambda i: (0, i))] * RING,
        out_specs=pl.BlockSpec((SUB, width // 2), lambda i: (0, i)),
        out_shape=jax.ShapeDtypeStruct((SUB, width), bf16),
        compiler_params=params,
        name="finish",
    )(*sums)


def solution(mesh):
    in_specs = (
        P(("batch", "seq"), "head"),
        P(("batch", "seq"), "head"),
        P(("batch", "seq"), None),
        P(("batch", "seq"), None),
        P("head", ("batch", "seq")),
        P("head", ("batch", "seq")),
        P("head"),
        P(),
        P("head", None),
    )
    out_specs = P(("batch", "seq", "head"), None)
    return jax.shard_map(body, mesh=mesh, in_specs=in_specs, out_specs=out_specs, check_vma=False)
```

```python
import jax
import jax.numpy as jnp
from jax import lax
from jax.experimental import pallas as pl
from jax.experimental.pallas import tpu as pltpu
from jax.sharding import PartitionSpec as P

HEAD_COUNT = 80
HEAD_DIM = 64
STATE = 128
GROUPS = 8
BLOCK = 256
RING = 4
SUB = 128
EXTRA = 8
PAD = 8

epsilon = 1e-05


f32 = jnp.float32
bf16 = jnp.bfloat16
TT = (((1,), (1,)), ((), ()))


def triangle(size, dtype):
    rows = lax.broadcasted_iota(jnp.int32, (size, size), 0)
    columns = lax.broadcasted_iota(jnp.int32, (size, size), 1)
    return (rows <= columns).astype(dtype)


def split3(value):
    high = value.astype(bf16)
    rest = value - high.astype(f32)
    middle = rest.astype(bf16)
    return high, middle, (rest - middle.astype(f32)).astype(bf16)


def join3(stacked, rows):
    return stacked[0:rows].astype(f32) + stacked[rows : 2 * rows].astype(f32) + stacked[2 * rows : 3 * rows].astype(f32)


def per_head(column, heads, lanes):
    return jnp.concatenate(
        [jnp.broadcast_to(column[h : h + 1, 0:1], (HEAD_DIM, lanes)) for h in range(heads)], axis=0
    )


def state_kernel(x_ref, b_hbm, c_hbm, step_ref, decay_ref, prefix_ref, total_ref, cum_ref, factor_ref, b_ref, c_ref, sems):
    heads, tokens = step_ref.shape
    blocks = tokens // BLOCK
    group = lax.axis_index("head") * heads * GROUPS // HEAD_COUNT
    columns = pl.ds(pl.multiple_of(group * STATE, STATE), STATE)
    fetch_b = pltpu.make_async_copy(b_hbm.at[:, columns], b_ref, sems.at[0])
    fetch_c = pltpu.make_async_copy(c_hbm.at[:, columns], c_ref, sems.at[1])
    fetch_b.start()
    fetch_c.start()
    fill = jnp.zeros((PAD - heads, BLOCK), f32)
    decay = jnp.concatenate(
        [piece for c in range(blocks) for piece in (decay_ref[:, c * BLOCK : (c + 1) * BLOCK], fill)], axis=0
    )
    sums = jnp.dot(
        jnp.concatenate(split3(decay), axis=0), triangle(BLOCK, bf16), preferred_element_type=f32
    )
    sums = join3(sums, blocks * PAD)
    offset = jnp.zeros((PAD, 1), f32)
    for c in range(blocks):
        span = slice(c * BLOCK, (c + 1) * BLOCK)
        cumulative = sums[c * PAD : (c + 1) * PAD]
        cum_ref[:, span] = cumulative
        factor_ref[:, span] = jnp.exp(cumulative + offset)
        offset = offset + cumulative[:, BLOCK - 1 :]
    fetch_b.wait()
    state = jnp.zeros((heads * HEAD_DIM, STATE), f32)
    for c in range(blocks):
        span = slice(c * BLOCK, (c + 1) * BLOCK)
        cumulative = sums[c * PAD : (c + 1) * PAD]
        end = cumulative[:, BLOCK - 1 :]
        prefix_ref[c] = state.astype(bf16)
        to_end = jnp.exp(end - cumulative)[0:heads] * step_ref[:, span]
        scaled = jnp.concatenate(
            [
                (x_ref[h * HEAD_DIM : (h + 1) * HEAD_DIM, span].astype(f32) * to_end[h : h + 1]).astype(bf16)
                for h in range(heads)
            ],
            axis=0,
        )
        block_state = jnp.dot(scaled, b_ref[span, :], preferred_element_type=f32)
        state = per_head(jnp.exp(end), heads, STATE) * state + block_state
    total_ref[0 : heads * HEAD_DIM, :] = state.astype(bf16)
    parts = split3(jnp.broadcast_to(offset, (PAD, STATE)))
    total_ref[heads * HEAD_DIM :, :] = jnp.concatenate(parts, axis=0)
    fetch_c.wait()


def within_kernel(skip_ref, x_ref, b_ref, c_ref, cum_ref, step_ref, prefix_ref, out_ref):
    heads = step_ref.shape[0]
    half = BLOCK // 2
    causal = triangle(half, f32).T > 0
    for k in range(step_ref.shape[1] // BLOCK):
        span = slice(k * BLOCK, (k + 1) * BLOCK)
        c_block = c_ref[span, :]
        b_block = b_ref[span, :]
        scores_first = lax.dot_general(c_block[:half], b_block[:half], TT, preferred_element_type=f32)
        scores_second = lax.dot_general(c_block[half:], b_block, TT, preferred_element_type=f32)
        across = lax.dot_general(prefix_ref[k], c_block, TT, preferred_element_type=f32)
        cumulative = cum_ref[:, span]
        factor = jnp.exp(cumulative)
        columns = cumulative.T
        for h in range(heads):
            channels = slice(h * HEAD_DIM, (h + 1) * HEAD_DIM)
            x_head = x_ref[channels, span]
            row = cumulative[h : h + 1]
            step = step_ref[h : h + 1, span]
            differ = columns[:half, h : h + 1] - row[:, :half]
            first = scores_first * jnp.exp(jnp.where(causal, differ, -jnp.inf)) * step[:, :half]
            column = columns[half:, h : h + 1]
            full = scores_second[:, :half] * jnp.exp(column - row[:, :half]) * step[:, :half]
            differ = column - row[:, half:]
            last = scores_second[:, half:] * jnp.exp(jnp.where(causal, differ, -jnp.inf)) * step[:, half:]
            second = jnp.concatenate([full, last], axis=1)
            within = jnp.concatenate(
                [
                    lax.dot_general(x_head[:, :half], first.astype(bf16), TT, preferred_element_type=f32),
                    lax.dot_general(x_head, second.astype(bf16), TT, preferred_element_type=f32),
                ],
                axis=1,
            )
            out_ref[channels, span] = (
                within + across[channels] * factor[h : h + 1] + skip_ref[h] * x_head.astype(f32)
            )


def ring_place():
    head_index = lax.axis_index("head")
    core = lax.axis_index("batch")
    y, x = head_index // RING, head_index % RING
    return core, jnp.where(core == 0, x, y), jnp.where(core == 0, y, x)


def head_at(core, u, v):
    return jnp.where(core == 0, v * RING + u, u * RING + v)


def gate_kernel(out_ref, gate_ref, c_ref, factor_ref, *refs):
    totals, results = refs[:-RING], refs[-RING:]
    channels = out_ref.shape[0]
    heads = channels // HEAD_DIM
    incoming = jnp.zeros((channels, STATE), f32)
    log_sum = jnp.zeros((PAD, STATE), f32)
    for total in totals:
        incoming = incoming + per_head(jnp.exp(log_sum), heads, STATE) * total[0:channels, :].astype(f32)
        log_sum = log_sum + join3(total[channels:, :], PAD)
    incoming = incoming.astype(bf16)
    core, u, v = ring_place()
    for su in range(RING):
        for sv in range(RING):
            place = head_at(core, (u + su) % RING, (v + sv) % RING)
            span = pl.ds(pl.multiple_of(place * SUB, SUB), SUB)
            across = lax.dot_general(incoming, c_ref[span, :], TT, preferred_element_type=f32)
            factor = factor_ref[:, span]
            for h in range(heads):
                rows = slice(h * HEAD_DIM, (h + 1) * HEAD_DIM)
                gate = gate_ref[rows, span].astype(f32)
                output = out_ref[rows, span] + across[rows] * factor[h : h + 1]
                gated = output * (gate / (1.0 + jnp.exp(-gate)))
                results[su][rows, sv * SUB : (sv + 1) * SUB] = gated.astype(bf16)


def project_kernel(gain_ref, *refs):
    rows = refs[:RING]
    weights = refs[RING : 2 * RING]
    results = refs[2 * RING : 3 * RING]
    (left,) = refs[3 * RING :]
    channels, width = weights[0].shape
    tile = 512
    core, u, v = ring_place()
    total = None
    gains = []
    for s in range(RING):
        values = rows[s][...].astype(f32)
        first = head_at(core, (u - s + RING) % RING, v) * channels
        lines = gain_ref[pl.ds(first // SUB, 3), :]
        line = jnp.concatenate([lines[i : i + 1] for i in range(3)], axis=1)
        shifted = jnp.concatenate([line[:, SUB // 2 :], line[:, : SUB // 2]], axis=1)
        gains.append(jnp.where(first % SUB == 0, line, shifted)[:, :channels])
        part = jnp.sum(values * values, axis=0, keepdims=True)
        total = part if total is None else total + part
    values = jnp.concatenate([r[...] for r in rows], axis=0).T
    left[...] = (values.astype(f32) * jnp.concatenate(gains, axis=1)).astype(bf16)
    zeros = jnp.zeros((EXTRA - 3, SUB), f32)
    for s in range(RING):
        parts = split3(total[:, s * SUB : (s + 1) * SUB])
        tail = jnp.concatenate([part.astype(f32) for part in parts] + [zeros], axis=0)
        results[s][SUB:, :] = jnp.concatenate([tail] * (width // SUB), axis=1).astype(bf16)
    for n in range(width // tile):
        span = slice(n * tile, (n + 1) * tile)
        right = jnp.concatenate([w[:, span] for w in weights], axis=0)
        product = jnp.dot(left[...], right, preferred_element_type=f32)
        for s in range(RING):
            results[s][0:SUB, span] = product[s * SUB : (s + 1) * SUB, :].astype(bf16)


def finish_kernel(channels, *refs):
    parts, out_ref = refs[:-1], refs[-1]
    total = parts[0][0:SUB, :].astype(f32)
    squares = parts[0][SUB:, 0:SUB].astype(f32)
    for part in parts[1:]:
        total = total + part[0:SUB, :].astype(f32)
        squares = squares + part[SUB:, 0:SUB].astype(f32)
    squares = jnp.sum(squares, axis=0, keepdims=True)
    scale = lax.rsqrt(squares / channels + epsilon)
    column = jnp.broadcast_to(scale, (SUB, SUB)).T[:, 0:1]
    out_ref[...] = (total * column).astype(bf16)


def ring_pairs(shift, gather):
    pairs = []
    for y in range(RING):
        for x in range(RING):
            for core in range(2):
                if (core == 0) == gather:
                    there = y * RING + (x + shift) % RING
                else:
                    there = ((y + shift) % RING) * RING + x
                pairs.append(((y * RING + x) * 2 + core, there * 2 + core))
    return pairs


def ring(value, shift, gather):
    return lax.ppermute(value, ("head", "batch"), ring_pairs(shift, gather))


def body(
    ssm_input, gate_input, b_proj, c_proj, step_size, log_decay, skip_gain, norm_gain, out_weight
):
    tokens, channels = ssm_input.shape
    heads = step_size.shape[0]
    width = out_weight.shape[1]
    blocks = tokens // BLOCK
    seq_count = lax.axis_size("seq")
    core, u, v = ring_place()
    weights = [out_weight] + [ring(out_weight, s, True) for s in range(1, RING)]

    params = pltpu.CompilerParams(vmem_limit_bytes=24 * 1024 * 1024)
    near = pl.BlockSpec(memory_space=pltpu.VMEM)

    def hold(*values):
        return [pltpu.with_memory_space_constraint(value, pltpu.VMEM) for value in values]

    def far(value):
        return pltpu.with_memory_space_constraint(value, pltpu.HBM)

    payload = channels + 3 * PAD
    ssm_columns, gate_columns = ssm_input.T, gate_input.T
    prefix, total, cum, factor, b_own, c_own = pl.pallas_call(
        state_kernel,
        in_specs=[near, pl.BlockSpec(memory_space=pltpu.HBM), pl.BlockSpec(memory_space=pltpu.HBM), near, near],
        out_specs=[near] * 6,
        out_shape=[
            pltpu.VMEM((blocks, channels, STATE), bf16),
            pltpu.VMEM((payload, STATE), bf16),
            pltpu.VMEM((PAD, tokens), f32),
            pltpu.VMEM((PAD, tokens), f32),
            pltpu.VMEM((tokens, STATE), bf16),
            pltpu.VMEM((tokens, STATE), bf16),
        ],
        scratch_shapes=[pltpu.SemaphoreType.DMA((2,))],
        compiler_params=params,
        name="state",
    )(*hold(ssm_columns), far(b_proj), far(c_proj), *hold(step_size, log_decay))

    totals = [
        lax.ppermute(total, "seq", [(k, k + s) for k in range(seq_count - s)]) for s in range(1, seq_count)
    ]

    local = pl.pallas_call(
        within_kernel,
        in_specs=[pl.BlockSpec(memory_space=pltpu.SMEM)] + [near] * 6,
        out_specs=near,
        out_shape=pltpu.VMEM((channels, tokens), f32),
        compiler_params=params,
        name="within",
    )(skip_gain, *hold(ssm_columns, b_own, c_own, cum, step_size, prefix))

    quarter = tokens // RING
    gated = pl.pallas_call(
        gate_kernel,
        in_specs=[near] * (4 + seq_count - 1),
        out_specs=[near] * RING,
        out_shape=[pltpu.VMEM((channels, quarter), bf16)] * RING,
        compiler_params=params,
        name="gate",
    )(*hold(local, gate_columns, c_own, factor, *totals))

    rows = [gated[0]] + [ring(gated[s], s, True) for s in range(1, RING)]

    parts = pl.pallas_call(
        project_kernel,
        in_specs=[near] * (1 + 2 * RING),
        out_specs=[near] * RING,
        scratch_shapes=[pltpu.VMEM((quarter, RING * channels), bf16)],
        out_shape=[pltpu.VMEM((SUB + EXTRA, width), bf16)] * RING,
        compiler_params=params,
        name="project",
    )(*hold(norm_gain.reshape(-1, SUB), *rows, *weights))

    sums = [parts[0]] + [ring(parts[s], s, False) for s in range(1, RING)]

    return pl.pallas_call(
        lambda *refs: finish_kernel(HEAD_COUNT * HEAD_DIM, *refs),
        in_specs=[near] * RING,
        out_specs=pl.BlockSpec((SUB, width), lambda: (0, 0)),
        out_shape=jax.ShapeDtypeStruct((SUB, width), bf16),
        compiler_params=params,
        name="finish",
    )(*hold(*sums))


def solution(mesh):
    in_specs = (
        P(("batch", "seq"), "head"),
        P(("batch", "seq"), "head"),
        P(("batch", "seq"), None),
        P(("batch", "seq"), None),
        P("head", ("batch", "seq")),
        P("head", ("batch", "seq")),
        P("head"),
        P(),
        P("head", None),
    )
    out_specs = P(("batch", "seq", "head"), None)
    return jax.shard_map(body, mesh=mesh, in_specs=in_specs, out_specs=out_specs, check_vma=False)
```

```python
import jax
import jax.numpy as jnp
from jax import lax
from jax.experimental import pallas as pl
from jax.experimental.pallas import tpu as pltpu
from jax.sharding import PartitionSpec as P


HEAD_COUNT = 80
HEAD_DIM = 64
STATE = 128
GROUPS = 8
BLOCK = 256
RING = 4
SUB = 128
EXTRA = 8
PAD = 8

epsilon = 1e-05


f32 = jnp.float32
bf16 = jnp.bfloat16
TT = (((1,), (1,)), ((), ()))


def triangle(size, dtype):
    rows = lax.broadcasted_iota(jnp.int32, (size, size), 0)
    columns = lax.broadcasted_iota(jnp.int32, (size, size), 1)
    return (rows <= columns).astype(dtype)


def split3(value):
    high = value.astype(bf16)
    rest = value - high.astype(f32)
    middle = rest.astype(bf16)
    return high, middle, (rest - middle.astype(f32)).astype(bf16)


def join3(stacked, rows):
    return stacked[0:rows].astype(f32) + stacked[rows : 2 * rows].astype(f32) + stacked[2 * rows : 3 * rows].astype(f32)


def per_head(column, heads, lanes):
    return jnp.concatenate(
        [jnp.broadcast_to(column[h : h + 1, 0:1], (HEAD_DIM, lanes)) for h in range(heads)], axis=0
    )


def state_kernel(x_ref, b_hbm, c_hbm, step_ref, decay_ref, prefix_ref, total_ref, cum_ref, factor_ref, b_ref, c_ref, sems):
    heads, tokens = step_ref.shape
    blocks = tokens // BLOCK
    group = lax.axis_index("head") * heads * GROUPS // HEAD_COUNT
    columns = pl.ds(pl.multiple_of(group * STATE, STATE), STATE)
    fetch_b = pltpu.make_async_copy(b_hbm.at[:, columns], b_ref, sems.at[0])
    fetch_c = pltpu.make_async_copy(c_hbm.at[:, columns], c_ref, sems.at[1])
    fetch_b.start()
    fetch_c.start()
    fill = jnp.zeros((PAD - heads, BLOCK), f32)
    decay = jnp.concatenate(
        [piece for c in range(blocks) for piece in (decay_ref[:, c * BLOCK : (c + 1) * BLOCK], fill)], axis=0
    )
    sums = jnp.dot(
        jnp.concatenate(split3(decay), axis=0), triangle(BLOCK, bf16), preferred_element_type=f32
    )
    sums = join3(sums, blocks * PAD)
    offset = jnp.zeros((PAD, 1), f32)
    for c in range(blocks):
        span = slice(c * BLOCK, (c + 1) * BLOCK)
        cumulative = sums[c * PAD : (c + 1) * PAD]
        cum_ref[:, span] = cumulative
        factor_ref[:, span] = jnp.exp(cumulative + offset)
        offset = offset + cumulative[:, BLOCK - 1 :]
    fetch_b.wait()
    state = jnp.zeros((heads * HEAD_DIM, STATE), f32)
    for c in range(blocks):
        span = slice(c * BLOCK, (c + 1) * BLOCK)
        cumulative = sums[c * PAD : (c + 1) * PAD]
        end = cumulative[:, BLOCK - 1 :]
        prefix_ref[c] = state.astype(bf16)
        to_end = jnp.exp(end - cumulative)[0:heads] * step_ref[:, span]
        scaled = jnp.concatenate(
            [
                (x_ref[h * HEAD_DIM : (h + 1) * HEAD_DIM, span].astype(f32) * to_end[h : h + 1]).astype(bf16)
                for h in range(heads)
            ],
            axis=0,
        )
        block_state = jnp.dot(scaled, b_ref[span, :], preferred_element_type=f32)
        state = per_head(jnp.exp(end), heads, STATE) * state + block_state
    total_ref[0 : heads * HEAD_DIM, :] = state.astype(bf16)
    parts = split3(jnp.broadcast_to(offset, (PAD, STATE)))
    total_ref[heads * HEAD_DIM :, :] = jnp.concatenate(parts, axis=0)
    fetch_c.wait()


def within_kernel(skip_ref, x_ref, b_ref, c_ref, cum_ref, step_ref, prefix_ref, out_ref):
    heads = step_ref.shape[0]
    half = BLOCK // 2
    causal = triangle(half, f32).T > 0
    for k in range(step_ref.shape[1] // BLOCK):
        span = slice(k * BLOCK, (k + 1) * BLOCK)
        c_block = c_ref[span, :]
        b_block = b_ref[span, :]
        scores_first = lax.dot_general(c_block[:half], b_block[:half], TT, preferred_element_type=f32)
        scores_second = lax.dot_general(c_block[half:], b_block, TT, preferred_element_type=f32)
        across = lax.dot_general(prefix_ref[k], c_block, TT, preferred_element_type=f32)
        cumulative = cum_ref[:, span]
        factor = jnp.exp(cumulative)
        columns = cumulative.T
        for h in range(heads):
            channels = slice(h * HEAD_DIM, (h + 1) * HEAD_DIM)
            x_head = x_ref[channels, span]
            row = cumulative[h : h + 1]
            step = step_ref[h : h + 1, span]
            differ = columns[:half, h : h + 1] - row[:, :half]
            first = scores_first * jnp.exp(jnp.where(causal, differ, -jnp.inf)) * step[:, :half]
            column = columns[half:, h : h + 1]
            full = scores_second[:, :half] * jnp.exp(column - row[:, :half]) * step[:, :half]
            differ = column - row[:, half:]
            last = scores_second[:, half:] * jnp.exp(jnp.where(causal, differ, -jnp.inf)) * step[:, half:]
            second = jnp.concatenate([full, last], axis=1)
            within = jnp.concatenate(
                [
                    lax.dot_general(x_head[:, :half], first.astype(bf16), TT, preferred_element_type=f32),
                    lax.dot_general(x_head, second.astype(bf16), TT, preferred_element_type=f32),
                ],
                axis=1,
            )
            out_ref[channels, span] = (
                within + across[channels] * factor[h : h + 1] + skip_ref[h] * x_head.astype(f32)
            )


def ring_place():
    head_index = lax.axis_index("head")
    core = lax.axis_index("batch")
    y, x = head_index // RING, head_index % RING
    return core, jnp.where(core == 0, x, y), jnp.where(core == 0, y, x)


def head_at(core, u, v):
    return jnp.where(core == 0, v * RING + u, u * RING + v)


def gate_kernel(out_ref, gate_ref, c_ref, factor_ref, *refs):
    totals, results = refs[:-RING], refs[-RING:]
    channels = out_ref.shape[0]
    heads = channels // HEAD_DIM
    incoming = jnp.zeros((channels, STATE), f32)
    log_sum = jnp.zeros((PAD, STATE), f32)
    for total in totals:
        incoming = incoming + per_head(jnp.exp(log_sum), heads, STATE) * total[0:channels, :].astype(f32)
        log_sum = log_sum + join3(total[channels:, :], PAD)
    incoming = incoming.astype(bf16)
    core, u, v = ring_place()
    for su in range(RING):
        for sv in range(RING):
            place = head_at(core, (u + su) % RING, (v + sv) % RING)
            span = pl.ds(pl.multiple_of(place * SUB, SUB), SUB)
            across = lax.dot_general(incoming, c_ref[span, :], TT, preferred_element_type=f32)
            factor = factor_ref[:, span]
            for h in range(heads):
                rows = slice(h * HEAD_DIM, (h + 1) * HEAD_DIM)
                gate = gate_ref[rows, span].astype(f32)
                output = out_ref[rows, span] + across[rows] * factor[h : h + 1]
                gated = output * (gate / (1.0 + jnp.exp(-gate)))
                results[su][rows, sv * SUB : (sv + 1) * SUB] = gated.astype(bf16)


def gain_row(gain_ref, head, channels):
    first = head * channels
    lines = gain_ref[pl.ds(first // SUB, 3), :]
    line = jnp.concatenate([lines[i : i + 1] for i in range(3)], axis=1)
    shifted = jnp.concatenate([line[:, SUB // 2 :], line[:, : SUB // 2]], axis=1)
    return jnp.where(first % SUB == 0, line, shifted)[:, :channels]


def left_side(gain_ref, rows, blocks):
    core, u, v = ring_place()
    channels = rows[0].shape[0]
    pick = [slice(k * SUB, (k + 1) * SUB) for k in blocks]
    values = jnp.concatenate([jnp.concatenate([r[:, span] for span in pick], axis=1) for r in rows], axis=0)
    wide = values.astype(f32)
    squares = jnp.sum(wide * wide, axis=0, keepdims=True)
    gains = jnp.concatenate(
        [gain_row(gain_ref, head_at(core, (u - s + RING) % RING, v), channels) for s in range(RING)], axis=1
    )
    return (values.T.astype(f32) * gains).astype(bf16), squares


def tail_rows(squares, width):
    parts = [part.astype(f32) for part in split3(squares)]
    tail = jnp.concatenate(parts + [jnp.zeros((EXTRA - 3, SUB), f32)], axis=0)
    return jnp.concatenate([tail] * (width // SUB), axis=1).astype(bf16)


def tail_squares(part):
    return jnp.sum(part[SUB:, 0:SUB].astype(f32), axis=0, keepdims=True)


def opposite_kernel(gain_ref, *refs):
    rows, weights = refs[:RING], refs[RING:-3]
    first_ref, second_ref, left = refs[-3:]
    half = first_ref.shape[1]
    left[...], squares = left_side(gain_ref, rows, (2,))
    first_ref[SUB:, :] = tail_rows(squares, half)
    tile = 256
    for n in range(2 * half // tile):
        right = jnp.concatenate([w[:, n * tile : (n + 1) * tile] for w in weights], axis=0)
        product = jnp.dot(left[...], right, preferred_element_type=f32).astype(bf16)
        if n * tile < half:
            first_ref[0:SUB, n * tile : (n + 1) * tile] = product
        else:
            second_ref[:, n * tile - half : (n + 1) * tile - half] = product


def project_kernel(gain_ref, *refs):
    rows, weights = refs[:RING], refs[RING:-7]
    next_first, next_second, last_first, last_second, own_ref, own_squares, left = refs[-7:]
    half = next_first.shape[1]
    left[...], squares = left_side(gain_ref, rows, (1, 3, 0))
    next_first[SUB:, :] = tail_rows(squares[:, 0:SUB], half)
    last_first[SUB:, :] = tail_rows(squares[:, SUB : 2 * SUB], half)
    own_squares[...] = jnp.broadcast_to(squares[:, 2 * SUB :], own_squares.shape)
    tile = 256
    for n in range(2 * half // tile):
        span = slice(n * tile, (n + 1) * tile)
        right = jnp.concatenate([w[:, span] for w in weights], axis=0)
        product = jnp.dot(left[...], right, preferred_element_type=f32)
        own_ref[:, span] = product[2 * SUB :]
        if n * tile < half:
            next_first[0:SUB, span] = product[0:SUB].astype(bf16)
            last_first[0:SUB, span] = product[SUB : 2 * SUB].astype(bf16)
        else:
            span = slice(n * tile - half, (n + 1) * tile - half)
            next_second[:, span] = product[0:SUB].astype(bf16)
            last_second[:, span] = product[SUB : 2 * SUB].astype(bf16)


def merge_kernel(next_first, last_second, got_first, got_second, next_ref, last_ref):
    next_ref[0:SUB, :] = (next_first[0:SUB, :].astype(f32) + got_first[0:SUB, :].astype(f32)).astype(bf16)
    squares = tail_squares(next_first) + tail_squares(got_first)
    next_ref[SUB:, :] = tail_rows(squares, next_ref.shape[1])
    last_ref[...] = (last_second[...].astype(f32) + got_second[...].astype(f32)).astype(bf16)


def finish_kernel(channels, own_ref, own_squares, next_first, next_second, last_first, last_second, out_ref):
    half = next_first.shape[1]
    squares = own_squares[0:1, :] + tail_squares(next_first) + tail_squares(last_first)
    scale = lax.rsqrt(squares / channels + epsilon)
    column = jnp.broadcast_to(scale, (SUB, SUB)).T[:, 0:1]
    first = own_ref[:, :half] + next_first[0:SUB, :].astype(f32) + last_first[0:SUB, :].astype(f32)
    second = own_ref[:, half:] + next_second[...].astype(f32) + last_second[...].astype(f32)
    out_ref[:, :half] = (first * column).astype(bf16)
    out_ref[:, half:] = (second * column).astype(bf16)


def ring_pairs(shift, gather):
    pairs = []
    for y in range(RING):
        for x in range(RING):
            for core in range(2):
                if (core == 0) == gather:
                    there = y * RING + (x + shift) % RING
                else:
                    there = ((y + shift) % RING) * RING + x
                pairs.append(((y * RING + x) * 2 + core, there * 2 + core))
    return pairs


def ring(value, shift, gather):
    return lax.ppermute(value, ("head", "batch"), ring_pairs(shift, gather))


def body(
    ssm_input, gate_input, b_proj, c_proj, step_size, log_decay, skip_gain, norm_gain, out_weight
):
    tokens, channels = ssm_input.shape
    width = out_weight.shape[1]
    blocks = tokens // BLOCK
    seq_count = lax.axis_size("seq")
    core, u, v = ring_place()
    following = RING - 1
    weight_before, weight_after = ring(out_weight, 1, True), ring(out_weight, following, True)

    params = pltpu.CompilerParams(vmem_limit_bytes=24 * 1024 * 1024)
    near = pl.BlockSpec(memory_space=pltpu.VMEM)

    def hold(*values):
        return [pltpu.with_memory_space_constraint(value, pltpu.VMEM) for value in values]

    def far(value):
        return pltpu.with_memory_space_constraint(value, pltpu.HBM)

    payload = channels + 3 * PAD
    ssm_columns, gate_columns = ssm_input.T, gate_input.T
    prefix, total, cum, factor, b_own, c_own = pl.pallas_call(
        state_kernel,
        in_specs=[near, pl.BlockSpec(memory_space=pltpu.HBM), pl.BlockSpec(memory_space=pltpu.HBM), near, near],
        out_specs=[near] * 6,
        out_shape=[
            pltpu.VMEM((blocks, channels, STATE), bf16),
            pltpu.VMEM((payload, STATE), bf16),
            pltpu.VMEM((PAD, tokens), f32),
            pltpu.VMEM((PAD, tokens), f32),
            pltpu.VMEM((tokens, STATE), bf16),
            pltpu.VMEM((tokens, STATE), bf16),
        ],
        scratch_shapes=[pltpu.SemaphoreType.DMA((2,))],
        compiler_params=params,
        name="state",
    )(*hold(ssm_columns), far(b_proj), far(c_proj), *hold(step_size, log_decay))

    totals = [
        lax.ppermute(total, "seq", [(k, k + s) for k in range(seq_count - s)]) for s in range(1, seq_count)
    ]

    local = pl.pallas_call(
        within_kernel,
        in_specs=[pl.BlockSpec(memory_space=pltpu.SMEM)] + [near] * 6,
        out_specs=near,
        out_shape=pltpu.VMEM((channels, tokens), f32),
        compiler_params=params,
        name="within",
    )(skip_gain, *hold(ssm_columns, b_own, c_own, cum, step_size, prefix))

    local, weight_before, weight_after = lax.optimization_barrier((local, weight_before, weight_after))
    middle = channels // 2
    upper, lower = weight_before[:middle], weight_after[middle:]
    upper, lower = ring(upper, 1, True), ring(lower, following, True)
    weights = [out_weight, weight_before, upper, lower, weight_after]

    quarter = tokens // RING
    gated = pl.pallas_call(
        gate_kernel,
        in_specs=[near] * (4 + seq_count - 1),
        out_specs=[near] * RING,
        out_shape=[pltpu.VMEM((channels, quarter), bf16)] * RING,
        compiler_params=params,
        name="gate",
    )(*hold(local, gate_columns, c_own, factor, *totals))

    rows = [gated[0]] + [ring(gated[s], s, True) for s in range(1, RING)]

    half = width // 2
    with_tail, without = pltpu.VMEM((SUB + EXTRA, half), bf16), pltpu.VMEM((SUB, half), bf16)
    operands = hold(norm_gain.reshape(-1, SUB), *rows, *weights)
    opposite_first, opposite_second = pl.pallas_call(
        opposite_kernel,
        in_specs=[near] * len(operands),
        out_specs=[near] * 2,
        scratch_shapes=[pltpu.VMEM((SUB, RING * channels), bf16)],
        out_shape=[with_tail, without],
        compiler_params=params,
        name="opposite",
    )(*operands)
    got_first = ring(opposite_first, 1, False)
    got_second = ring(opposite_second, following, False)
    next_first, next_second, last_first, last_second, own, own_squares = pl.pallas_call(
        project_kernel,
        in_specs=[near] * len(operands),
        out_specs=[near] * 6,
        scratch_shapes=[pltpu.VMEM((3 * SUB, RING * channels), bf16)],
        out_shape=[with_tail, without, with_tail, without, pltpu.VMEM((SUB, width), f32), pltpu.VMEM((PAD, SUB), f32)],
        compiler_params=params,
        name="project",
    )(*operands)
    sent_second = ring(next_second, 1, False)
    sent_first = ring(last_first, following, False)
    next_sum, last_sum = pl.pallas_call(
        merge_kernel,
        in_specs=[near] * 4,
        out_specs=[near] * 2,
        out_shape=[with_tail, without],
        compiler_params=params,
        name="merge",
    )(*hold(next_first, last_second, got_first, got_second))
    from_before = ring(next_sum, 1, False)
    from_after = ring(last_sum, following, False)

    return pl.pallas_call(
        lambda *refs: finish_kernel(HEAD_COUNT * HEAD_DIM, *refs),
        in_specs=[near] * 6,
        out_specs=pl.BlockSpec((SUB, width), lambda: (0, 0)),
        out_shape=jax.ShapeDtypeStruct((SUB, width), bf16),
        compiler_params=params,
        name="finish",
    )(*hold(own, own_squares, from_before, sent_second, sent_first, from_after))


def solution(mesh):
    in_specs = (
        P(("batch", "seq"), "head"),
        P(("batch", "seq"), "head"),
        P(("batch", "seq"), None),
        P(("batch", "seq"), None),
        P("head", ("batch", "seq")),
        P("head", ("batch", "seq")),
        P("head"),
        P(),
        P("head", None),
    )
    out_specs = P(("batch", "seq", "head"), None)

    return jax.shard_map(body, mesh=mesh, in_specs=in_specs, out_specs=out_specs, check_vma=False)
```

```python
import jax
import jax.numpy as jnp
from jax import lax
from jax.experimental import pallas as pl
from jax.experimental.pallas import tpu as pltpu
from jax.sharding import PartitionSpec as P


HEAD_COUNT = 80
HEAD_DIM = 64
STATE = 128
GROUPS = 8
BLOCK = 256
RING = 4
SUB = 128
EXTRA = 8
PAD = 8

epsilon = 1e-05


f32 = jnp.float32
bf16 = jnp.bfloat16
TT = (((1,), (1,)), ((), ()))


def triangle(size, dtype):
    rows = lax.broadcasted_iota(jnp.int32, (size, size), 0)
    columns = lax.broadcasted_iota(jnp.int32, (size, size), 1)
    return (rows <= columns).astype(dtype)


def split3(value):
    high = value.astype(bf16)
    rest = value - high.astype(f32)
    middle = rest.astype(bf16)
    return high, middle, (rest - middle.astype(f32)).astype(bf16)


def join3(stacked, rows):
    return stacked[0:rows].astype(f32) + stacked[rows : 2 * rows].astype(f32) + stacked[2 * rows : 3 * rows].astype(f32)


def per_head(column, heads, lanes):
    return jnp.concatenate(
        [jnp.broadcast_to(column[h : h + 1, 0:1], (HEAD_DIM, lanes)) for h in range(heads)], axis=0
    )


def state_kernel(
    x_hbm, b_hbm, c_hbm, step_hbm, decay_hbm, prefix_ref, total_ref, cum_ref, factor_ref, x_ref, b_ref, c_ref, step_ref, decay_ref, sems
):
    heads, tokens = step_ref.shape
    blocks = tokens // BLOCK
    group = lax.axis_index("head") * heads * GROUPS // HEAD_COUNT
    columns = pl.ds(pl.multiple_of(group * STATE, STATE), STATE)
    sources = (decay_hbm, step_hbm, x_hbm, b_hbm.at[:, columns], c_hbm.at[:, columns])
    targets = (decay_ref, step_ref, x_ref, b_ref, c_ref)
    fetches = [pltpu.make_async_copy(sources[k], targets[k], sems.at[k]) for k in range(5)]
    for fetch in fetches:
        fetch.start()
    fetches[0].wait()
    fill = jnp.zeros((PAD - heads, BLOCK), f32)
    decay = jnp.concatenate(
        [piece for c in range(blocks) for piece in (decay_ref[:, c * BLOCK : (c + 1) * BLOCK], fill)], axis=0
    )
    sums = jnp.dot(
        jnp.concatenate(split3(decay), axis=0), triangle(BLOCK, bf16), preferred_element_type=f32
    )
    sums = join3(sums, blocks * PAD)
    offset = jnp.zeros((PAD, 1), f32)
    for c in range(blocks):
        span = slice(c * BLOCK, (c + 1) * BLOCK)
        cumulative = sums[c * PAD : (c + 1) * PAD]
        cum_ref[:, span] = cumulative
        factor_ref[:, span] = jnp.exp(cumulative + offset)
        offset = offset + cumulative[:, BLOCK - 1 :]
    for fetch in fetches[1:4]:
        fetch.wait()
    state = jnp.zeros((heads * HEAD_DIM, STATE), f32)
    for c in range(blocks):
        span = slice(c * BLOCK, (c + 1) * BLOCK)
        cumulative = sums[c * PAD : (c + 1) * PAD]
        end = cumulative[:, BLOCK - 1 :]
        prefix_ref[c] = state.astype(bf16)
        to_end = jnp.exp(end - cumulative)[0:heads] * step_ref[:, span]
        scaled = jnp.concatenate(
            [
                (x_ref[h * HEAD_DIM : (h + 1) * HEAD_DIM, span].astype(f32) * to_end[h : h + 1]).astype(bf16)
                for h in range(heads)
            ],
            axis=0,
        )
        block_state = jnp.dot(scaled, b_ref[span, :], preferred_element_type=f32)
        state = per_head(jnp.exp(end), heads, STATE) * state + block_state
    total_ref[0 : heads * HEAD_DIM, :] = state.astype(bf16)
    parts = split3(jnp.broadcast_to(offset, (PAD, STATE)))
    total_ref[heads * HEAD_DIM :, :] = jnp.concatenate(parts, axis=0)
    fetches[4].wait()


def pair_kernel(total_ref, before_ref, pair_ref):
    channels = total_ref.shape[0] - 3 * PAD
    heads = channels // HEAD_DIM
    logs = join3(total_ref[channels:, :], PAD)
    decayed = per_head(jnp.exp(logs), heads, STATE) * before_ref[0:channels, :].astype(f32)
    pair_ref[0:channels, :] = (total_ref[0:channels, :].astype(f32) + decayed).astype(bf16)
    pair_ref[channels:, :] = jnp.concatenate(split3(logs + join3(before_ref[channels:, :], PAD)), axis=0)


def within_kernel(first_head, last_head, skip_ref, x_ref, b_ref, c_ref, cum_ref, step_ref, prefix_ref, out_ref):
    half = BLOCK // 2
    chosen = slice(first_head * HEAD_DIM, last_head * HEAD_DIM)
    causal = triangle(half, f32).T > 0
    for k in range(step_ref.shape[1] // BLOCK):
        span = slice(k * BLOCK, (k + 1) * BLOCK)
        c_block = c_ref[span, :]
        b_block = b_ref[span, :]
        scores_first = lax.dot_general(c_block[:half], b_block[:half], TT, preferred_element_type=f32)
        scores_second = lax.dot_general(c_block[half:], b_block, TT, preferred_element_type=f32)
        across = lax.dot_general(prefix_ref[k, chosen], c_block, TT, preferred_element_type=f32)
        cumulative = cum_ref[:, span]
        factor = jnp.exp(cumulative)
        columns = cumulative.T
        for h in range(first_head, last_head):
            channels = slice((h - first_head) * HEAD_DIM, (h - first_head + 1) * HEAD_DIM)
            x_head = x_ref[h * HEAD_DIM : (h + 1) * HEAD_DIM, span]
            row = cumulative[h : h + 1]
            step = step_ref[h : h + 1, span]
            differ = columns[:half, h : h + 1] - row[:, :half]
            first = scores_first * jnp.exp(jnp.where(causal, differ, -jnp.inf)) * step[:, :half]
            column = columns[half:, h : h + 1]
            full = scores_second[:, :half] * jnp.exp(column - row[:, :half]) * step[:, :half]
            differ = column - row[:, half:]
            last = scores_second[:, half:] * jnp.exp(jnp.where(causal, differ, -jnp.inf)) * step[:, half:]
            second = jnp.concatenate([full, last], axis=1)
            within = jnp.concatenate(
                [
                    lax.dot_general(x_head[:, :half], first.astype(bf16), TT, preferred_element_type=f32),
                    lax.dot_general(x_head, second.astype(bf16), TT, preferred_element_type=f32),
                ],
                axis=1,
            )
            out_ref[channels, span] = (
                within + across[channels] * factor[h : h + 1] + skip_ref[h] * x_head.astype(f32)
            )


def ring_place():
    head_index = lax.axis_index("head")
    core = lax.axis_index("batch")
    y, x = head_index // RING, head_index % RING
    return core, jnp.where(core == 0, x, y), jnp.where(core == 0, y, x)


def head_at(core, u, v):
    return jnp.where(core == 0, v * RING + u, u * RING + v)


def gate_kernel(out_first, out_last, gate_ref, c_ref, factor_ref, *refs):
    totals, results = refs[:-RING], refs[-RING:]
    channels = gate_ref.shape[0]
    heads = channels // HEAD_DIM
    split = out_first.shape[0]
    incoming = jnp.zeros((channels, STATE), f32)
    log_sum = jnp.zeros((PAD, STATE), f32)
    for total in totals:
        incoming = incoming + per_head(jnp.exp(log_sum), heads, STATE) * total[0:channels, :].astype(f32)
        log_sum = log_sum + join3(total[channels:, :], PAD)
    incoming = incoming.astype(bf16)
    core, u, v = ring_place()
    for su in range(RING):
        for sv in range(RING):
            place = head_at(core, (u + su) % RING, (v + sv) % RING)
            span = pl.ds(pl.multiple_of(place * SUB, SUB), SUB)
            across = lax.dot_general(incoming, c_ref[span, :], TT, preferred_element_type=f32)
            factor = factor_ref[:, span]
            for h in range(heads):
                rows = slice(h * HEAD_DIM, (h + 1) * HEAD_DIM)
                gate = gate_ref[rows, span].astype(f32)
                if rows.start < split:
                    local = out_first[rows, span]
                else:
                    local = out_last[rows.start - split : rows.stop - split, span]
                output = local + across[rows] * factor[h : h + 1]
                gated = output * (gate / (1.0 + jnp.exp(-gate)))
                results[su][rows, sv * SUB : (sv + 1) * SUB] = gated.astype(bf16)


def gain_row(gain_ref, head, channels):
    first = head * channels
    lines = gain_ref[pl.ds(first // SUB, 3), :]
    line = jnp.concatenate([lines[i : i + 1] for i in range(3)], axis=1)
    shifted = jnp.concatenate([line[:, SUB // 2 :], line[:, : SUB // 2]], axis=1)
    return jnp.where(first % SUB == 0, line, shifted)[:, :channels]


def left_side(gain_ref, rows, blocks):
    core, u, v = ring_place()
    channels = rows[0].shape[0]
    pick = [slice(k * SUB, (k + 1) * SUB) for k in blocks]
    values = jnp.concatenate([jnp.concatenate([r[:, span] for span in pick], axis=1) for r in rows], axis=0)
    wide = values.astype(f32)
    squares = jnp.sum(wide * wide, axis=0, keepdims=True)
    gains = jnp.concatenate(
        [gain_row(gain_ref, head_at(core, (u - s + RING) % RING, v), channels) for s in range(RING)], axis=1
    )
    return (values.T.astype(f32) * gains).astype(bf16), squares


def tail_rows(squares, width):
    parts = [part.astype(f32) for part in split3(squares)]
    tail = jnp.concatenate(parts + [jnp.zeros((EXTRA - 3, SUB), f32)], axis=0)
    return jnp.concatenate([tail] * (width // SUB), axis=1).astype(bf16)


def tail_squares(part):
    return jnp.sum(part[SUB:, 0:SUB].astype(f32), axis=0, keepdims=True)


def opposite_kernel(gain_ref, *refs):
    rows, weights = refs[:RING], refs[RING:-3]
    first_ref, second_ref, left = refs[-3:]
    half = first_ref.shape[1]
    left[...], squares = left_side(gain_ref, rows, (2,))
    first_ref[SUB:, :] = tail_rows(squares, half)
    tile = 256
    for n in range(2 * half // tile):
        right = jnp.concatenate([w[:, n * tile : (n + 1) * tile] for w in weights], axis=0)
        product = jnp.dot(left[...], right, preferred_element_type=f32).astype(bf16)
        if n * tile < half:
            first_ref[0:SUB, n * tile : (n + 1) * tile] = product
        else:
            second_ref[:, n * tile - half : (n + 1) * tile - half] = product


def project_kernel(gain_ref, *refs):
    rows, weights = refs[:RING], refs[RING:-7]
    next_first, next_second, last_first, last_second, own_ref, own_squares, left = refs[-7:]
    half = next_first.shape[1]
    left[...], squares = left_side(gain_ref, rows, (1, 3, 0))
    next_first[SUB:, :] = tail_rows(squares[:, 0:SUB], half)
    last_first[SUB:, :] = tail_rows(squares[:, SUB : 2 * SUB], half)
    own_squares[...] = jnp.broadcast_to(squares[:, 2 * SUB :], own_squares.shape)
    tile = 256
    for n in range(2 * half // tile):
        span = slice(n * tile, (n + 1) * tile)
        right = jnp.concatenate([w[:, span] for w in weights], axis=0)
        product = jnp.dot(left[...], right, preferred_element_type=f32)
        own_ref[:, span] = product[2 * SUB :]
        if n * tile < half:
            next_first[0:SUB, span] = product[0:SUB].astype(bf16)
            last_first[0:SUB, span] = product[SUB : 2 * SUB].astype(bf16)
        else:
            span = slice(n * tile - half, (n + 1) * tile - half)
            next_second[:, span] = product[0:SUB].astype(bf16)
            last_second[:, span] = product[SUB : 2 * SUB].astype(bf16)


def merge_kernel(next_first, last_second, got_first, got_second, next_ref, last_ref):
    next_ref[0:SUB, :] = (next_first[0:SUB, :].astype(f32) + got_first[0:SUB, :].astype(f32)).astype(bf16)
    squares = tail_squares(next_first) + tail_squares(got_first)
    next_ref[SUB:, :] = tail_rows(squares, next_ref.shape[1])
    last_ref[...] = (last_second[...].astype(f32) + got_second[...].astype(f32)).astype(bf16)


def finish_kernel(channels, own_ref, own_squares, next_first, next_second, last_first, last_second, out_ref):
    half = next_first.shape[1]
    squares = own_squares[0:1, :] + tail_squares(next_first) + tail_squares(last_first)
    scale = lax.rsqrt(squares / channels + epsilon)
    column = jnp.broadcast_to(scale, (SUB, SUB)).T[:, 0:1]
    first = own_ref[:, :half] + next_first[0:SUB, :].astype(f32) + last_first[0:SUB, :].astype(f32)
    second = own_ref[:, half:] + next_second[...].astype(f32) + last_second[...].astype(f32)
    out_ref[:, :half] = (first * column).astype(bf16)
    out_ref[:, half:] = (second * column).astype(bf16)


def ring_pairs(shift, gather):
    pairs = []
    for y in range(RING):
        for x in range(RING):
            for core in range(2):
                if (core == 0) == gather:
                    there = y * RING + (x + shift) % RING
                else:
                    there = ((y + shift) % RING) * RING + x
                pairs.append(((y * RING + x) * 2 + core, there * 2 + core))
    return pairs


def ring(value, shift, gather):
    return lax.ppermute(value, ("head", "batch"), ring_pairs(shift, gather))


def body(
    ssm_input, gate_input, b_proj, c_proj, step_size, log_decay, skip_gain, norm_gain, out_weight
):
    tokens, channels = ssm_input.shape
    heads = step_size.shape[0]
    width = out_weight.shape[1]
    blocks = tokens // BLOCK
    seq_count = lax.axis_size("seq")
    core, u, v = ring_place()
    following = RING - 1
    weight_before, weight_after = ring(out_weight, 1, True), ring(out_weight, following, True)

    params = pltpu.CompilerParams(vmem_limit_bytes=24 * 1024 * 1024)
    near = pl.BlockSpec(memory_space=pltpu.VMEM)

    def hold(*values):
        return [pltpu.with_memory_space_constraint(value, pltpu.VMEM) for value in values]

    def far(value):
        return pltpu.with_memory_space_constraint(value, pltpu.HBM)

    payload = channels + 3 * PAD
    ssm_columns, gate_columns = ssm_input.T, gate_input.T
    prefix, total, cum, factor, x_own, b_own, c_own, step_own = pl.pallas_call(
        state_kernel,
        in_specs=[pl.BlockSpec(memory_space=pltpu.HBM)] * 5,
        out_specs=[near] * 8,
        out_shape=[
            pltpu.VMEM((blocks, channels, STATE), bf16),
            pltpu.VMEM((payload, STATE), bf16),
            pltpu.VMEM((PAD, tokens), f32),
            pltpu.VMEM((PAD, tokens), f32),
            pltpu.VMEM((channels, tokens), bf16),
            pltpu.VMEM((tokens, STATE), bf16),
            pltpu.VMEM((tokens, STATE), bf16),
            pltpu.VMEM((heads, tokens), f32),
        ],
        scratch_shapes=[pltpu.VMEM((heads, tokens), f32), pltpu.SemaphoreType.DMA((5,))],
        compiler_params=params,
        name="state",
    )(*[far(value) for value in (ssm_columns, b_proj, c_proj, step_size, log_decay)])

    def along(value, shift):
        return lax.ppermute(value, "seq", [(k, k + shift) for k in range(seq_count - shift)])

    def within(first_head, last_head):
        return pl.pallas_call(
            lambda *refs: within_kernel(first_head, last_head, *refs),
            in_specs=[pl.BlockSpec(memory_space=pltpu.SMEM)] + [near] * 6,
            out_specs=near,
            out_shape=pltpu.VMEM(((last_head - first_head) * HEAD_DIM, tokens), f32),
            compiler_params=params,
        )(skip_gain, *hold(x_own, b_own, c_own, cum, step_own, prefix))

    split = heads // 2 + 1
    before = along(total, 1)
    local_first = within(0, split)
    before, local_first = lax.optimization_barrier((before, local_first))
    pair = pl.pallas_call(
        pair_kernel,
        in_specs=[near] * 2,
        out_specs=near,
        out_shape=pltpu.VMEM((payload, STATE), bf16),
        compiler_params=params,
        name="pair",
    )(*hold(total, before))
    totals = [along(pair, shift) for shift in range(1, seq_count, 2)]
    local_last = within(split, heads)

    local_last, weight_before, weight_after = lax.optimization_barrier((local_last, weight_before, weight_after))
    middle = channels // 2
    upper, lower = weight_before[:middle], weight_after[middle:]
    upper, lower = ring(upper, 1, True), ring(lower, following, True)
    weights = [out_weight, weight_before, upper, lower, weight_after]

    quarter = tokens // RING
    gated = pl.pallas_call(
        gate_kernel,
        in_specs=[near] * (5 + len(totals)),
        out_specs=[near] * RING,
        out_shape=[pltpu.VMEM((channels, quarter), bf16)] * RING,
        compiler_params=params,
        name="gate",
    )(*hold(local_first, local_last, gate_columns, c_own, factor, *totals))

    rows = [gated[0]] + [ring(gated[s], s, True) for s in range(1, RING)]

    half = width // 2
    with_tail, without = pltpu.VMEM((SUB + EXTRA, half), bf16), pltpu.VMEM((SUB, half), bf16)
    operands = hold(norm_gain.reshape(-1, SUB), *rows, *weights)
    opposite_first, opposite_second = pl.pallas_call(
        opposite_kernel,
        in_specs=[near] * len(operands),
        out_specs=[near] * 2,
        scratch_shapes=[pltpu.VMEM((SUB, RING * channels), bf16)],
        out_shape=[with_tail, without],
        compiler_params=params,
        name="opposite",
    )(*operands)
    got_first = ring(opposite_first, 1, False)
    got_second = ring(opposite_second, following, False)
    next_first, next_second, last_first, last_second, own, own_squares = pl.pallas_call(
        project_kernel,
        in_specs=[near] * len(operands),
        out_specs=[near] * 6,
        scratch_shapes=[pltpu.VMEM((3 * SUB, RING * channels), bf16)],
        out_shape=[with_tail, without, with_tail, without, pltpu.VMEM((SUB, width), f32), pltpu.VMEM((PAD, SUB), f32)],
        compiler_params=params,
        name="project",
    )(*operands)
    sent_second = ring(next_second, 1, False)
    sent_first = ring(last_first, following, False)
    next_sum, last_sum = pl.pallas_call(
        merge_kernel,
        in_specs=[near] * 4,
        out_specs=[near] * 2,
        out_shape=[with_tail, without],
        compiler_params=params,
        name="merge",
    )(*hold(next_first, last_second, got_first, got_second))
    from_before = ring(next_sum, 1, False)
    from_after = ring(last_sum, following, False)

    return pl.pallas_call(
        lambda *refs: finish_kernel(HEAD_COUNT * HEAD_DIM, *refs),
        in_specs=[near] * 6,
        out_specs=pl.BlockSpec((SUB, width), lambda: (0, 0)),
        out_shape=jax.ShapeDtypeStruct((SUB, width), bf16),
        compiler_params=params,
        name="finish",
    )(*hold(own, own_squares, from_before, sent_second, sent_first, from_after))


def solution(mesh):
    in_specs = (
        P(("batch", "seq"), "head"),
        P(("batch", "seq"), "head"),
        P(("batch", "seq"), None),
        P(("batch", "seq"), None),
        P("head", ("batch", "seq")),
        P("head", ("batch", "seq")),
        P("head"),
        P(),
        P("head", None),
    )
    out_specs = P(("batch", "seq", "head"), None)

    return jax.shard_map(body, mesh=mesh, in_specs=in_specs, out_specs=out_specs, check_vma=False)
```

```python
import jax
import jax.numpy as jnp
from jax import lax
from jax.experimental import pallas as pl
from jax.experimental.pallas import tpu as pltpu
from jax.sharding import PartitionSpec as P


HEAD_COUNT = 80
HEAD_DIM = 64
STATE = 128
GROUPS = 8
BLOCK = 256
RING = 4
SUB = 128
EXTRA = 8
PAD = 8

epsilon = 1e-05


f32 = jnp.float32
bf16 = jnp.bfloat16
TT = (((1,), (1,)), ((), ()))


def triangle(size, dtype):
    rows = lax.broadcasted_iota(jnp.int32, (size, size), 0)
    columns = lax.broadcasted_iota(jnp.int32, (size, size), 1)
    return (rows <= columns).astype(dtype)


def split3(value):
    high = value.astype(bf16)
    rest = value - high.astype(f32)
    middle = rest.astype(bf16)
    return high, middle, (rest - middle.astype(f32)).astype(bf16)


def join3(stacked, rows):
    return stacked[0:rows].astype(f32) + stacked[rows : 2 * rows].astype(f32) + stacked[2 * rows : 3 * rows].astype(f32)


def per_head(column, heads, lanes):
    return jnp.concatenate(
        [jnp.broadcast_to(column[h : h + 1, 0:1], (HEAD_DIM, lanes)) for h in range(heads)], axis=0
    )


def state_kernel(
    x_hbm, b_hbm, c_hbm, step_hbm, decay_hbm, prefix_ref, total_ref, cum_ref, factor_ref, x_ref, b_ref, c_ref, step_ref, decay_ref, sems
):
    heads, tokens = step_ref.shape
    blocks = tokens // BLOCK
    group = lax.axis_index("head") * heads * GROUPS // HEAD_COUNT
    columns = pl.ds(pl.multiple_of(group * STATE, STATE), STATE)
    sources = (decay_hbm, step_hbm, x_hbm, b_hbm.at[:, columns], c_hbm.at[:, columns])
    targets = (decay_ref, step_ref, x_ref, b_ref, c_ref)
    fetches = [pltpu.make_async_copy(sources[k], targets[k], sems.at[k]) for k in range(5)]
    for fetch in fetches:
        fetch.start()
    fetches[0].wait()
    fill = jnp.zeros((PAD - heads, BLOCK), f32)
    decay = jnp.concatenate(
        [piece for c in range(blocks) for piece in (decay_ref[:, c * BLOCK : (c + 1) * BLOCK], fill)], axis=0
    )
    sums = jnp.dot(
        jnp.concatenate(split3(decay), axis=0), triangle(BLOCK, bf16), preferred_element_type=f32
    )
    sums = join3(sums, blocks * PAD)
    offset = jnp.zeros((PAD, 1), f32)
    for c in range(blocks):
        span = slice(c * BLOCK, (c + 1) * BLOCK)
        cumulative = sums[c * PAD : (c + 1) * PAD]
        cum_ref[:, span] = cumulative
        factor_ref[:, span] = jnp.exp(cumulative + offset)
        offset = offset + cumulative[:, BLOCK - 1 :]
    for fetch in fetches[1:4]:
        fetch.wait()
    state = jnp.zeros((heads * HEAD_DIM, STATE), f32)
    for c in range(blocks):
        span = slice(c * BLOCK, (c + 1) * BLOCK)
        cumulative = sums[c * PAD : (c + 1) * PAD]
        end = cumulative[:, BLOCK - 1 :]
        prefix_ref[c] = state.astype(bf16)
        to_end = jnp.exp(end - cumulative)[0:heads] * step_ref[:, span]
        scaled = jnp.concatenate(
            [
                (x_ref[h * HEAD_DIM : (h + 1) * HEAD_DIM, span].astype(f32) * to_end[h : h + 1]).astype(bf16)
                for h in range(heads)
            ],
            axis=0,
        )
        block_state = jnp.dot(scaled, b_ref[span, :], preferred_element_type=f32)
        state = per_head(jnp.exp(end), heads, STATE) * state + block_state
    total_ref[0 : heads * HEAD_DIM, :] = state.astype(bf16)
    parts = split3(jnp.broadcast_to(offset, (PAD, STATE)))
    total_ref[heads * HEAD_DIM :, :] = jnp.concatenate(parts, axis=0)
    fetches[4].wait()


def pair_kernel(total_ref, before_ref, pair_ref):
    channels = total_ref.shape[0] - 3 * PAD
    heads = channels // HEAD_DIM
    logs = join3(total_ref[channels:, :], PAD)
    decayed = per_head(jnp.exp(logs), heads, STATE) * before_ref[0:channels, :].astype(f32)
    pair_ref[0:channels, :] = (total_ref[0:channels, :].astype(f32) + decayed).astype(bf16)
    pair_ref[channels:, :] = jnp.concatenate(split3(logs + join3(before_ref[channels:, :], PAD)), axis=0)


def within_kernel(skip_ref, x_ref, b_ref, c_ref, cum_ref, step_ref, prefix_ref, out_ref):
    heads = step_ref.shape[0]
    half = BLOCK // 2
    causal = triangle(half, f32).T > 0
    for k in range(step_ref.shape[1] // BLOCK):
        span = slice(k * BLOCK, (k + 1) * BLOCK)
        c_block = c_ref[span, :]
        b_block = b_ref[span, :]
        scores_first = lax.dot_general(c_block[:half], b_block[:half], TT, preferred_element_type=f32)
        scores_second = lax.dot_general(c_block[half:], b_block, TT, preferred_element_type=f32)
        across = lax.dot_general(prefix_ref[k], c_block, TT, preferred_element_type=f32)
        cumulative = cum_ref[:, span]
        factor = jnp.exp(cumulative)
        columns = cumulative.T
        for h in range(heads):
            channels = slice(h * HEAD_DIM, (h + 1) * HEAD_DIM)
            x_head = x_ref[channels, span]
            row = cumulative[h : h + 1]
            step = step_ref[h : h + 1, span]
            differ = columns[:half, h : h + 1] - row[:, :half]
            first = scores_first * jnp.exp(jnp.where(causal, differ, -jnp.inf)) * step[:, :half]
            column = columns[half:, h : h + 1]
            full = scores_second[:, :half] * jnp.exp(column - row[:, :half]) * step[:, :half]
            differ = column - row[:, half:]
            last = scores_second[:, half:] * jnp.exp(jnp.where(causal, differ, -jnp.inf)) * step[:, half:]
            second = jnp.concatenate([full, last], axis=1)
            within = jnp.concatenate(
                [
                    lax.dot_general(x_head[:, :half], first.astype(bf16), TT, preferred_element_type=f32),
                    lax.dot_general(x_head, second.astype(bf16), TT, preferred_element_type=f32),
                ],
                axis=1,
            )
            out_ref[channels, span] = (
                within + across[channels] * factor[h : h + 1] + skip_ref[h] * x_head.astype(f32)
            )


def ring_place():
    head_index = lax.axis_index("head")
    core = lax.axis_index("batch")
    y, x = head_index // RING, head_index % RING
    return core, jnp.where(core == 0, x, y), jnp.where(core == 0, y, x)


def head_at(core, u, v):
    return jnp.where(core == 0, v * RING + u, u * RING + v)


def gate_kernel(out_ref, gate_ref, c_ref, factor_ref, *refs):
    totals, results = refs[:-RING], refs[-RING:]
    channels = gate_ref.shape[0]
    heads = channels // HEAD_DIM
    incoming = jnp.zeros((channels, STATE), f32)
    log_sum = jnp.zeros((PAD, STATE), f32)
    for total in totals:
        incoming = incoming + per_head(jnp.exp(log_sum), heads, STATE) * total[0:channels, :].astype(f32)
        log_sum = log_sum + join3(total[channels:, :], PAD)
    incoming = incoming.astype(bf16)
    core, u, v = ring_place()
    for su in range(RING):
        for sv in range(RING):
            place = head_at(core, (u + su) % RING, (v + sv) % RING)
            span = pl.ds(pl.multiple_of(place * SUB, SUB), SUB)
            across = lax.dot_general(incoming, c_ref[span, :], TT, preferred_element_type=f32)
            factor = factor_ref[:, span]
            for h in range(heads):
                rows = slice(h * HEAD_DIM, (h + 1) * HEAD_DIM)
                gate = gate_ref[rows, span].astype(f32)
                output = out_ref[rows, span] + across[rows] * factor[h : h + 1]
                gated = output * (gate / (1.0 + jnp.exp(-gate)))
                results[su][rows, sv * SUB : (sv + 1) * SUB] = gated.astype(bf16)


def gain_row(gain_ref, head, channels):
    first = head * channels
    lines = gain_ref[pl.ds(first // SUB, 3), :]
    line = jnp.concatenate([lines[i : i + 1] for i in range(3)], axis=1)
    shifted = jnp.concatenate([line[:, SUB // 2 :], line[:, : SUB // 2]], axis=1)
    return jnp.where(first % SUB == 0, line, shifted)[:, :channels]


def left_side(gain_ref, rows, blocks):
    core, u, v = ring_place()
    channels = rows[0].shape[0]
    pick = [slice(k * SUB, (k + 1) * SUB) for k in blocks]
    values = jnp.concatenate([jnp.concatenate([r[:, span] for span in pick], axis=1) for r in rows], axis=0)
    wide = values.astype(f32)
    squares = jnp.sum(wide * wide, axis=0, keepdims=True)
    gains = jnp.concatenate(
        [gain_row(gain_ref, head_at(core, (u - s + RING) % RING, v), channels) for s in range(RING)], axis=1
    )
    return (values.T.astype(f32) * gains).astype(bf16), squares


def tail_rows(squares, width):
    parts = [part.astype(f32) for part in split3(squares)]
    tail = jnp.concatenate(parts + [jnp.zeros((EXTRA - 3, SUB), f32)], axis=0)
    return jnp.concatenate([tail] * (width // SUB), axis=1).astype(bf16)


def tail_squares(part):
    return jnp.sum(part[SUB:, 0:SUB].astype(f32), axis=0, keepdims=True)


def opposite_kernel(gain_ref, *refs):
    rows, weights = refs[:RING], refs[RING:-3]
    first_ref, second_ref, left = refs[-3:]
    half = first_ref.shape[1]
    left[...], squares = left_side(gain_ref, rows, (2,))
    first_ref[SUB:, :] = tail_rows(squares, half)
    tile = 256
    for n in range(2 * half // tile):
        right = jnp.concatenate([w[:, n * tile : (n + 1) * tile] for w in weights], axis=0)
        product = jnp.dot(left[...], right, preferred_element_type=f32).astype(bf16)
        if n * tile < half:
            first_ref[0:SUB, n * tile : (n + 1) * tile] = product
        else:
            second_ref[:, n * tile - half : (n + 1) * tile - half] = product


def project_kernel(gain_ref, *refs):
    rows, weights = refs[:RING], refs[RING:-7]
    next_first, next_second, last_first, last_second, own_ref, own_squares, left = refs[-7:]
    half = next_first.shape[1]
    left[...], squares = left_side(gain_ref, rows, (1, 3, 0))
    next_first[SUB:, :] = tail_rows(squares[:, 0:SUB], half)
    last_first[SUB:, :] = tail_rows(squares[:, SUB : 2 * SUB], half)
    own_squares[...] = jnp.broadcast_to(squares[:, 2 * SUB :], own_squares.shape)
    tile = 256
    for n in range(2 * half // tile):
        span = slice(n * tile, (n + 1) * tile)
        right = jnp.concatenate([w[:, span] for w in weights], axis=0)
        product = jnp.dot(left[...], right, preferred_element_type=f32)
        own_ref[:, span] = product[2 * SUB :]
        if n * tile < half:
            next_first[0:SUB, span] = product[0:SUB].astype(bf16)
            last_first[0:SUB, span] = product[SUB : 2 * SUB].astype(bf16)
        else:
            span = slice(n * tile - half, (n + 1) * tile - half)
            next_second[:, span] = product[0:SUB].astype(bf16)
            last_second[:, span] = product[SUB : 2 * SUB].astype(bf16)


def merge_kernel(next_first, last_second, got_first, got_second, next_ref, last_ref):
    next_ref[0:SUB, :] = (next_first[0:SUB, :].astype(f32) + got_first[0:SUB, :].astype(f32)).astype(bf16)
    squares = tail_squares(next_first) + tail_squares(got_first)
    next_ref[SUB:, :] = tail_rows(squares, next_ref.shape[1])
    last_ref[...] = (last_second[...].astype(f32) + got_second[...].astype(f32)).astype(bf16)


def finish_kernel(channels, own_ref, own_squares, next_first, next_second, last_first, last_second, out_ref):
    half = next_first.shape[1]
    squares = own_squares[0:1, :] + tail_squares(next_first) + tail_squares(last_first)
    scale = lax.rsqrt(squares / channels + epsilon)
    column = jnp.broadcast_to(scale, (SUB, SUB)).T[:, 0:1]
    first = own_ref[:, :half] + next_first[0:SUB, :].astype(f32) + last_first[0:SUB, :].astype(f32)
    second = own_ref[:, half:] + next_second[...].astype(f32) + last_second[...].astype(f32)
    out_ref[:, :half] = (first * column).astype(bf16)
    out_ref[:, half:] = (second * column).astype(bf16)


def ring_pairs(shift, gather):
    pairs = []
    for y in range(RING):
        for x in range(RING):
            for core in range(2):
                if (core == 0) == gather:
                    there = y * RING + (x + shift) % RING
                else:
                    there = ((y + shift) % RING) * RING + x
                pairs.append(((y * RING + x) * 2 + core, there * 2 + core))
    return pairs


def ring(value, shift, gather):
    return lax.ppermute(value, ("head", "batch"), ring_pairs(shift, gather))


def body(
    ssm_input, gate_input, b_proj, c_proj, step_size, log_decay, skip_gain, norm_gain, out_weight
):
    tokens, channels = ssm_input.shape
    heads = step_size.shape[0]
    width = out_weight.shape[1]
    blocks = tokens // BLOCK
    seq_count = lax.axis_size("seq")
    core, u, v = ring_place()
    following = RING - 1
    weight_before, weight_after = ring(out_weight, 1, True), ring(out_weight, following, True)

    params = pltpu.CompilerParams(vmem_limit_bytes=24 * 1024 * 1024)
    near = pl.BlockSpec(memory_space=pltpu.VMEM)

    def hold(*values):
        return [pltpu.with_memory_space_constraint(value, pltpu.VMEM) for value in values]

    def far(value):
        return pltpu.with_memory_space_constraint(value, pltpu.HBM)

    payload = channels + 3 * PAD
    ssm_columns, gate_columns = ssm_input.T, gate_input.T
    prefix, total, cum, factor, x_own, b_own, c_own, step_own = pl.pallas_call(
        state_kernel,
        in_specs=[pl.BlockSpec(memory_space=pltpu.HBM)] * 5,
        out_specs=[near] * 8,
        out_shape=[
            pltpu.VMEM((blocks, channels, STATE), bf16),
            pltpu.VMEM((payload, STATE), bf16),
            pltpu.VMEM((PAD, tokens), f32),
            pltpu.VMEM((PAD, tokens), f32),
            pltpu.VMEM((channels, tokens), bf16),
            pltpu.VMEM((tokens, STATE), bf16),
            pltpu.VMEM((tokens, STATE), bf16),
            pltpu.VMEM((heads, tokens), f32),
        ],
        scratch_shapes=[pltpu.VMEM((heads, tokens), f32), pltpu.SemaphoreType.DMA((5,))],
        compiler_params=params,
        name="state",
    )(*[far(value) for value in (ssm_columns, b_proj, c_proj, step_size, log_decay)])

    def along(value, shift):
        return lax.ppermute(value, "seq", [(k, k + shift) for k in range(seq_count - shift)])

    before = along(total, 1)
    local = pl.pallas_call(
        within_kernel,
        in_specs=[pl.BlockSpec(memory_space=pltpu.SMEM)] + [near] * 6,
        out_specs=near,
        out_shape=pltpu.VMEM((channels, tokens), f32),
        compiler_params=params,
        name="within",
    )(skip_gain, *hold(x_own, b_own, c_own, cum, step_own, prefix))
    before, local = lax.optimization_barrier((before, local))
    pair = pl.pallas_call(
        pair_kernel,
        in_specs=[near] * 2,
        out_specs=near,
        out_shape=pltpu.VMEM((payload, STATE), bf16),
        compiler_params=params,
        name="pair",
    )(*hold(total, before))
    totals = [along(pair, shift) for shift in range(1, seq_count, 2)]

    weight_before, weight_after, pair = lax.optimization_barrier((weight_before, weight_after, pair))
    middle = channels // 2
    upper, lower = weight_before[:middle], weight_after[middle:]
    upper, lower = ring(upper, 1, True), ring(lower, following, True)
    weights = [out_weight, weight_before, upper, lower, weight_after]

    quarter = tokens // RING
    gated = pl.pallas_call(
        gate_kernel,
        in_specs=[near] * (4 + len(totals)),
        out_specs=[near] * RING,
        out_shape=[pltpu.VMEM((channels, quarter), bf16)] * RING,
        compiler_params=params,
        name="gate",
    )(*hold(local, gate_columns, c_own, factor, *totals))

    rows = [gated[0]] + [ring(gated[s], s, True) for s in range(1, RING)]

    half = width // 2
    with_tail, without = pltpu.VMEM((SUB + EXTRA, half), bf16), pltpu.VMEM((SUB, half), bf16)
    operands = hold(norm_gain.reshape(-1, SUB), *rows, *weights)
    opposite_first, opposite_second = pl.pallas_call(
        opposite_kernel,
        in_specs=[near] * len(operands),
        out_specs=[near] * 2,
        scratch_shapes=[pltpu.VMEM((SUB, RING * channels), bf16)],
        out_shape=[with_tail, without],
        compiler_params=params,
        name="opposite",
    )(*operands)
    got_first = ring(opposite_first, 1, False)
    got_second = ring(opposite_second, following, False)
    next_first, next_second, last_first, last_second, own, own_squares = pl.pallas_call(
        project_kernel,
        in_specs=[near] * len(operands),
        out_specs=[near] * 6,
        scratch_shapes=[pltpu.VMEM((3 * SUB, RING * channels), bf16)],
        out_shape=[with_tail, without, with_tail, without, pltpu.VMEM((SUB, width), f32), pltpu.VMEM((PAD, SUB), f32)],
        compiler_params=params,
        name="project",
    )(*operands)
    sent_second = ring(next_second, 1, False)
    sent_first = ring(last_first, following, False)
    next_sum, last_sum = pl.pallas_call(
        merge_kernel,
        in_specs=[near] * 4,
        out_specs=[near] * 2,
        out_shape=[with_tail, without],
        compiler_params=params,
        name="merge",
    )(*hold(next_first, last_second, got_first, got_second))
    from_before = ring(next_sum, 1, False)
    from_after = ring(last_sum, following, False)

    return pl.pallas_call(
        lambda *refs: finish_kernel(HEAD_COUNT * HEAD_DIM, *refs),
        in_specs=[near] * 6,
        out_specs=pl.BlockSpec((SUB, width), lambda: (0, 0)),
        out_shape=jax.ShapeDtypeStruct((SUB, width), bf16),
        compiler_params=params,
        name="finish",
    )(*hold(own, own_squares, from_before, sent_second, sent_first, from_after))


def solution(mesh):
    in_specs = (
        P(("batch", "seq"), "head"),
        P(("batch", "seq"), "head"),
        P(("batch", "seq"), None),
        P(("batch", "seq"), None),
        P("head", ("batch", "seq")),
        P("head", ("batch", "seq")),
        P("head"),
        P(),
        P("head", None),
    )
    out_specs = P(("batch", "seq", "head"), None)

    return jax.shard_map(body, mesh=mesh, in_specs=in_specs, out_specs=out_specs, check_vma=False)
```

```python
import jax
import jax.numpy as jnp
from jax import lax
from jax.experimental import pallas as pl
from jax.experimental.pallas import tpu as pltpu
from jax.sharding import PartitionSpec as P


HEAD_COUNT = 80
HEAD_DIM = 64
STATE = 128
GROUPS = 8
BLOCK = 256
RING = 4
SUB = 128
EXTRA = 8
PAD = 8

epsilon = 1e-05


f32 = jnp.float32
bf16 = jnp.bfloat16
TT = (((1,), (1,)), ((), ()))


def triangle(size, dtype):
    rows = lax.broadcasted_iota(jnp.int32, (size, size), 0)
    columns = lax.broadcasted_iota(jnp.int32, (size, size), 1)
    return (rows <= columns).astype(dtype)


def split3(value):
    high = value.astype(bf16)
    rest = value - high.astype(f32)
    middle = rest.astype(bf16)
    return high, middle, (rest - middle.astype(f32)).astype(bf16)


def join3(stacked, rows):
    return stacked[0:rows].astype(f32) + stacked[rows : 2 * rows].astype(f32) + stacked[2 * rows : 3 * rows].astype(f32)


def per_head(column, heads, lanes):
    return jnp.concatenate(
        [jnp.broadcast_to(column[h : h + 1, 0:1], (HEAD_DIM, lanes)) for h in range(heads)], axis=0
    )


def state_kernel(
    x_hbm, b_hbm, c_hbm, step_hbm, decay_hbm, prefix_ref, total_ref, cum_ref, factor_ref, x_ref, b_ref, c_ref, step_ref, decay_ref, sems
):
    heads, tokens = step_ref.shape
    blocks = tokens // BLOCK
    group = lax.axis_index("head") * heads * GROUPS // HEAD_COUNT
    columns = pl.ds(pl.multiple_of(group * STATE, STATE), STATE)
    sources = (decay_hbm, step_hbm, x_hbm, b_hbm.at[:, columns], c_hbm.at[:, columns])
    targets = (decay_ref, step_ref, x_ref, b_ref, c_ref)
    fetches = [pltpu.make_async_copy(sources[k], targets[k], sems.at[k]) for k in range(5)]
    for fetch in fetches:
        fetch.start()
    fetches[0].wait()
    fill = jnp.zeros((PAD - heads, BLOCK), f32)
    decay = jnp.concatenate(
        [piece for c in range(blocks) for piece in (decay_ref[:, c * BLOCK : (c + 1) * BLOCK], fill)], axis=0
    )
    sums = jnp.dot(
        jnp.concatenate(split3(decay), axis=0), triangle(BLOCK, bf16), preferred_element_type=f32
    )
    sums = join3(sums, blocks * PAD)
    offset = jnp.zeros((PAD, 1), f32)
    for c in range(blocks):
        span = slice(c * BLOCK, (c + 1) * BLOCK)
        cumulative = sums[c * PAD : (c + 1) * PAD]
        cum_ref[:, span] = cumulative
        factor_ref[:, span] = jnp.exp(cumulative + offset)
        offset = offset + cumulative[:, BLOCK - 1 :]
    for fetch in fetches[1:4]:
        fetch.wait()
    state = jnp.zeros((heads * HEAD_DIM, STATE), f32)
    for c in range(blocks):
        span = slice(c * BLOCK, (c + 1) * BLOCK)
        cumulative = sums[c * PAD : (c + 1) * PAD]
        end = cumulative[:, BLOCK - 1 :]
        prefix_ref[c] = state.astype(bf16)
        to_end = jnp.exp(end - cumulative)[0:heads] * step_ref[:, span]
        scaled = jnp.concatenate(
            [
                (x_ref[h * HEAD_DIM : (h + 1) * HEAD_DIM, span].astype(f32) * to_end[h : h + 1]).astype(bf16)
                for h in range(heads)
            ],
            axis=0,
        )
        block_state = jnp.dot(scaled, b_ref[span, :], preferred_element_type=f32)
        state = per_head(jnp.exp(end), heads, STATE) * state + block_state
    total_ref[0 : heads * HEAD_DIM, :] = state.astype(bf16)
    parts = split3(jnp.broadcast_to(offset, (PAD, STATE)))
    total_ref[heads * HEAD_DIM :, :] = jnp.concatenate(parts, axis=0)
    fetches[4].wait()


def pair_kernel(total_ref, before_ref, pair_ref):
    channels = total_ref.shape[0] - 3 * PAD
    heads = channels // HEAD_DIM
    logs = join3(total_ref[channels:, :], PAD)
    decayed = per_head(jnp.exp(logs), heads, STATE) * before_ref[0:channels, :].astype(f32)
    pair_ref[0:channels, :] = (total_ref[0:channels, :].astype(f32) + decayed).astype(bf16)
    pair_ref[channels:, :] = jnp.concatenate(split3(logs + join3(before_ref[channels:, :], PAD)), axis=0)


def within_kernel(skip_ref, x_ref, b_ref, c_ref, cum_ref, step_ref, prefix_ref, out_ref):
    heads = step_ref.shape[0]
    half = BLOCK // 2
    causal = triangle(half, f32).T > 0
    for k in range(step_ref.shape[1] // BLOCK):
        span = slice(k * BLOCK, (k + 1) * BLOCK)
        c_block = c_ref[span, :]
        b_block = b_ref[span, :]
        scores_first = lax.dot_general(c_block[:half], b_block[:half], TT, preferred_element_type=f32)
        scores_second = lax.dot_general(c_block[half:], b_block, TT, preferred_element_type=f32)
        across = lax.dot_general(prefix_ref[k], c_block, TT, preferred_element_type=f32)
        cumulative = cum_ref[:, span]
        factor = jnp.exp(cumulative)
        columns = cumulative.T
        for h in range(heads):
            channels = slice(h * HEAD_DIM, (h + 1) * HEAD_DIM)
            x_head = x_ref[channels, span]
            row = cumulative[h : h + 1]
            step = step_ref[h : h + 1, span]
            differ = columns[:half, h : h + 1] - row[:, :half]
            first = scores_first * jnp.exp(jnp.where(causal, differ, -jnp.inf)) * step[:, :half]
            column = columns[half:, h : h + 1]
            full = scores_second[:, :half] * jnp.exp(column - row[:, :half]) * step[:, :half]
            differ = column - row[:, half:]
            last = scores_second[:, half:] * jnp.exp(jnp.where(causal, differ, -jnp.inf)) * step[:, half:]
            second = jnp.concatenate([full, last], axis=1)
            within = jnp.concatenate(
                [
                    lax.dot_general(x_head[:, :half], first.astype(bf16), TT, preferred_element_type=f32),
                    lax.dot_general(x_head, second.astype(bf16), TT, preferred_element_type=f32),
                ],
                axis=1,
            )
            out_ref[channels, span] = (
                within + across[channels] * factor[h : h + 1] + skip_ref[h] * x_head.astype(f32)
            )


def ring_place():
    head_index = lax.axis_index("head")
    core = lax.axis_index("batch")
    y, x = head_index // RING, head_index % RING
    return core, jnp.where(core == 0, x, y), jnp.where(core == 0, y, x)


def head_at(core, u, v):
    return jnp.where(core == 0, v * RING + u, u * RING + v)


def gate_kernel(out_ref, gate_ref, c_ref, factor_ref, *refs):
    totals, results = refs[:-RING], refs[-RING:]
    channels = gate_ref.shape[0]
    heads = channels // HEAD_DIM
    incoming = jnp.zeros((channels, STATE), f32)
    log_sum = jnp.zeros((PAD, STATE), f32)
    for total in totals:
        incoming = incoming + per_head(jnp.exp(log_sum), heads, STATE) * total[0:channels, :].astype(f32)
        log_sum = log_sum + join3(total[channels:, :], PAD)
    incoming = incoming.astype(bf16)
    core, u, v = ring_place()
    for su in range(RING):
        for sv in range(RING):
            place = head_at(core, (u + su) % RING, (v + sv) % RING)
            span = pl.ds(pl.multiple_of(place * SUB, SUB), SUB)
            across = lax.dot_general(incoming, c_ref[span, :], TT, preferred_element_type=f32)
            factor = factor_ref[:, span]
            for h in range(heads):
                rows = slice(h * HEAD_DIM, (h + 1) * HEAD_DIM)
                gate = gate_ref[rows, span].astype(f32)
                output = out_ref[rows, span] + across[rows] * factor[h : h + 1]
                gated = output * (gate / (1.0 + jnp.exp(-gate)))
                results[su][rows, sv * SUB : (sv + 1) * SUB] = gated.astype(bf16)


def gain_row(gain_ref, head, channels):
    first = head * channels
    lines = gain_ref[pl.ds(first // SUB, 3), :]
    line = jnp.concatenate([lines[i : i + 1] for i in range(3)], axis=1)
    shifted = jnp.concatenate([line[:, SUB // 2 :], line[:, : SUB // 2]], axis=1)
    return jnp.where(first % SUB == 0, line, shifted)[:, :channels]


def left_side(gain_ref, rows, blocks):
    core, u, v = ring_place()
    channels = rows[0].shape[0]
    pick = [slice(k * SUB, (k + 1) * SUB) for k in blocks]
    values = jnp.concatenate([jnp.concatenate([r[:, span] for span in pick], axis=1) for r in rows], axis=0)
    wide = values.astype(f32)
    squares = jnp.sum(wide * wide, axis=0, keepdims=True)
    gains = jnp.concatenate(
        [gain_row(gain_ref, head_at(core, (u - s + RING) % RING, v), channels) for s in range(RING)], axis=1
    )
    return (values.T.astype(f32) * gains).astype(bf16), squares


def tail_rows(squares, width):
    parts = [part.astype(f32) for part in split3(squares)]
    tail = jnp.concatenate(parts + [jnp.zeros((EXTRA - 3, SUB), f32)], axis=0)
    return jnp.concatenate([tail] * (width // SUB), axis=1).astype(bf16)


def tail_squares(part):
    return jnp.sum(part[SUB:, 0:SUB].astype(f32), axis=0, keepdims=True)


def opposite_kernel(gain_ref, *refs):
    rows, weights = refs[:RING], refs[RING:-3]
    first_ref, second_ref, left = refs[-3:]
    half = first_ref.shape[1]
    left[...], squares = left_side(gain_ref, rows, (2,))
    first_ref[SUB:, :] = tail_rows(squares, half)
    tile = 256
    for n in range(2 * half // tile):
        right = jnp.concatenate([w[:, n * tile : (n + 1) * tile] for w in weights], axis=0)
        product = jnp.dot(left[...], right, preferred_element_type=f32).astype(bf16)
        if n * tile < half:
            first_ref[0:SUB, n * tile : (n + 1) * tile] = product
        else:
            second_ref[:, n * tile - half : (n + 1) * tile - half] = product


def project_kernel(gain_ref, *refs):
    rows, weights = refs[:RING], refs[RING:-7]
    next_first, next_second, last_first, last_second, own_ref, own_squares, left = refs[-7:]
    half = next_first.shape[1]
    left[...], squares = left_side(gain_ref, rows, (1, 3, 0))
    next_first[SUB:, :] = tail_rows(squares[:, 0:SUB], half)
    last_first[SUB:, :] = tail_rows(squares[:, SUB : 2 * SUB], half)
    own_squares[...] = jnp.broadcast_to(squares[:, 2 * SUB :], own_squares.shape)
    tile = 256
    for n in range(2 * half // tile):
        span = slice(n * tile, (n + 1) * tile)
        right = jnp.concatenate([w[:, span] for w in weights], axis=0)
        product = jnp.dot(left[...], right, preferred_element_type=f32)
        own_ref[:, span] = product[2 * SUB :]
        if n * tile < half:
            next_first[0:SUB, span] = product[0:SUB].astype(bf16)
            last_first[0:SUB, span] = product[SUB : 2 * SUB].astype(bf16)
        else:
            span = slice(n * tile - half, (n + 1) * tile - half)
            next_second[:, span] = product[0:SUB].astype(bf16)
            last_second[:, span] = product[SUB : 2 * SUB].astype(bf16)


def merge_kernel(next_first, last_second, got_first, got_second, next_ref, last_ref):
    next_ref[0:SUB, :] = (next_first[0:SUB, :].astype(f32) + got_first[0:SUB, :].astype(f32)).astype(bf16)
    squares = tail_squares(next_first) + tail_squares(got_first)
    next_ref[SUB:, :] = tail_rows(squares, next_ref.shape[1])
    last_ref[...] = (last_second[...].astype(f32) + got_second[...].astype(f32)).astype(bf16)


def finish_kernel(channels, own_ref, own_squares, next_first, next_second, last_first, last_second, out_ref):
    half = next_first.shape[1]
    squares = own_squares[0:1, :] + tail_squares(next_first) + tail_squares(last_first)
    scale = lax.rsqrt(squares / channels + epsilon)
    column = jnp.broadcast_to(scale, (SUB, SUB)).T[:, 0:1]
    first = own_ref[:, :half] + next_first[0:SUB, :].astype(f32) + last_first[0:SUB, :].astype(f32)
    second = own_ref[:, half:] + next_second[...].astype(f32) + last_second[...].astype(f32)
    out_ref[:, :half] = (first * column).astype(bf16)
    out_ref[:, half:] = (second * column).astype(bf16)


def ring_pairs(shift, gather):
    pairs = []
    for y in range(RING):
        for x in range(RING):
            for core in range(2):
                if (core == 0) == gather:
                    there = y * RING + (x + shift) % RING
                else:
                    there = ((y + shift) % RING) * RING + x
                pairs.append(((y * RING + x) * 2 + core, there * 2 + core))
    return pairs


def ring(value, shift, gather):
    return lax.ppermute(value, ("head", "batch"), ring_pairs(shift, gather))


def body(
    ssm_input, gate_input, b_proj, c_proj, step_size, log_decay, skip_gain, norm_gain, out_weight
):
    tokens, channels = ssm_input.shape
    heads = step_size.shape[0]
    width = out_weight.shape[1]
    blocks = tokens // BLOCK
    seq_count = lax.axis_size("seq")
    core, u, v = ring_place()
    following = RING - 1
    middle = channels // 2
    own_upper, own_lower = out_weight[:middle], out_weight[middle:]
    before_upper, after_lower = ring(own_upper, 1, True), ring(own_lower, following, True)

    params = pltpu.CompilerParams(vmem_limit_bytes=24 * 1024 * 1024)
    near = pl.BlockSpec(memory_space=pltpu.VMEM)

    def hold(*values):
        return [pltpu.with_memory_space_constraint(value, pltpu.VMEM) for value in values]

    def far(value):
        return pltpu.with_memory_space_constraint(value, pltpu.HBM)

    payload = channels + 3 * PAD
    ssm_columns, gate_columns = ssm_input.T, gate_input.T
    prefix, total, cum, factor, x_own, b_own, c_own, step_own = pl.pallas_call(
        state_kernel,
        in_specs=[pl.BlockSpec(memory_space=pltpu.HBM)] * 5,
        out_specs=[near] * 8,
        out_shape=[
            pltpu.VMEM((blocks, channels, STATE), bf16),
            pltpu.VMEM((payload, STATE), bf16),
            pltpu.VMEM((PAD, tokens), f32),
            pltpu.VMEM((PAD, tokens), f32),
            pltpu.VMEM((channels, tokens), bf16),
            pltpu.VMEM((tokens, STATE), bf16),
            pltpu.VMEM((tokens, STATE), bf16),
            pltpu.VMEM((heads, tokens), f32),
        ],
        scratch_shapes=[pltpu.VMEM((heads, tokens), f32), pltpu.SemaphoreType.DMA((5,))],
        compiler_params=params,
        name="state",
    )(*[far(value) for value in (ssm_columns, b_proj, c_proj, step_size, log_decay)])

    def along(value, shift):
        return lax.ppermute(value, "seq", [(k, k + shift) for k in range(seq_count - shift)])

    before = along(total, 1)
    before_lower, after_upper = ring(own_lower, 1, True), ring(own_upper, following, True)
    local = pl.pallas_call(
        within_kernel,
        in_specs=[pl.BlockSpec(memory_space=pltpu.SMEM)] + [near] * 6,
        out_specs=near,
        out_shape=pltpu.VMEM((channels, tokens), f32),
        compiler_params=params,
        name="within",
    )(skip_gain, *hold(x_own, b_own, c_own, cum, step_own, prefix))
    before, local, upper, lower = lax.optimization_barrier((before, local, before_upper, after_lower))
    upper, lower = ring(upper, 1, True), ring(lower, following, True)
    weights = [own_upper, own_lower, before_upper, before_lower, upper, lower, after_upper, after_lower]
    pair = pl.pallas_call(
        pair_kernel,
        in_specs=[near] * 2,
        out_specs=near,
        out_shape=pltpu.VMEM((payload, STATE), bf16),
        compiler_params=params,
        name="pair",
    )(*hold(total, before))
    totals = [along(pair, shift) for shift in range(1, seq_count, 2)]

    quarter = tokens // RING
    gated = pl.pallas_call(
        gate_kernel,
        in_specs=[near] * (4 + len(totals)),
        out_specs=[near] * RING,
        out_shape=[pltpu.VMEM((channels, quarter), bf16)] * RING,
        compiler_params=params,
        name="gate",
    )(*hold(local, gate_columns, c_own, factor, *totals))

    rows = [gated[0]] + [ring(gated[s], s, True) for s in range(1, RING)]

    half = width // 2
    with_tail, without = pltpu.VMEM((SUB + EXTRA, half), bf16), pltpu.VMEM((SUB, half), bf16)
    operands = hold(norm_gain.reshape(-1, SUB), *rows, *weights)
    opposite_first, opposite_second = pl.pallas_call(
        opposite_kernel,
        in_specs=[near] * len(operands),
        out_specs=[near] * 2,
        scratch_shapes=[pltpu.VMEM((SUB, RING * channels), bf16)],
        out_shape=[with_tail, without],
        compiler_params=params,
        name="opposite",
    )(*operands)
    got_first = ring(opposite_first, 1, False)
    got_second = ring(opposite_second, following, False)
    next_first, next_second, last_first, last_second, own, own_squares = pl.pallas_call(
        project_kernel,
        in_specs=[near] * len(operands),
        out_specs=[near] * 6,
        scratch_shapes=[pltpu.VMEM((3 * SUB, RING * channels), bf16)],
        out_shape=[with_tail, without, with_tail, without, pltpu.VMEM((SUB, width), f32), pltpu.VMEM((PAD, SUB), f32)],
        compiler_params=params,
        name="project",
    )(*operands)
    sent_second = ring(next_second, 1, False)
    sent_first = ring(last_first, following, False)
    next_sum, last_sum = pl.pallas_call(
        merge_kernel,
        in_specs=[near] * 4,
        out_specs=[near] * 2,
        out_shape=[with_tail, without],
        compiler_params=params,
        name="merge",
    )(*hold(next_first, last_second, got_first, got_second))
    from_before = ring(next_sum, 1, False)
    from_after = ring(last_sum, following, False)

    return pl.pallas_call(
        lambda *refs: finish_kernel(HEAD_COUNT * HEAD_DIM, *refs),
        in_specs=[near] * 6,
        out_specs=pl.BlockSpec((SUB, width), lambda: (0, 0)),
        out_shape=jax.ShapeDtypeStruct((SUB, width), bf16),
        compiler_params=params,
        name="finish",
    )(*hold(own, own_squares, from_before, sent_second, sent_first, from_after))


def solution(mesh):
    in_specs = (
        P(("batch", "seq"), "head"),
        P(("batch", "seq"), "head"),
        P(("batch", "seq"), None),
        P(("batch", "seq"), None),
        P("head", ("batch", "seq")),
        P("head", ("batch", "seq")),
        P("head"),
        P(),
        P("head", None),
    )
    out_specs = P(("batch", "seq", "head"), None)

    return jax.shard_map(body, mesh=mesh, in_specs=in_specs, out_specs=out_specs, check_vma=False)
```

```python
import jax
import jax.numpy as jnp
from jax import lax
from jax.experimental import pallas as pl
from jax.experimental.pallas import tpu as pltpu
from jax.sharding import PartitionSpec as P


HEAD_COUNT = 80
HEAD_DIM = 64
STATE = 128
GROUPS = 8
BLOCK = 256
RING = 4
SUB = 128
EXTRA = 8
PAD = 8

epsilon = 1e-05


f32 = jnp.float32
bf16 = jnp.bfloat16
TT = (((1,), (1,)), ((), ()))


def triangle(size, dtype):
    rows = lax.broadcasted_iota(jnp.int32, (size, size), 0)
    columns = lax.broadcasted_iota(jnp.int32, (size, size), 1)
    return (rows <= columns).astype(dtype)


def split3(value):
    high = value.astype(bf16)
    rest = value - high.astype(f32)
    middle = rest.astype(bf16)
    return high, middle, (rest - middle.astype(f32)).astype(bf16)


def join3(stacked, rows):
    return stacked[0:rows].astype(f32) + stacked[rows : 2 * rows].astype(f32) + stacked[2 * rows : 3 * rows].astype(f32)


def per_head(column, heads, lanes):
    return jnp.concatenate(
        [jnp.broadcast_to(column[h : h + 1, 0:1], (HEAD_DIM, lanes)) for h in range(heads)], axis=0
    )


def state_kernel(
    x_hbm, b_hbm, c_hbm, step_hbm, decay_hbm, prefix_ref, total_ref, cum_ref, factor_ref, x_ref, b_ref, c_ref, step_ref, decay_ref, sems
):
    heads, tokens = step_ref.shape
    blocks = tokens // BLOCK
    group = lax.axis_index("head") * heads * GROUPS // HEAD_COUNT
    columns = pl.ds(pl.multiple_of(group * STATE, STATE), STATE)
    sources = (decay_hbm, step_hbm, x_hbm, b_hbm.at[:, columns], c_hbm.at[:, columns])
    targets = (decay_ref, step_ref, x_ref, b_ref, c_ref)
    fetches = [pltpu.make_async_copy(sources[k], targets[k], sems.at[k]) for k in range(5)]
    for fetch in fetches:
        fetch.start()
    fetches[0].wait()
    fill = jnp.zeros((PAD - heads, BLOCK), f32)
    decay = jnp.concatenate(
        [piece for c in range(blocks) for piece in (decay_ref[:, c * BLOCK : (c + 1) * BLOCK], fill)], axis=0
    )
    sums = jnp.dot(
        jnp.concatenate(split3(decay), axis=0), triangle(BLOCK, bf16), preferred_element_type=f32
    )
    sums = join3(sums, blocks * PAD)
    offset = jnp.zeros((PAD, 1), f32)
    for c in range(blocks):
        span = slice(c * BLOCK, (c + 1) * BLOCK)
        cumulative = sums[c * PAD : (c + 1) * PAD]
        cum_ref[:, span] = cumulative
        factor_ref[:, span] = jnp.exp(cumulative + offset)
        offset = offset + cumulative[:, BLOCK - 1 :]
    for fetch in fetches[1:4]:
        fetch.wait()
    state = jnp.zeros((heads * HEAD_DIM, STATE), f32)
    for c in range(blocks):
        span = slice(c * BLOCK, (c + 1) * BLOCK)
        cumulative = sums[c * PAD : (c + 1) * PAD]
        end = cumulative[:, BLOCK - 1 :]
        prefix_ref[c] = state.astype(bf16)
        to_end = jnp.exp(end - cumulative)[0:heads] * step_ref[:, span]
        scaled = jnp.concatenate(
            [
                (x_ref[h * HEAD_DIM : (h + 1) * HEAD_DIM, span].astype(f32) * to_end[h : h + 1]).astype(bf16)
                for h in range(heads)
            ],
            axis=0,
        )
        block_state = jnp.dot(scaled, b_ref[span, :], preferred_element_type=f32)
        state = per_head(jnp.exp(end), heads, STATE) * state + block_state
    total_ref[0 : heads * HEAD_DIM, :] = state.astype(bf16)
    parts = split3(jnp.broadcast_to(offset, (PAD, STATE)))
    total_ref[heads * HEAD_DIM :, :] = jnp.concatenate(parts, axis=0)
    fetches[4].wait()


def pair_kernel(total_ref, before_ref, pair_ref):
    channels = total_ref.shape[0] - 3 * PAD
    heads = channels // HEAD_DIM
    logs = join3(total_ref[channels:, :], PAD)
    decayed = per_head(jnp.exp(logs), heads, STATE) * before_ref[0:channels, :].astype(f32)
    pair_ref[0:channels, :] = (total_ref[0:channels, :].astype(f32) + decayed).astype(bf16)
    pair_ref[channels:, :] = jnp.concatenate(split3(logs + join3(before_ref[channels:, :], PAD)), axis=0)


def within_kernel(skip_ref, x_ref, b_ref, c_ref, cum_ref, step_ref, prefix_ref, out_ref):
    heads = step_ref.shape[0]
    half = BLOCK // 2
    causal = triangle(half, f32).T > 0
    for k in range(step_ref.shape[1] // BLOCK):
        span = slice(k * BLOCK, (k + 1) * BLOCK)
        c_block = c_ref[span, :]
        b_block = b_ref[span, :]
        scores_first = lax.dot_general(c_block[:half], b_block[:half], TT, preferred_element_type=f32)
        scores_second = lax.dot_general(c_block[half:], b_block, TT, preferred_element_type=f32)
        across = lax.dot_general(prefix_ref[k], c_block, TT, preferred_element_type=f32)
        cumulative = cum_ref[:, span]
        factor = jnp.exp(cumulative)
        columns = cumulative.T
        for h in range(heads):
            channels = slice(h * HEAD_DIM, (h + 1) * HEAD_DIM)
            x_head = x_ref[channels, span]
            row = cumulative[h : h + 1]
            step = step_ref[h : h + 1, span]
            differ = columns[:half, h : h + 1] - row[:, :half]
            first = scores_first * jnp.exp(jnp.where(causal, differ, -jnp.inf)) * step[:, :half]
            column = columns[half:, h : h + 1]
            full = scores_second[:, :half] * jnp.exp(column - row[:, :half]) * step[:, :half]
            differ = column - row[:, half:]
            last = scores_second[:, half:] * jnp.exp(jnp.where(causal, differ, -jnp.inf)) * step[:, half:]
            second = jnp.concatenate([full, last], axis=1)
            within = jnp.concatenate(
                [
                    lax.dot_general(x_head[:, :half], first.astype(bf16), TT, preferred_element_type=f32),
                    lax.dot_general(x_head, second.astype(bf16), TT, preferred_element_type=f32),
                ],
                axis=1,
            )
            out_ref[channels, span] = (
                within + across[channels] * factor[h : h + 1] + skip_ref[h] * x_head.astype(f32)
            )


def ring_place():
    head_index = lax.axis_index("head")
    core = lax.axis_index("batch")
    y, x = head_index // RING, head_index % RING
    return core, jnp.where(core == 0, x, y), jnp.where(core == 0, y, x)


def head_at(core, u, v):
    return jnp.where(core == 0, v * RING + u, u * RING + v)


def gate_kernel(out_ref, gate_ref, c_ref, factor_ref, *refs):
    totals, results = refs[:-RING], refs[-RING:]
    channels = gate_ref.shape[0]
    heads = channels // HEAD_DIM
    incoming = jnp.zeros((channels, STATE), f32)
    log_sum = jnp.zeros((PAD, STATE), f32)
    for total in totals:
        incoming = incoming + per_head(jnp.exp(log_sum), heads, STATE) * total[0:channels, :].astype(f32)
        log_sum = log_sum + join3(total[channels:, :], PAD)
    incoming = incoming.astype(bf16)
    core, u, v = ring_place()
    for su in range(RING):
        for sv in range(RING):
            place = head_at(core, (u + su) % RING, (v + sv) % RING)
            span = pl.ds(pl.multiple_of(place * SUB, SUB), SUB)
            across = lax.dot_general(incoming, c_ref[span, :], TT, preferred_element_type=f32)
            factor = factor_ref[:, span]
            for h in range(heads):
                rows = slice(h * HEAD_DIM, (h + 1) * HEAD_DIM)
                gate = gate_ref[rows, span].astype(f32)
                output = out_ref[rows, span] + across[rows] * factor[h : h + 1]
                gated = output * (gate / (1.0 + jnp.exp(-gate)))
                results[su][rows, sv * SUB : (sv + 1) * SUB] = gated.astype(bf16)


def gain_row(gain_ref, head, channels):
    first = head * channels
    lines = gain_ref[pl.ds(first // SUB, 3), :]
    line = jnp.concatenate([lines[i : i + 1] for i in range(3)], axis=1)
    shifted = jnp.concatenate([line[:, SUB // 2 :], line[:, : SUB // 2]], axis=1)
    return jnp.where(first % SUB == 0, line, shifted)[:, :channels]


def left_side(gain_ref, rows, sources, blocks):
    core, u, v = ring_place()
    channels = rows[0].shape[0]
    pick = [slice(k * SUB, (k + 1) * SUB) for k in blocks]
    values = jnp.concatenate([jnp.concatenate([r[:, span] for span in pick], axis=1) for r in rows], axis=0)
    wide = values.astype(f32)
    squares = jnp.sum(wide * wide, axis=0, keepdims=True)
    gains = jnp.concatenate(
        [gain_row(gain_ref, head_at(core, (u - s + RING) % RING, v), channels) for s in sources], axis=1
    )
    return (values.T.astype(f32) * gains).astype(bf16), squares


def tail_rows(squares, width):
    parts = [part.astype(f32) for part in split3(squares)]
    tail = jnp.concatenate(parts + [jnp.zeros((EXTRA - 3, SUB), f32)], axis=0)
    return jnp.concatenate([tail] * (width // SUB), axis=1).astype(bf16)


def tail_squares(part):
    return jnp.sum(part[SUB:, 0:SUB].astype(f32), axis=0, keepdims=True)


def begin_kernel(gain_ref, *refs):
    rows, weights = refs[:2], refs[2:-3]
    product_ref, squares_ref, left = refs[-3:]
    left[...], squares = left_side(gain_ref, rows, (0, 1), range(RING))
    squares_ref[...] = jnp.broadcast_to(squares, squares_ref.shape)
    tile = 256
    for n in range(product_ref.shape[1] // tile):
        span = slice(n * tile, (n + 1) * tile)
        right = jnp.concatenate([w[:, span] for w in weights], axis=0)
        product_ref[:, span] = jnp.dot(left[...], right, preferred_element_type=f32)


def opposite_kernel(gain_ref, begun_ref, begun_squares, *refs):
    rows, weights = refs[:2], refs[2:-3]
    first_ref, second_ref, left = refs[-3:]
    half = first_ref.shape[1]
    block = slice(2 * SUB, 3 * SUB)
    left[...], squares = left_side(gain_ref, rows, (2, 3), (2,))
    first_ref[SUB:, :] = tail_rows(squares + begun_squares[0:1, block], half)
    tile = 256
    for n in range(2 * half // tile):
        span = slice(n * tile, (n + 1) * tile)
        right = jnp.concatenate([w[:, span] for w in weights], axis=0)
        product = begun_ref[block, span] + jnp.dot(left[...], right, preferred_element_type=f32)
        if n * tile < half:
            first_ref[0:SUB, span] = product.astype(bf16)
        else:
            second_ref[:, n * tile - half : (n + 1) * tile - half] = product.astype(bf16)


def project_kernel(gain_ref, begun_ref, begun_squares, *refs):
    rows, weights = refs[:2], refs[2:-7]
    next_first, next_second, last_first, last_second, own_ref, own_squares, left = refs[-7:]
    half = next_first.shape[1]
    own, following, previous = slice(0, SUB), slice(SUB, 2 * SUB), slice(3 * SUB, 4 * SUB)
    left[...], squares = left_side(gain_ref, rows, (2, 3), (1, 3, 0))
    next_first[SUB:, :] = tail_rows(squares[:, 0:SUB] + begun_squares[0:1, following], half)
    last_first[SUB:, :] = tail_rows(squares[:, SUB : 2 * SUB] + begun_squares[0:1, previous], half)
    own_squares[...] = jnp.broadcast_to(squares[:, 2 * SUB :] + begun_squares[0:1, own], own_squares.shape)
    tile = 256
    for n in range(2 * half // tile):
        span = slice(n * tile, (n + 1) * tile)
        right = jnp.concatenate([w[:, span] for w in weights], axis=0)
        product = jnp.dot(left[...], right, preferred_element_type=f32)
        own_ref[:, span] = product[2 * SUB :] + begun_ref[own, span]
        next_rows = (product[0:SUB] + begun_ref[following, span]).astype(bf16)
        last_rows = (product[SUB : 2 * SUB] + begun_ref[previous, span]).astype(bf16)
        if n * tile < half:
            next_first[0:SUB, span] = next_rows
            last_first[0:SUB, span] = last_rows
        else:
            span = slice(n * tile - half, (n + 1) * tile - half)
            next_second[:, span] = next_rows
            last_second[:, span] = last_rows


def merge_kernel(next_first, last_second, got_first, got_second, next_ref, last_ref):
    next_ref[0:SUB, :] = (next_first[0:SUB, :].astype(f32) + got_first[0:SUB, :].astype(f32)).astype(bf16)
    squares = tail_squares(next_first) + tail_squares(got_first)
    next_ref[SUB:, :] = tail_rows(squares, next_ref.shape[1])
    last_ref[...] = (last_second[...].astype(f32) + got_second[...].astype(f32)).astype(bf16)


def finish_kernel(channels, own_ref, own_squares, next_first, next_second, last_first, last_second, out_ref):
    half = next_first.shape[1]
    squares = own_squares[0:1, :] + tail_squares(next_first) + tail_squares(last_first)
    scale = lax.rsqrt(squares / channels + epsilon)
    column = jnp.broadcast_to(scale, (SUB, SUB)).T[:, 0:1]
    first = own_ref[:, :half] + next_first[0:SUB, :].astype(f32) + last_first[0:SUB, :].astype(f32)
    second = own_ref[:, half:] + next_second[...].astype(f32) + last_second[...].astype(f32)
    out_ref[:, :half] = (first * column).astype(bf16)
    out_ref[:, half:] = (second * column).astype(bf16)


def ring_pairs(shift, gather):
    pairs = []
    for y in range(RING):
        for x in range(RING):
            for core in range(2):
                if (core == 0) == gather:
                    there = y * RING + (x + shift) % RING
                else:
                    there = ((y + shift) % RING) * RING + x
                pairs.append(((y * RING + x) * 2 + core, there * 2 + core))
    return pairs


def ring(value, shift, gather):
    return lax.ppermute(value, ("head", "batch"), ring_pairs(shift, gather))


def body(
    ssm_input, gate_input, b_proj, c_proj, step_size, log_decay, skip_gain, norm_gain, out_weight
):
    tokens, channels = ssm_input.shape
    heads = step_size.shape[0]
    width = out_weight.shape[1]
    blocks = tokens // BLOCK
    seq_count = lax.axis_size("seq")
    core, u, v = ring_place()
    following = RING - 1
    weight_before, weight_after = ring(out_weight, 1, True), ring(out_weight, following, True)

    params = pltpu.CompilerParams(vmem_limit_bytes=24 * 1024 * 1024)
    near = pl.BlockSpec(memory_space=pltpu.VMEM)

    def hold(*values):
        return [pltpu.with_memory_space_constraint(value, pltpu.VMEM) for value in values]

    def far(value):
        return pltpu.with_memory_space_constraint(value, pltpu.HBM)

    payload = channels + 3 * PAD
    ssm_columns, gate_columns = ssm_input.T, gate_input.T
    prefix, total, cum, factor, x_own, b_own, c_own, step_own = pl.pallas_call(
        state_kernel,
        in_specs=[pl.BlockSpec(memory_space=pltpu.HBM)] * 5,
        out_specs=[near] * 8,
        out_shape=[
            pltpu.VMEM((blocks, channels, STATE), bf16),
            pltpu.VMEM((payload, STATE), bf16),
            pltpu.VMEM((PAD, tokens), f32),
            pltpu.VMEM((PAD, tokens), f32),
            pltpu.VMEM((channels, tokens), bf16),
            pltpu.VMEM((tokens, STATE), bf16),
            pltpu.VMEM((tokens, STATE), bf16),
            pltpu.VMEM((heads, tokens), f32),
        ],
        scratch_shapes=[pltpu.VMEM((heads, tokens), f32), pltpu.SemaphoreType.DMA((5,))],
        compiler_params=params,
        name="state",
    )(*[far(value) for value in (ssm_columns, b_proj, c_proj, step_size, log_decay)])

    def along(value, shift):
        return lax.ppermute(value, "seq", [(k, k + shift) for k in range(seq_count - shift)])

    before = along(total, 1)
    pair = pl.pallas_call(
        pair_kernel,
        in_specs=[near] * 2,
        out_specs=near,
        out_shape=pltpu.VMEM((payload, STATE), bf16),
        compiler_params=params,
        name="pair",
    )(*hold(total, before))
    totals = [along(pair, shift) for shift in range(1, seq_count, 2)]

    local = pl.pallas_call(
        within_kernel,
        in_specs=[pl.BlockSpec(memory_space=pltpu.SMEM)] + [near] * 6,
        out_specs=near,
        out_shape=pltpu.VMEM((channels, tokens), f32),
        compiler_params=params,
        name="within",
    )(skip_gain, *hold(x_own, b_own, c_own, cum, step_own, prefix))
    local, weight_before, weight_after = lax.optimization_barrier((local, weight_before, weight_after))
    middle = channels // 2
    upper, lower = weight_before[:middle], weight_after[middle:]
    upper, lower = ring(upper, 1, True), ring(lower, following, True)

    quarter = tokens // RING
    gated = pl.pallas_call(
        gate_kernel,
        in_specs=[near] * (4 + len(totals)),
        out_specs=[near] * RING,
        out_shape=[pltpu.VMEM((channels, quarter), bf16)] * RING,
        compiler_params=params,
        name="gate",
    )(*hold(local, gate_columns, c_own, factor, *totals))

    rows_before = ring(gated[1], 1, True)
    rows_later = [ring(gated[s], s, True) for s in range(2, RING)]

    half = width // 2
    with_tail, without = pltpu.VMEM((SUB + EXTRA, half), bf16), pltpu.VMEM((SUB, half), bf16)
    gain_lines = norm_gain.reshape(-1, SUB)
    begun, begun_squares = pl.pallas_call(
        begin_kernel,
        in_specs=[near] * 5,
        out_specs=[near] * 2,
        scratch_shapes=[pltpu.VMEM((quarter, 2 * channels), bf16)],
        out_shape=[pltpu.VMEM((quarter, width), f32), pltpu.VMEM((PAD, quarter), f32)],
        compiler_params=params,
        name="begin",
    )(*hold(gain_lines, gated[0], rows_before, out_weight, weight_before))
    operands = hold(gain_lines, begun, begun_squares, *rows_later, upper, lower, weight_after)
    opposite_first, opposite_second = pl.pallas_call(
        opposite_kernel,
        in_specs=[near] * len(operands),
        out_specs=[near] * 2,
        scratch_shapes=[pltpu.VMEM((SUB, 2 * channels), bf16)],
        out_shape=[with_tail, without],
        compiler_params=params,
        name="opposite",
    )(*operands)
    got_first = ring(opposite_first, 1, False)
    got_second = ring(opposite_second, following, False)
    next_first, next_second, last_first, last_second, own, own_squares = pl.pallas_call(
        project_kernel,
        in_specs=[near] * len(operands),
        out_specs=[near] * 6,
        scratch_shapes=[pltpu.VMEM((3 * SUB, 2 * channels), bf16)],
        out_shape=[with_tail, without, with_tail, without, pltpu.VMEM((SUB, width), f32), pltpu.VMEM((PAD, SUB), f32)],
        compiler_params=params,
        name="project",
    )(*operands)
    sent_second = ring(next_second, 1, False)
    sent_first = ring(last_first, following, False)
    next_sum, last_sum = pl.pallas_call(
        merge_kernel,
        in_specs=[near] * 4,
        out_specs=[near] * 2,
        out_shape=[with_tail, without],
        compiler_params=params,
        name="merge",
    )(*hold(next_first, last_second, got_first, got_second))
    from_before = ring(next_sum, 1, False)
    from_after = ring(last_sum, following, False)

    return pl.pallas_call(
        lambda *refs: finish_kernel(HEAD_COUNT * HEAD_DIM, *refs),
        in_specs=[near] * 6,
        out_specs=pl.BlockSpec((SUB, width), lambda: (0, 0)),
        out_shape=jax.ShapeDtypeStruct((SUB, width), bf16),
        compiler_params=params,
        name="finish",
    )(*hold(own, own_squares, from_before, sent_second, sent_first, from_after))


def solution(mesh):
    in_specs = (
        P(("batch", "seq"), "head"),
        P(("batch", "seq"), "head"),
        P(("batch", "seq"), None),
        P(("batch", "seq"), None),
        P("head", ("batch", "seq")),
        P("head", ("batch", "seq")),
        P("head"),
        P(),
        P("head", None),
    )
    out_specs = P(("batch", "seq", "head"), None)

    return jax.shard_map(body, mesh=mesh, in_specs=in_specs, out_specs=out_specs, check_vma=False)
```

```python
import jax
import jax.numpy as jnp
from jax import lax
from jax.experimental import pallas as pl
from jax.experimental.pallas import tpu as pltpu
from jax.sharding import PartitionSpec as P


HEAD_COUNT = 80
HEAD_DIM = 64
STATE = 128
GROUPS = 8
BLOCK = 256
RING = 4
SUB = 128
EXTRA = 8
PAD = 8

epsilon = 1e-05


f32 = jnp.float32
bf16 = jnp.bfloat16
TT = (((1,), (1,)), ((), ()))


def triangle(size, dtype):
    rows = lax.broadcasted_iota(jnp.int32, (size, size), 0)
    columns = lax.broadcasted_iota(jnp.int32, (size, size), 1)
    return (rows <= columns).astype(dtype)


def split3(value):
    high = value.astype(bf16)
    rest = value - high.astype(f32)
    middle = rest.astype(bf16)
    return high, middle, (rest - middle.astype(f32)).astype(bf16)


def join3(stacked, rows):
    return stacked[0:rows].astype(f32) + stacked[rows : 2 * rows].astype(f32) + stacked[2 * rows : 3 * rows].astype(f32)


def per_head(column, heads, lanes):
    return jnp.concatenate(
        [jnp.broadcast_to(column[h : h + 1, 0:1], (HEAD_DIM, lanes)) for h in range(heads)], axis=0
    )


def state_kernel(
    x_hbm, b_hbm, c_hbm, step_hbm, decay_hbm, prefix_ref, total_ref, cum_ref, factor_ref, x_ref, b_ref, c_ref, step_ref, decay_ref, sems
):
    heads, tokens = step_ref.shape
    blocks = tokens // BLOCK
    group = lax.axis_index("head") * heads * GROUPS // HEAD_COUNT
    columns = pl.ds(pl.multiple_of(group * STATE, STATE), STATE)
    sources = (decay_hbm, step_hbm, x_hbm, b_hbm.at[:, columns], c_hbm.at[:, columns])
    targets = (decay_ref, step_ref, x_ref, b_ref, c_ref)
    fetches = [pltpu.make_async_copy(sources[k], targets[k], sems.at[k]) for k in range(5)]
    for fetch in fetches:
        fetch.start()
    fetches[0].wait()
    fill = jnp.zeros((PAD - heads, BLOCK), f32)
    decay = jnp.concatenate(
        [piece for c in range(blocks) for piece in (decay_ref[:, c * BLOCK : (c + 1) * BLOCK], fill)], axis=0
    )
    sums = jnp.dot(
        jnp.concatenate(split3(decay), axis=0), triangle(BLOCK, bf16), preferred_element_type=f32
    )
    sums = join3(sums, blocks * PAD)
    offset = jnp.zeros((PAD, 1), f32)
    for c in range(blocks):
        span = slice(c * BLOCK, (c + 1) * BLOCK)
        cumulative = sums[c * PAD : (c + 1) * PAD]
        cum_ref[:, span] = cumulative
        factor_ref[:, span] = jnp.exp(cumulative + offset)
        offset = offset + cumulative[:, BLOCK - 1 :]
    for fetch in fetches[1:4]:
        fetch.wait()
    state = jnp.zeros((heads * HEAD_DIM, STATE), f32)
    for c in range(blocks):
        span = slice(c * BLOCK, (c + 1) * BLOCK)
        cumulative = sums[c * PAD : (c + 1) * PAD]
        end = cumulative[:, BLOCK - 1 :]
        prefix_ref[c] = state.astype(bf16)
        to_end = jnp.exp(end - cumulative)[0:heads] * step_ref[:, span]
        scaled = jnp.concatenate(
            [
                (x_ref[h * HEAD_DIM : (h + 1) * HEAD_DIM, span].astype(f32) * to_end[h : h + 1]).astype(bf16)
                for h in range(heads)
            ],
            axis=0,
        )
        block_state = jnp.dot(scaled, b_ref[span, :], preferred_element_type=f32)
        state = per_head(jnp.exp(end), heads, STATE) * state + block_state
    total_ref[0 : heads * HEAD_DIM, :] = state.astype(bf16)
    parts = split3(jnp.broadcast_to(offset, (PAD, STATE)))
    total_ref[heads * HEAD_DIM :, :] = jnp.concatenate(parts, axis=0)
    fetches[4].wait()


def pair_kernel(total_ref, before_ref, pair_ref):
    channels = total_ref.shape[0] - 3 * PAD
    heads = channels // HEAD_DIM
    logs = join3(total_ref[channels:, :], PAD)
    decayed = per_head(jnp.exp(logs), heads, STATE) * before_ref[0:channels, :].astype(f32)
    pair_ref[0:channels, :] = (total_ref[0:channels, :].astype(f32) + decayed).astype(bf16)
    pair_ref[channels:, :] = jnp.concatenate(split3(logs + join3(before_ref[channels:, :], PAD)), axis=0)


def within_kernel(skip_ref, x_ref, b_ref, c_ref, cum_ref, step_ref, prefix_ref, out_ref):
    heads = step_ref.shape[0]
    half = BLOCK // 2
    causal = triangle(half, f32).T > 0
    for k in range(step_ref.shape[1] // BLOCK):
        span = slice(k * BLOCK, (k + 1) * BLOCK)
        c_block = c_ref[span, :]
        b_block = b_ref[span, :]
        scores_first = lax.dot_general(c_block[:half], b_block[:half], TT, preferred_element_type=f32)
        scores_second = lax.dot_general(c_block[half:], b_block, TT, preferred_element_type=f32)
        across = lax.dot_general(prefix_ref[k], c_block, TT, preferred_element_type=f32)
        cumulative = cum_ref[:, span]
        factor = jnp.exp(cumulative)
        columns = cumulative.T
        for h in range(heads):
            channels = slice(h * HEAD_DIM, (h + 1) * HEAD_DIM)
            x_head = x_ref[channels, span]
            row = cumulative[h : h + 1]
            step = step_ref[h : h + 1, span]
            differ = columns[:half, h : h + 1] - row[:, :half]
            first = scores_first * jnp.exp(jnp.where(causal, differ, -jnp.inf)) * step[:, :half]
            column = columns[half:, h : h + 1]
            full = scores_second[:, :half] * jnp.exp(column - row[:, :half]) * step[:, :half]
            differ = column - row[:, half:]
            last = scores_second[:, half:] * jnp.exp(jnp.where(causal, differ, -jnp.inf)) * step[:, half:]
            second = jnp.concatenate([full, last], axis=1)
            within = jnp.concatenate(
                [
                    lax.dot_general(x_head[:, :half], first.astype(bf16), TT, preferred_element_type=f32),
                    lax.dot_general(x_head, second.astype(bf16), TT, preferred_element_type=f32),
                ],
                axis=1,
            )
            out_ref[channels, span] = (
                within + across[channels] * factor[h : h + 1] + skip_ref[h] * x_head.astype(f32)
            )


def ring_place():
    head_index = lax.axis_index("head")
    core = lax.axis_index("batch")
    y, x = head_index // RING, head_index % RING
    return core, jnp.where(core == 0, x, y), jnp.where(core == 0, y, x)


def head_at(core, u, v):
    return jnp.where(core == 0, v * RING + u, u * RING + v)


def gate_kernel(out_ref, gate_ref, c_ref, factor_ref, *refs):
    totals, results = refs[:-RING], refs[-RING:]
    channels = gate_ref.shape[0]
    heads = channels // HEAD_DIM
    incoming = jnp.zeros((channels, STATE), f32)
    log_sum = jnp.zeros((PAD, STATE), f32)
    for total in totals:
        incoming = incoming + per_head(jnp.exp(log_sum), heads, STATE) * total[0:channels, :].astype(f32)
        log_sum = log_sum + join3(total[channels:, :], PAD)
    incoming = incoming.astype(bf16)
    core, u, v = ring_place()
    for su in range(RING):
        for sv in range(RING):
            place = head_at(core, (u + su) % RING, (v + sv) % RING)
            span = pl.ds(pl.multiple_of(place * SUB, SUB), SUB)
            across = lax.dot_general(incoming, c_ref[span, :], TT, preferred_element_type=f32)
            factor = factor_ref[:, span]
            for h in range(heads):
                rows = slice(h * HEAD_DIM, (h + 1) * HEAD_DIM)
                gate = gate_ref[rows, span].astype(f32)
                output = out_ref[rows, span] + across[rows] * factor[h : h + 1]
                gated = output * (gate / (1.0 + jnp.exp(-gate)))
                results[su][rows, sv * SUB : (sv + 1) * SUB] = gated.astype(bf16)


def gain_row(gain_ref, head, channels):
    first = head * channels
    lines = gain_ref[pl.ds(first // SUB, 3), :]
    line = jnp.concatenate([lines[i : i + 1] for i in range(3)], axis=1)
    shifted = jnp.concatenate([line[:, SUB // 2 :], line[:, : SUB // 2]], axis=1)
    return jnp.where(first % SUB == 0, line, shifted)[:, :channels]


def left_side(gain_ref, rows, sources, blocks):
    core, u, v = ring_place()
    channels = rows[0].shape[0]
    pick = [slice(k * SUB, (k + 1) * SUB) for k in blocks]
    values = jnp.concatenate([jnp.concatenate([r[:, span] for span in pick], axis=1) for r in rows], axis=0)
    wide = values.astype(f32)
    squares = jnp.sum(wide * wide, axis=0, keepdims=True)
    gains = jnp.concatenate(
        [gain_row(gain_ref, head_at(core, (u - s + RING) % RING, v), channels) for s in sources], axis=1
    )
    return (values.T.astype(f32) * gains).astype(bf16), squares


def tail_rows(squares, width):
    parts = [part.astype(f32) for part in split3(squares)]
    tail = jnp.concatenate(parts + [jnp.zeros((EXTRA - 3, SUB), f32)], axis=0)
    return jnp.concatenate([tail] * (width // SUB), axis=1).astype(bf16)


def tail_squares(part):
    return jnp.sum(part[SUB:, 0:SUB].astype(f32), axis=0, keepdims=True)


def begin_kernel(gain_ref, *refs):
    rows, weights = refs[:2], refs[2:-3]
    product_ref, squares_ref, left = refs[-3:]
    left[...], squares = left_side(gain_ref, rows, (0, 2), range(RING))
    squares_ref[...] = jnp.broadcast_to(squares, squares_ref.shape)
    tile = 256
    for n in range(product_ref.shape[1] // tile):
        span = slice(n * tile, (n + 1) * tile)
        right = jnp.concatenate([w[:, span] for w in weights], axis=0)
        product_ref[:, span] = jnp.dot(left[...], right, preferred_element_type=f32)


def opposite_kernel(gain_ref, begun_ref, begun_squares, *refs):
    rows, weights = refs[:2], refs[2:-3]
    first_ref, second_ref, left = refs[-3:]
    half = first_ref.shape[1]
    block = slice(2 * SUB, 3 * SUB)
    left[...], squares = left_side(gain_ref, rows, (1, 3), (2,))
    first_ref[SUB:, :] = tail_rows(squares + begun_squares[0:1, block], half)
    tile = 256
    for n in range(2 * half // tile):
        span = slice(n * tile, (n + 1) * tile)
        right = jnp.concatenate([w[:, span] for w in weights], axis=0)
        product = begun_ref[block, span] + jnp.dot(left[...], right, preferred_element_type=f32)
        if n * tile < half:
            first_ref[0:SUB, span] = product.astype(bf16)
        else:
            second_ref[:, n * tile - half : (n + 1) * tile - half] = product.astype(bf16)


def project_kernel(gain_ref, begun_ref, begun_squares, *refs):
    rows, weights = refs[:2], refs[2:-7]
    next_first, next_second, last_first, last_second, own_ref, own_squares, left = refs[-7:]
    half = next_first.shape[1]
    own, following, previous = slice(0, SUB), slice(SUB, 2 * SUB), slice(3 * SUB, 4 * SUB)
    left[...], squares = left_side(gain_ref, rows, (1, 3), (1, 3, 0))
    next_first[SUB:, :] = tail_rows(squares[:, 0:SUB] + begun_squares[0:1, following], half)
    last_first[SUB:, :] = tail_rows(squares[:, SUB : 2 * SUB] + begun_squares[0:1, previous], half)
    own_squares[...] = jnp.broadcast_to(squares[:, 2 * SUB :] + begun_squares[0:1, own], own_squares.shape)
    tile = 256
    for n in range(2 * half // tile):
        span = slice(n * tile, (n + 1) * tile)
        right = jnp.concatenate([w[:, span] for w in weights], axis=0)
        product = jnp.dot(left[...], right, preferred_element_type=f32)
        own_ref[:, span] = product[2 * SUB :] + begun_ref[own, span]
        next_rows = (product[0:SUB] + begun_ref[following, span]).astype(bf16)
        last_rows = (product[SUB : 2 * SUB] + begun_ref[previous, span]).astype(bf16)
        if n * tile < half:
            next_first[0:SUB, span] = next_rows
            last_first[0:SUB, span] = last_rows
        else:
            span = slice(n * tile - half, (n + 1) * tile - half)
            next_second[:, span] = next_rows
            last_second[:, span] = last_rows


def merge_kernel(next_first, last_second, got_first, got_second, next_ref, last_ref):
    next_ref[0:SUB, :] = (next_first[0:SUB, :].astype(f32) + got_first[0:SUB, :].astype(f32)).astype(bf16)
    squares = tail_squares(next_first) + tail_squares(got_first)
    next_ref[SUB:, :] = tail_rows(squares, next_ref.shape[1])
    last_ref[...] = (last_second[...].astype(f32) + got_second[...].astype(f32)).astype(bf16)


def finish_kernel(channels, own_ref, own_squares, next_first, next_second, last_first, last_second, out_ref):
    half = next_first.shape[1]
    squares = own_squares[0:1, :] + tail_squares(next_first) + tail_squares(last_first)
    scale = lax.rsqrt(squares / channels + epsilon)
    column = jnp.broadcast_to(scale, (SUB, SUB)).T[:, 0:1]
    first = own_ref[:, :half] + next_first[0:SUB, :].astype(f32) + last_first[0:SUB, :].astype(f32)
    second = own_ref[:, half:] + next_second[...].astype(f32) + last_second[...].astype(f32)
    out_ref[:, :half] = (first * column).astype(bf16)
    out_ref[:, half:] = (second * column).astype(bf16)


def ring_pairs(shift, gather):
    pairs = []
    for y in range(RING):
        for x in range(RING):
            for core in range(2):
                if (core == 0) == gather:
                    there = y * RING + (x + shift) % RING
                else:
                    there = ((y + shift) % RING) * RING + x
                pairs.append(((y * RING + x) * 2 + core, there * 2 + core))
    return pairs


def ring(value, shift, gather):
    return lax.ppermute(value, ("head", "batch"), ring_pairs(shift, gather))


def body(
    ssm_input, gate_input, b_proj, c_proj, step_size, log_decay, skip_gain, norm_gain, out_weight
):
    tokens, channels = ssm_input.shape
    heads = step_size.shape[0]
    width = out_weight.shape[1]
    blocks = tokens // BLOCK
    seq_count = lax.axis_size("seq")
    core, u, v = ring_place()
    following = RING - 1
    weight_before, weight_after = ring(out_weight, 1, True), ring(out_weight, following, True)

    params = pltpu.CompilerParams(vmem_limit_bytes=24 * 1024 * 1024)
    near = pl.BlockSpec(memory_space=pltpu.VMEM)

    def hold(*values):
        return [pltpu.with_memory_space_constraint(value, pltpu.VMEM) for value in values]

    def far(value):
        return pltpu.with_memory_space_constraint(value, pltpu.HBM)

    payload = channels + 3 * PAD
    ssm_columns, gate_columns = ssm_input.T, gate_input.T
    prefix, total, cum, factor, x_own, b_own, c_own, step_own = pl.pallas_call(
        state_kernel,
        in_specs=[pl.BlockSpec(memory_space=pltpu.HBM)] * 5,
        out_specs=[near] * 8,
        out_shape=[
            pltpu.VMEM((blocks, channels, STATE), bf16),
            pltpu.VMEM((payload, STATE), bf16),
            pltpu.VMEM((PAD, tokens), f32),
            pltpu.VMEM((PAD, tokens), f32),
            pltpu.VMEM((channels, tokens), bf16),
            pltpu.VMEM((tokens, STATE), bf16),
            pltpu.VMEM((tokens, STATE), bf16),
            pltpu.VMEM((heads, tokens), f32),
        ],
        scratch_shapes=[pltpu.VMEM((heads, tokens), f32), pltpu.SemaphoreType.DMA((5,))],
        compiler_params=params,
        name="state",
    )(*[far(value) for value in (ssm_columns, b_proj, c_proj, step_size, log_decay)])

    def along(value, shift):
        return lax.ppermute(value, "seq", [(k, k + shift) for k in range(seq_count - shift)])

    before = along(total, 1)
    local = pl.pallas_call(
        within_kernel,
        in_specs=[pl.BlockSpec(memory_space=pltpu.SMEM)] + [near] * 6,
        out_specs=near,
        out_shape=pltpu.VMEM((channels, tokens), f32),
        compiler_params=params,
        name="within",
    )(skip_gain, *hold(x_own, b_own, c_own, cum, step_own, prefix))
    before, local = lax.optimization_barrier((before, local))
    pair = pl.pallas_call(
        pair_kernel,
        in_specs=[near] * 2,
        out_specs=near,
        out_shape=pltpu.VMEM((payload, STATE), bf16),
        compiler_params=params,
        name="pair",
    )(*hold(total, before))
    totals = [along(pair, shift) for shift in range(1, seq_count, 2)]

    weight_before, weight_after, pair = lax.optimization_barrier((weight_before, weight_after, pair))
    middle = channels // 2
    upper, lower = weight_before[:middle], weight_after[middle:]
    upper, lower = ring(upper, 1, True), ring(lower, following, True)

    quarter = tokens // RING
    gated = pl.pallas_call(
        gate_kernel,
        in_specs=[near] * (4 + len(totals)),
        out_specs=[near] * RING,
        out_shape=[pltpu.VMEM((channels, quarter), bf16)] * RING,
        compiler_params=params,
        name="gate",
    )(*hold(local, gate_columns, c_own, factor, *totals))

    rows_opposite = ring(gated[2], 2, True)
    rows_near = [ring(gated[s], s, True) for s in (1, following)]

    half = width // 2
    with_tail, without = pltpu.VMEM((SUB + EXTRA, half), bf16), pltpu.VMEM((SUB, half), bf16)
    gain_lines = norm_gain.reshape(-1, SUB)
    begun, begun_squares = pl.pallas_call(
        begin_kernel,
        in_specs=[near] * 6,
        out_specs=[near] * 2,
        scratch_shapes=[pltpu.VMEM((quarter, 2 * channels), bf16)],
        out_shape=[pltpu.VMEM((quarter, width), f32), pltpu.VMEM((PAD, quarter), f32)],
        compiler_params=params,
        name="begin",
    )(*hold(gain_lines, gated[0], rows_opposite, out_weight, upper, lower))
    operands = hold(gain_lines, begun, begun_squares, *rows_near, weight_before, weight_after)
    opposite_first, opposite_second = pl.pallas_call(
        opposite_kernel,
        in_specs=[near] * len(operands),
        out_specs=[near] * 2,
        scratch_shapes=[pltpu.VMEM((SUB, 2 * channels), bf16)],
        out_shape=[with_tail, without],
        compiler_params=params,
        name="opposite",
    )(*operands)
    got_first = ring(opposite_first, 1, False)
    got_second = ring(opposite_second, following, False)
    next_first, next_second, last_first, last_second, own, own_squares = pl.pallas_call(
        project_kernel,
        in_specs=[near] * len(operands),
        out_specs=[near] * 6,
        scratch_shapes=[pltpu.VMEM((3 * SUB, 2 * channels), bf16)],
        out_shape=[with_tail, without, with_tail, without, pltpu.VMEM((SUB, width), f32), pltpu.VMEM((PAD, SUB), f32)],
        compiler_params=params,
        name="project",
    )(*operands)
    sent_second = ring(next_second, 1, False)
    sent_first = ring(last_first, following, False)
    next_sum, last_sum = pl.pallas_call(
        merge_kernel,
        in_specs=[near] * 4,
        out_specs=[near] * 2,
        out_shape=[with_tail, without],
        compiler_params=params,
        name="merge",
    )(*hold(next_first, last_second, got_first, got_second))
    from_before = ring(next_sum, 1, False)
    from_after = ring(last_sum, following, False)

    return pl.pallas_call(
        lambda *refs: finish_kernel(HEAD_COUNT * HEAD_DIM, *refs),
        in_specs=[near] * 6,
        out_specs=pl.BlockSpec((SUB, width), lambda: (0, 0)),
        out_shape=jax.ShapeDtypeStruct((SUB, width), bf16),
        compiler_params=params,
        name="finish",
    )(*hold(own, own_squares, from_before, sent_second, sent_first, from_after))


def solution(mesh):
    in_specs = (
        P(("batch", "seq"), "head"),
        P(("batch", "seq"), "head"),
        P(("batch", "seq"), None),
        P(("batch", "seq"), None),
        P("head", ("batch", "seq")),
        P("head", ("batch", "seq")),
        P("head"),
        P(),
        P("head", None),
    )
    out_specs = P(("batch", "seq", "head"), None)

    return jax.shard_map(body, mesh=mesh, in_specs=in_specs, out_specs=out_specs, check_vma=False)
```

```python
import jax
import jax.numpy as jnp
from jax import lax
from jax.experimental import pallas as pl
from jax.experimental.pallas import tpu as pltpu
from jax.sharding import PartitionSpec as P


HEAD_COUNT = 80
HEAD_DIM = 64
STATE = 128
GROUPS = 8
BLOCK = 256
RING = 4
SUB = 128
EXTRA = 8
PAD = 8
PIECES = 4

epsilon = 1e-05


f32 = jnp.float32
bf16 = jnp.bfloat16
TT = (((1,), (1,)), ((), ()))


def triangle(size, dtype):
    rows = lax.broadcasted_iota(jnp.int32, (size, size), 0)
    columns = lax.broadcasted_iota(jnp.int32, (size, size), 1)
    return (rows <= columns).astype(dtype)


def split3(value):
    high = value.astype(bf16)
    rest = value - high.astype(f32)
    middle = rest.astype(bf16)
    return high, middle, (rest - middle.astype(f32)).astype(bf16)


def join3(stacked, rows):
    return stacked[0:rows].astype(f32) + stacked[rows : 2 * rows].astype(f32) + stacked[2 * rows : 3 * rows].astype(f32)


def per_head(column, heads, lanes):
    return jnp.concatenate(
        [jnp.broadcast_to(column[h : h + 1, 0:1], (HEAD_DIM, lanes)) for h in range(heads)], axis=0
    )


def state_kernel(
    x_hbm, b_hbm, c_hbm, step_hbm, decay_hbm, prefix_ref, total_ref, cum_ref, factor_ref, x_ref, b_ref, c_ref, step_ref, decay_ref, sems
):
    heads, tokens = step_ref.shape
    blocks = tokens // BLOCK
    group = lax.axis_index("head") * heads * GROUPS // HEAD_COUNT
    columns = pl.ds(pl.multiple_of(group * STATE, STATE), STATE)
    piece = tokens // PIECES
    pieces = [slice(k * piece, (k + 1) * piece) for k in range(PIECES)]
    sources = [decay_hbm, step_hbm, b_hbm.at[:, columns]] + [x_hbm.at[:, span] for span in pieces] + [c_hbm.at[:, columns]]
    targets = [decay_ref, step_ref, b_ref] + [x_ref.at[:, span] for span in pieces] + [c_ref]
    fetches = [pltpu.make_async_copy(sources[k], targets[k], sems.at[k]) for k in range(PIECES + 4)]
    for fetch in fetches:
        fetch.start()
    fetches[0].wait()
    fill = jnp.zeros((PAD - heads, BLOCK), f32)
    decay = jnp.concatenate(
        [piece for c in range(blocks) for piece in (decay_ref[:, c * BLOCK : (c + 1) * BLOCK], fill)], axis=0
    )
    sums = jnp.dot(
        jnp.concatenate(split3(decay), axis=0), triangle(BLOCK, bf16), preferred_element_type=f32
    )
    sums = join3(sums, blocks * PAD)
    offset = jnp.zeros((PAD, 1), f32)
    for c in range(blocks):
        span = slice(c * BLOCK, (c + 1) * BLOCK)
        cumulative = sums[c * PAD : (c + 1) * PAD]
        cum_ref[:, span] = cumulative
        factor_ref[:, span] = jnp.exp(cumulative + offset)
        offset = offset + cumulative[:, BLOCK - 1 :]
    fetches[1].wait()
    fetches[2].wait()
    state = jnp.zeros((heads * HEAD_DIM, STATE), f32)
    for c in range(blocks):
        span = slice(c * BLOCK, (c + 1) * BLOCK)
        if c * BLOCK % piece == 0:
            fetches[3 + c * BLOCK // piece].wait()
        cumulative = sums[c * PAD : (c + 1) * PAD]
        end = cumulative[:, BLOCK - 1 :]
        prefix_ref[c] = state.astype(bf16)
        to_end = jnp.exp(end - cumulative)[0:heads] * step_ref[:, span]
        scaled = jnp.concatenate(
            [
                (x_ref[h * HEAD_DIM : (h + 1) * HEAD_DIM, span].astype(f32) * to_end[h : h + 1]).astype(bf16)
                for h in range(heads)
            ],
            axis=0,
        )
        block_state = jnp.dot(scaled, b_ref[span, :], preferred_element_type=f32)
        state = per_head(jnp.exp(end), heads, STATE) * state + block_state
    total_ref[0 : heads * HEAD_DIM, :] = state.astype(bf16)
    parts = split3(jnp.broadcast_to(offset, (PAD, STATE)))
    total_ref[heads * HEAD_DIM :, :] = jnp.concatenate(parts, axis=0)
    fetches[-1].wait()


def within_kernel(skip_ref, x_ref, b_ref, c_ref, cum_ref, step_ref, prefix_ref, out_ref):
    heads = step_ref.shape[0]
    half = BLOCK // 2
    causal = triangle(half, f32).T > 0
    for k in range(step_ref.shape[1] // BLOCK):
        span = slice(k * BLOCK, (k + 1) * BLOCK)
        c_block = c_ref[span, :]
        b_block = b_ref[span, :]
        scores_first = lax.dot_general(c_block[:half], b_block[:half], TT, preferred_element_type=f32)
        scores_second = lax.dot_general(c_block[half:], b_block, TT, preferred_element_type=f32)
        across = lax.dot_general(prefix_ref[k], c_block, TT, preferred_element_type=f32)
        cumulative = cum_ref[:, span]
        factor = jnp.exp(cumulative)
        columns = cumulative.T
        for h in range(heads):
            channels = slice(h * HEAD_DIM, (h + 1) * HEAD_DIM)
            x_head = x_ref[channels, span]
            row = cumulative[h : h + 1]
            step = step_ref[h : h + 1, span]
            differ = columns[:half, h : h + 1] - row[:, :half]
            first = scores_first * jnp.exp(jnp.where(causal, differ, -jnp.inf)) * step[:, :half]
            column = columns[half:, h : h + 1]
            full = scores_second[:, :half] * jnp.exp(column - row[:, :half]) * step[:, :half]
            differ = column - row[:, half:]
            last = scores_second[:, half:] * jnp.exp(jnp.where(causal, differ, -jnp.inf)) * step[:, half:]
            second = jnp.concatenate([full, last], axis=1)
            within = jnp.concatenate(
                [
                    lax.dot_general(x_head[:, :half], first.astype(bf16), TT, preferred_element_type=f32),
                    lax.dot_general(x_head, second.astype(bf16), TT, preferred_element_type=f32),
                ],
                axis=1,
            )
            out_ref[channels, span] = (
                within + across[channels] * factor[h : h + 1] + skip_ref[h] * x_head.astype(f32)
            )


def ring_place():
    head_index = lax.axis_index("head")
    core = lax.axis_index("batch")
    y, x = head_index // RING, head_index % RING
    return core, jnp.where(core == 0, x, y), jnp.where(core == 0, y, x)


def head_at(core, u, v):
    return jnp.where(core == 0, v * RING + u, u * RING + v)


def gate_kernel(out_ref, gate_ref, c_ref, factor_ref, *refs):
    totals, results = refs[:-RING], refs[-RING:]
    channels = gate_ref.shape[0]
    heads = channels // HEAD_DIM
    incoming = jnp.zeros((channels, STATE), f32)
    log_sum = jnp.zeros((PAD, STATE), f32)
    for total in totals:
        incoming = incoming + per_head(jnp.exp(log_sum), heads, STATE) * total[0:channels, :].astype(f32)
        log_sum = log_sum + join3(total[channels:, :], PAD)
    incoming = incoming.astype(bf16)
    core, u, v = ring_place()
    for su in range(RING):
        for sv in range(RING):
            place = head_at(core, (u + su) % RING, (v + sv) % RING)
            span = pl.ds(pl.multiple_of(place * SUB, SUB), SUB)
            across = lax.dot_general(incoming, c_ref[span, :], TT, preferred_element_type=f32)
            factor = factor_ref[:, span]
            for h in range(heads):
                rows = slice(h * HEAD_DIM, (h + 1) * HEAD_DIM)
                gate = gate_ref[rows, span].astype(f32)
                output = out_ref[rows, span] + across[rows] * factor[h : h + 1]
                gated = output * (gate / (1.0 + jnp.exp(-gate)))
                results[su][rows, sv * SUB : (sv + 1) * SUB] = gated.astype(bf16)


def gain_row(gain_ref, head, channels):
    first = head * channels
    lines = gain_ref[pl.ds(first // SUB, 3), :]
    line = jnp.concatenate([lines[i : i + 1] for i in range(3)], axis=1)
    shifted = jnp.concatenate([line[:, SUB // 2 :], line[:, : SUB // 2]], axis=1)
    return jnp.where(first % SUB == 0, line, shifted)[:, :channels]


def left_side(gain_ref, rows, sources, blocks):
    core, u, v = ring_place()
    channels = rows[0].shape[0]
    pick = [slice(k * SUB, (k + 1) * SUB) for k in blocks]
    values = jnp.concatenate([jnp.concatenate([r[:, span] for span in pick], axis=1) for r in rows], axis=0)
    wide = values.astype(f32)
    squares = jnp.sum(wide * wide, axis=0, keepdims=True)
    gains = jnp.concatenate(
        [gain_row(gain_ref, head_at(core, (u - s + RING) % RING, v), channels) for s in sources], axis=1
    )
    return (values.T.astype(f32) * gains).astype(bf16), squares


def tail_rows(squares, width):
    parts = [part.astype(f32) for part in split3(squares)]
    tail = jnp.concatenate(parts + [jnp.zeros((EXTRA - 3, SUB), f32)], axis=0)
    return jnp.concatenate([tail] * (width // SUB), axis=1).astype(bf16)


def tail_squares(part):
    return jnp.sum(part[SUB:, 0:SUB].astype(f32), axis=0, keepdims=True)


def begin_kernel(gain_ref, *refs):
    rows, weights = refs[:2], refs[2:-3]
    product_ref, squares_ref, left = refs[-3:]
    left[...], squares = left_side(gain_ref, rows, (0, 2), range(RING))
    squares_ref[...] = jnp.broadcast_to(squares, squares_ref.shape)
    tile = 256
    for n in range(product_ref.shape[1] // tile):
        span = slice(n * tile, (n + 1) * tile)
        right = jnp.concatenate([w[:, span] for w in weights], axis=0)
        product_ref[:, span] = jnp.dot(left[...], right, preferred_element_type=f32)


def opposite_kernel(gain_ref, begun_ref, begun_squares, *refs):
    rows, weights = refs[:2], refs[2:-3]
    first_ref, second_ref, left = refs[-3:]
    half = first_ref.shape[1]
    block = slice(2 * SUB, 3 * SUB)
    left[...], squares = left_side(gain_ref, rows, (1, 3), (2,))
    first_ref[SUB:, :] = tail_rows(squares + begun_squares[0:1, block], half)
    tile = 256
    for n in range(2 * half // tile):
        span = slice(n * tile, (n + 1) * tile)
        right = jnp.concatenate([w[:, span] for w in weights], axis=0)
        product = begun_ref[block, span] + jnp.dot(left[...], right, preferred_element_type=f32)
        if n * tile < half:
            first_ref[0:SUB, span] = product.astype(bf16)
        else:
            second_ref[:, n * tile - half : (n + 1) * tile - half] = product.astype(bf16)


def project_kernel(gain_ref, begun_ref, begun_squares, *refs):
    rows, weights = refs[:2], refs[2:-7]
    next_first, next_second, last_first, last_second, own_ref, own_squares, left = refs[-7:]
    half = next_first.shape[1]
    own, following, previous = slice(0, SUB), slice(SUB, 2 * SUB), slice(3 * SUB, 4 * SUB)
    left[...], squares = left_side(gain_ref, rows, (1, 3), (1, 3, 0))
    next_first[SUB:, :] = tail_rows(squares[:, 0:SUB] + begun_squares[0:1, following], half)
    last_first[SUB:, :] = tail_rows(squares[:, SUB : 2 * SUB] + begun_squares[0:1, previous], half)
    own_squares[...] = jnp.broadcast_to(squares[:, 2 * SUB :] + begun_squares[0:1, own], own_squares.shape)
    tile = 256
    for n in range(2 * half // tile):
        span = slice(n * tile, (n + 1) * tile)
        right = jnp.concatenate([w[:, span] for w in weights], axis=0)
        product = jnp.dot(left[...], right, preferred_element_type=f32)
        own_ref[:, span] = product[2 * SUB :] + begun_ref[own, span]
        next_rows = (product[0:SUB] + begun_ref[following, span]).astype(bf16)
        last_rows = (product[SUB : 2 * SUB] + begun_ref[previous, span]).astype(bf16)
        if n * tile < half:
            next_first[0:SUB, span] = next_rows
            last_first[0:SUB, span] = last_rows
        else:
            span = slice(n * tile - half, (n + 1) * tile - half)
            next_second[:, span] = next_rows
            last_second[:, span] = last_rows


def merge_kernel(next_first, last_second, got_first, got_second, next_ref, last_ref):
    next_ref[0:SUB, :] = (next_first[0:SUB, :].astype(f32) + got_first[0:SUB, :].astype(f32)).astype(bf16)
    squares = tail_squares(next_first) + tail_squares(got_first)
    next_ref[SUB:, :] = tail_rows(squares, next_ref.shape[1])
    last_ref[...] = (last_second[...].astype(f32) + got_second[...].astype(f32)).astype(bf16)


def finish_kernel(channels, own_ref, own_squares, next_first, next_second, last_first, last_second, out_ref):
    half = next_first.shape[1]
    squares = own_squares[0:1, :] + tail_squares(next_first) + tail_squares(last_first)
    scale = lax.rsqrt(squares / channels + epsilon)
    column = jnp.broadcast_to(scale, (SUB, SUB)).T[:, 0:1]
    first = own_ref[:, :half] + next_first[0:SUB, :].astype(f32) + last_first[0:SUB, :].astype(f32)
    second = own_ref[:, half:] + next_second[...].astype(f32) + last_second[...].astype(f32)
    out_ref[:, :half] = (first * column).astype(bf16)
    out_ref[:, half:] = (second * column).astype(bf16)


def ring_pairs(shift, gather):
    pairs = []
    for y in range(RING):
        for x in range(RING):
            for core in range(2):
                if (core == 0) == gather:
                    there = y * RING + (x + shift) % RING
                else:
                    there = ((y + shift) % RING) * RING + x
                pairs.append(((y * RING + x) * 2 + core, there * 2 + core))
    return pairs


def ring(value, shift, gather):
    return lax.ppermute(value, ("head", "batch"), ring_pairs(shift, gather))


def body(
    ssm_input, gate_input, b_proj, c_proj, step_size, log_decay, skip_gain, norm_gain, out_weight
):
    tokens, channels = ssm_input.shape
    heads = step_size.shape[0]
    width = out_weight.shape[1]
    blocks = tokens // BLOCK
    seq_count = lax.axis_size("seq")
    core, u, v = ring_place()
    following = RING - 1
    weight_before, weight_after = ring(out_weight, 1, True), ring(out_weight, following, True)

    params = pltpu.CompilerParams(vmem_limit_bytes=24 * 1024 * 1024)
    near = pl.BlockSpec(memory_space=pltpu.VMEM)

    def hold(*values):
        return [pltpu.with_memory_space_constraint(value, pltpu.VMEM) for value in values]

    def far(value):
        return pltpu.with_memory_space_constraint(value, pltpu.HBM)

    payload = channels + 3 * PAD
    ssm_columns, gate_columns = ssm_input.T, gate_input.T
    prefix, total, cum, factor, x_own, b_own, c_own, step_own = pl.pallas_call(
        state_kernel,
        in_specs=[pl.BlockSpec(memory_space=pltpu.HBM)] * 5,
        out_specs=[near] * 8,
        out_shape=[
            pltpu.VMEM((blocks, channels, STATE), bf16),
            pltpu.VMEM((payload, STATE), bf16),
            pltpu.VMEM((PAD, tokens), f32),
            pltpu.VMEM((PAD, tokens), f32),
            pltpu.VMEM((channels, tokens), bf16),
            pltpu.VMEM((tokens, STATE), bf16),
            pltpu.VMEM((tokens, STATE), bf16),
            pltpu.VMEM((heads, tokens), f32),
        ],
        scratch_shapes=[pltpu.VMEM((heads, tokens), f32), pltpu.SemaphoreType.DMA((PIECES + 4,))],
        compiler_params=params,
        name="state",
    )(*[far(value) for value in (ssm_columns, b_proj, c_proj, step_size, log_decay)])

    def along(value, shift):
        return lax.ppermute(value, "seq", [(k, k + shift) for k in range(seq_count - shift)])

    totals = []
    for shift in range(1, seq_count):
        totals.append(along(total, shift))
    local = pl.pallas_call(
        within_kernel,
        in_specs=[pl.BlockSpec(memory_space=pltpu.SMEM)] + [near] * 6,
        out_specs=near,
        out_shape=pltpu.VMEM((channels, tokens), f32),
        compiler_params=params,
        name="within",
    )(skip_gain, *hold(x_own, b_own, c_own, cum, step_own, prefix))
    local, weight_before, weight_after = lax.optimization_barrier((local, weight_before, weight_after))
    middle = channels // 2
    upper, lower = weight_before[:middle], weight_after[middle:]
    upper, lower = ring(upper, 1, True), ring(lower, following, True)

    quarter = tokens // RING
    gated = pl.pallas_call(
        gate_kernel,
        in_specs=[near] * (4 + len(totals)),
        out_specs=[near] * RING,
        out_shape=[pltpu.VMEM((channels, quarter), bf16)] * RING,
        compiler_params=params,
        name="gate",
    )(*hold(local, gate_columns, c_own, factor, *totals))

    rows_opposite = ring(gated[2], 2, True)
    rows_near = [ring(gated[s], s, True) for s in (1, following)]

    half = width // 2
    with_tail, without = pltpu.VMEM((SUB + EXTRA, half), bf16), pltpu.VMEM((SUB, half), bf16)
    gain_lines = norm_gain.reshape(-1, SUB)
    begun, begun_squares = pl.pallas_call(
        begin_kernel,
        in_specs=[near] * 6,
        out_specs=[near] * 2,
        scratch_shapes=[pltpu.VMEM((quarter, 2 * channels), bf16)],
        out_shape=[pltpu.VMEM((quarter, width), f32), pltpu.VMEM((PAD, quarter), f32)],
        compiler_params=params,
        name="begin",
    )(*hold(gain_lines, gated[0], rows_opposite, out_weight, upper, lower))
    operands = hold(gain_lines, begun, begun_squares, *rows_near, weight_before, weight_after)
    opposite_first, opposite_second = pl.pallas_call(
        opposite_kernel,
        in_specs=[near] * len(operands),
        out_specs=[near] * 2,
        scratch_shapes=[pltpu.VMEM((SUB, 2 * channels), bf16)],
        out_shape=[with_tail, without],
        compiler_params=params,
        name="opposite",
    )(*operands)
    got_first = ring(opposite_first, 1, False)
    got_second = ring(opposite_second, following, False)
    next_first, next_second, last_first, last_second, own, own_squares = pl.pallas_call(
        project_kernel,
        in_specs=[near] * len(operands),
        out_specs=[near] * 6,
        scratch_shapes=[pltpu.VMEM((3 * SUB, 2 * channels), bf16)],
        out_shape=[with_tail, without, with_tail, without, pltpu.VMEM((SUB, width), f32), pltpu.VMEM((PAD, SUB), f32)],
        compiler_params=params,
        name="project",
    )(*operands)
    sent_second = ring(next_second, 1, False)
    sent_first = ring(last_first, following, False)
    next_sum, last_sum = pl.pallas_call(
        merge_kernel,
        in_specs=[near] * 4,
        out_specs=[near] * 2,
        out_shape=[with_tail, without],
        compiler_params=params,
        name="merge",
    )(*hold(next_first, last_second, got_first, got_second))
    from_before = ring(next_sum, 1, False)
    from_after = ring(last_sum, following, False)

    return pl.pallas_call(
        lambda *refs: finish_kernel(HEAD_COUNT * HEAD_DIM, *refs),
        in_specs=[near] * 6,
        out_specs=pl.BlockSpec((SUB, width), lambda: (0, 0)),
        out_shape=jax.ShapeDtypeStruct((SUB, width), bf16),
        compiler_params=params,
        name="finish",
    )(*hold(own, own_squares, from_before, sent_second, sent_first, from_after))


def solution(mesh):
    in_specs = (
        P(("batch", "seq"), "head"),
        P(("batch", "seq"), "head"),
        P(("batch", "seq"), None),
        P(("batch", "seq"), None),
        P("head", ("batch", "seq")),
        P("head", ("batch", "seq")),
        P("head"),
        P(),
        P("head", None),
    )
    out_specs = P(("batch", "seq", "head"), None)

    return jax.shard_map(body, mesh=mesh, in_specs=in_specs, out_specs=out_specs, check_vma=False)
```

```python
import jax
import jax.numpy as jnp
from jax import lax
from jax.experimental import pallas as pl
from jax.experimental.pallas import tpu as pltpu
from jax.sharding import PartitionSpec as P


HEAD_COUNT = 80
HEAD_DIM = 64
STATE = 128
GROUPS = 8
BLOCK = 256
RING = 4
SUB = 128
EXTRA = 8
PAD = 8

epsilon = 1e-05
LOG2E = 1.4426950408889634


f32 = jnp.float32
bf16 = jnp.bfloat16
TT = (((1,), (1,)), ((), ()))


def triangle(size, dtype):
    rows = lax.broadcasted_iota(jnp.int32, (size, size), 0)
    columns = lax.broadcasted_iota(jnp.int32, (size, size), 1)
    return (rows <= columns).astype(dtype)


def split3(value):
    high = value.astype(bf16)
    rest = value - high.astype(f32)
    middle = rest.astype(bf16)
    return high, middle, (rest - middle.astype(f32)).astype(bf16)


def join3(stacked, rows):
    return stacked[0:rows].astype(f32) + stacked[rows : 2 * rows].astype(f32) + stacked[2 * rows : 3 * rows].astype(f32)


def per_head(column, heads, lanes):
    return jnp.concatenate(
        [jnp.broadcast_to(column[h : h + 1, 0:1], (HEAD_DIM, lanes)) for h in range(heads)], axis=0
    )


def state_kernel(
    x_hbm, b_hbm, c_hbm, step_hbm, decay_hbm, prefix_ref, total_ref, cum_ref, shift_ref, factor_ref, x_ref, b_ref, c_ref, step_ref, decay_ref, sems
):
    heads, tokens = step_ref.shape
    blocks = tokens // BLOCK
    group = lax.axis_index("head") * heads * GROUPS // HEAD_COUNT
    columns = pl.ds(pl.multiple_of(group * STATE, STATE), STATE)
    sources = (decay_hbm, step_hbm, x_hbm, b_hbm.at[:, columns], c_hbm.at[:, columns])
    targets = (decay_ref, step_ref, x_ref, b_ref, c_ref)
    fetches = [pltpu.make_async_copy(sources[k], targets[k], sems.at[k]) for k in range(5)]
    for fetch in fetches:
        fetch.start()
    fetches[0].wait()
    fill = jnp.zeros((PAD - heads, BLOCK), f32)
    decay = jnp.concatenate(
        [piece for c in range(blocks) for piece in (decay_ref[:, c * BLOCK : (c + 1) * BLOCK], fill)], axis=0
    )
    sums = jnp.dot(
        jnp.concatenate(split3(decay), axis=0), triangle(BLOCK, bf16), preferred_element_type=f32
    )
    sums = join3(sums, blocks * PAD)
    offset = jnp.zeros((PAD, 1), f32)
    for c in range(blocks):
        span = slice(c * BLOCK, (c + 1) * BLOCK)
        cumulative = sums[c * PAD : (c + 1) * PAD]
        cum_ref[:, span] = cumulative * LOG2E
        factor_ref[:, span] = jnp.exp(cumulative + offset)
        offset = offset + cumulative[:, BLOCK - 1 :]
    fetches[1].wait()
    shift_ref[...] = cum_ref[0:heads, :] - jnp.log2(step_ref[...])
    for fetch in fetches[2:4]:
        fetch.wait()
    state = jnp.zeros((heads * HEAD_DIM, STATE), f32)
    for c in range(blocks):
        span = slice(c * BLOCK, (c + 1) * BLOCK)
        cumulative = sums[c * PAD : (c + 1) * PAD]
        end = cumulative[:, BLOCK - 1 :]
        prefix_ref[c] = state.astype(bf16)
        to_end = jnp.exp(end - cumulative)[0:heads] * step_ref[:, span]
        scaled = jnp.concatenate(
            [
                (x_ref[h * HEAD_DIM : (h + 1) * HEAD_DIM, span].astype(f32) * to_end[h : h + 1]).astype(bf16)
                for h in range(heads)
            ],
            axis=0,
        )
        block_state = jnp.dot(scaled, b_ref[span, :], preferred_element_type=f32)
        state = per_head(jnp.exp(end), heads, STATE) * state + block_state
    total_ref[0 : heads * HEAD_DIM, :] = state.astype(bf16)
    parts = split3(jnp.broadcast_to(offset, (PAD, STATE)))
    total_ref[heads * HEAD_DIM :, :] = jnp.concatenate(parts, axis=0)
    fetches[4].wait()


def pair_kernel(total_ref, before_ref, pair_ref):
    channels = total_ref.shape[0] - 3 * PAD
    heads = channels // HEAD_DIM
    logs = join3(total_ref[channels:, :], PAD)
    decayed = per_head(jnp.exp(logs), heads, STATE) * before_ref[0:channels, :].astype(f32)
    pair_ref[0:channels, :] = (total_ref[0:channels, :].astype(f32) + decayed).astype(bf16)
    pair_ref[channels:, :] = jnp.concatenate(split3(logs + join3(before_ref[channels:, :], PAD)), axis=0)


def within_kernel(skip_ref, x_ref, b_ref, c_ref, cum_ref, shift_ref, prefix_ref, out_ref):
    heads = shift_ref.shape[0]
    half = BLOCK // 2
    causal = triangle(half, f32).T > 0
    blocks = shift_ref.shape[1] // BLOCK

    def shared(k):
        span = slice(k * BLOCK, (k + 1) * BLOCK)
        c_block, b_block = c_ref[span, :], b_ref[span, :]
        cumulative = cum_ref[:, span]
        return (
            lax.dot_general(c_block[:half], b_block[:half], TT, preferred_element_type=f32),
            lax.dot_general(c_block[half:], b_block, TT, preferred_element_type=f32),
            lax.dot_general(prefix_ref[k], c_block, TT, preferred_element_type=f32),
            jnp.exp2(cumulative),
            cumulative.T,
        )

    ahead = shared(0)
    for k in range(blocks):
        span = slice(k * BLOCK, (k + 1) * BLOCK)
        scores_first, scores_second, across, factor, columns = ahead
        if k + 1 < blocks:
            ahead = shared(k + 1)
        for h in range(heads):
            channels = slice(h * HEAD_DIM, (h + 1) * HEAD_DIM)
            x_head = x_ref[channels, span]
            row = shift_ref[h : h + 1, span]
            differ = columns[:half, h : h + 1] - row[:, :half]
            first = scores_first * jnp.exp2(jnp.where(causal, differ, -jnp.inf))
            column = columns[half:, h : h + 1]
            full = scores_second[:, :half] * jnp.exp2(column - row[:, :half])
            differ = column - row[:, half:]
            last = scores_second[:, half:] * jnp.exp2(jnp.where(causal, differ, -jnp.inf))
            second = jnp.concatenate([full, last], axis=1)
            within = jnp.concatenate(
                [
                    lax.dot_general(x_head[:, :half], first.astype(bf16), TT, preferred_element_type=f32),
                    lax.dot_general(x_head, second.astype(bf16), TT, preferred_element_type=f32),
                ],
                axis=1,
            )
            out_ref[channels, span] = (
                within + across[channels] * factor[h : h + 1] + skip_ref[h] * x_head.astype(f32)
            )


def ring_place():
    head_index = lax.axis_index("head")
    core = lax.axis_index("batch")
    y, x = head_index // RING, head_index % RING
    return core, jnp.where(core == 0, x, y), jnp.where(core == 0, y, x)


def head_at(core, u, v):
    return jnp.where(core == 0, v * RING + u, u * RING + v)


def gate_kernel(out_ref, gate_ref, c_ref, factor_ref, *refs):
    totals, results = refs[:-RING], refs[-RING:]
    channels = gate_ref.shape[0]
    heads = channels // HEAD_DIM
    incoming = jnp.zeros((channels, STATE), f32)
    log_sum = jnp.zeros((PAD, STATE), f32)
    for total in totals:
        incoming = incoming + per_head(jnp.exp(log_sum), heads, STATE) * total[0:channels, :].astype(f32)
        log_sum = log_sum + join3(total[channels:, :], PAD)
    incoming = incoming.astype(bf16)
    core, u, v = ring_place()
    for su in range(RING):
        for sv in range(RING):
            place = head_at(core, (u + su) % RING, (v + sv) % RING)
            span = pl.ds(pl.multiple_of(place * SUB, SUB), SUB)
            across = lax.dot_general(incoming, c_ref[span, :], TT, preferred_element_type=f32)
            factor = factor_ref[:, span]
            for h in range(heads):
                rows = slice(h * HEAD_DIM, (h + 1) * HEAD_DIM)
                gate = gate_ref[rows, span].astype(f32)
                output = out_ref[rows, span] + across[rows] * factor[h : h + 1]
                gated = output * (gate / (1.0 + jnp.exp(-gate)))
                results[su][rows, sv * SUB : (sv + 1) * SUB] = gated.astype(bf16)


def gain_row(gain_ref, head, channels):
    first = head * channels
    lines = gain_ref[pl.ds(first // SUB, 3), :]
    line = jnp.concatenate([lines[i : i + 1] for i in range(3)], axis=1)
    shifted = jnp.concatenate([line[:, SUB // 2 :], line[:, : SUB // 2]], axis=1)
    return jnp.where(first % SUB == 0, line, shifted)[:, :channels]


def left_side(gain_ref, rows, sources, blocks):
    core, u, v = ring_place()
    channels = rows[0].shape[0]
    pick = [slice(k * SUB, (k + 1) * SUB) for k in blocks]
    values = jnp.concatenate([jnp.concatenate([r[:, span] for span in pick], axis=1) for r in rows], axis=0)
    wide = values.astype(f32)
    squares = jnp.sum(wide * wide, axis=0, keepdims=True)
    gains = jnp.concatenate(
        [gain_row(gain_ref, head_at(core, (u - s + RING) % RING, v), channels) for s in sources], axis=1
    )
    return (values.T.astype(f32) * gains).astype(bf16), squares


def tail_rows(squares, width):
    parts = [part.astype(f32) for part in split3(squares)]
    tail = jnp.concatenate(parts + [jnp.zeros((EXTRA - 3, SUB), f32)], axis=0)
    return jnp.concatenate([tail] * (width // SUB), axis=1).astype(bf16)


def tail_squares(part):
    return jnp.sum(part[SUB:, 0:SUB].astype(f32), axis=0, keepdims=True)


def begin_kernel(gain_ref, *refs):
    rows, weights = refs[:2], refs[2:-3]
    product_ref, squares_ref, left = refs[-3:]
    left[...], squares = left_side(gain_ref, rows, (0, 2), range(RING))
    squares_ref[...] = jnp.broadcast_to(squares, squares_ref.shape)
    tile = 256
    for n in range(product_ref.shape[1] // tile):
        span = slice(n * tile, (n + 1) * tile)
        right = jnp.concatenate([w[:, span] for w in weights], axis=0)
        product_ref[:, span] = jnp.dot(left[...], right, preferred_element_type=f32)


def opposite_kernel(gain_ref, begun_ref, begun_squares, *refs):
    rows, weights = refs[:2], refs[2:-3]
    first_ref, second_ref, left = refs[-3:]
    half = first_ref.shape[1]
    block = slice(2 * SUB, 3 * SUB)
    left[...], squares = left_side(gain_ref, rows, (1, 3), (2,))
    first_ref[SUB:, :] = tail_rows(squares + begun_squares[0:1, block], half)
    tile = 256
    for n in range(2 * half // tile):
        span = slice(n * tile, (n + 1) * tile)
        right = jnp.concatenate([w[:, span] for w in weights], axis=0)
        product = begun_ref[block, span] + jnp.dot(left[...], right, preferred_element_type=f32)
        if n * tile < half:
            first_ref[0:SUB, span] = product.astype(bf16)
        else:
            second_ref[:, n * tile - half : (n + 1) * tile - half] = product.astype(bf16)


def project_kernel(gain_ref, begun_ref, begun_squares, *refs):
    rows, weights = refs[:2], refs[2:-7]
    next_first, next_second, last_first, last_second, own_ref, own_squares, left = refs[-7:]
    half = next_first.shape[1]
    own, following, previous = slice(0, SUB), slice(SUB, 2 * SUB), slice(3 * SUB, 4 * SUB)
    left[...], squares = left_side(gain_ref, rows, (1, 3), (1, 3, 0))
    next_first[SUB:, :] = tail_rows(squares[:, 0:SUB] + begun_squares[0:1, following], half)
    last_first[SUB:, :] = tail_rows(squares[:, SUB : 2 * SUB] + begun_squares[0:1, previous], half)
    own_squares[...] = jnp.broadcast_to(squares[:, 2 * SUB :] + begun_squares[0:1, own], own_squares.shape)
    tile = 256
    for n in range(2 * half // tile):
        span = slice(n * tile, (n + 1) * tile)
        right = jnp.concatenate([w[:, span] for w in weights], axis=0)
        product = jnp.dot(left[...], right, preferred_element_type=f32)
        own_ref[:, span] = product[2 * SUB :] + begun_ref[own, span]
        next_rows = (product[0:SUB] + begun_ref[following, span]).astype(bf16)
        last_rows = (product[SUB : 2 * SUB] + begun_ref[previous, span]).astype(bf16)
        if n * tile < half:
            next_first[0:SUB, span] = next_rows
            last_first[0:SUB, span] = last_rows
        else:
            span = slice(n * tile - half, (n + 1) * tile - half)
            next_second[:, span] = next_rows
            last_second[:, span] = last_rows


def merge_kernel(next_first, last_second, got_first, got_second, next_ref, last_ref):
    next_ref[0:SUB, :] = (next_first[0:SUB, :].astype(f32) + got_first[0:SUB, :].astype(f32)).astype(bf16)
    squares = tail_squares(next_first) + tail_squares(got_first)
    next_ref[SUB:, :] = tail_rows(squares, next_ref.shape[1])
    last_ref[...] = (last_second[...].astype(f32) + got_second[...].astype(f32)).astype(bf16)


def finish_kernel(channels, own_ref, own_squares, next_first, next_second, last_first, last_second, out_ref):
    half = next_first.shape[1]
    squares = own_squares[0:1, :] + tail_squares(next_first) + tail_squares(last_first)
    scale = lax.rsqrt(squares / channels + epsilon)
    column = jnp.broadcast_to(scale, (SUB, SUB)).T[:, 0:1]
    first = own_ref[:, :half] + next_first[0:SUB, :].astype(f32) + last_first[0:SUB, :].astype(f32)
    second = own_ref[:, half:] + next_second[...].astype(f32) + last_second[...].astype(f32)
    out_ref[:, :half] = (first * column).astype(bf16)
    out_ref[:, half:] = (second * column).astype(bf16)


def ring_pairs(shift, gather):
    pairs = []
    for y in range(RING):
        for x in range(RING):
            for core in range(2):
                if (core == 0) == gather:
                    there = y * RING + (x + shift) % RING
                else:
                    there = ((y + shift) % RING) * RING + x
                pairs.append(((y * RING + x) * 2 + core, there * 2 + core))
    return pairs


def ring(value, shift, gather):
    return lax.ppermute(value, ("head", "batch"), ring_pairs(shift, gather))


def body(
    ssm_input, gate_input, b_proj, c_proj, step_size, log_decay, skip_gain, norm_gain, out_weight
):
    tokens, channels = ssm_input.shape
    heads = step_size.shape[0]
    width = out_weight.shape[1]
    blocks = tokens // BLOCK
    seq_count = lax.axis_size("seq")
    core, u, v = ring_place()
    following = RING - 1
    weight_before, weight_after = ring(out_weight, 1, True), ring(out_weight, following, True)

    params = pltpu.CompilerParams(vmem_limit_bytes=24 * 1024 * 1024)
    near = pl.BlockSpec(memory_space=pltpu.VMEM)

    def hold(*values):
        return [pltpu.with_memory_space_constraint(value, pltpu.VMEM) for value in values]

    def far(value):
        return pltpu.with_memory_space_constraint(value, pltpu.HBM)

    payload = channels + 3 * PAD
    ssm_columns, gate_columns = ssm_input.T, gate_input.T
    prefix, total, cum, shift, factor, x_own, b_own, c_own = pl.pallas_call(
        state_kernel,
        in_specs=[pl.BlockSpec(memory_space=pltpu.HBM)] * 5,
        out_specs=[near] * 8,
        out_shape=[
            pltpu.VMEM((blocks, channels, STATE), bf16),
            pltpu.VMEM((payload, STATE), bf16),
            pltpu.VMEM((PAD, tokens), f32),
            pltpu.VMEM((heads, tokens), f32),
            pltpu.VMEM((PAD, tokens), f32),
            pltpu.VMEM((channels, tokens), bf16),
            pltpu.VMEM((tokens, STATE), bf16),
            pltpu.VMEM((tokens, STATE), bf16),
        ],
        scratch_shapes=[pltpu.VMEM((heads, tokens), f32)] * 2 + [pltpu.SemaphoreType.DMA((5,))],
        compiler_params=params,
        name="state",
    )(*[far(value) for value in (ssm_columns, b_proj, c_proj, step_size, log_decay)])

    def along(value, shift):
        return lax.ppermute(value, "seq", [(k, k + shift) for k in range(seq_count - shift)])

    before = along(total, 1)
    local = pl.pallas_call(
        within_kernel,
        in_specs=[pl.BlockSpec(memory_space=pltpu.SMEM)] + [near] * 6,
        out_specs=near,
        out_shape=pltpu.VMEM((channels, tokens), f32),
        compiler_params=params,
        name="within",
    )(skip_gain, *hold(x_own, b_own, c_own, cum, shift, prefix))
    before, local = lax.optimization_barrier((before, local))
    pair = pl.pallas_call(
        pair_kernel,
        in_specs=[near] * 2,
        out_specs=near,
        out_shape=pltpu.VMEM((payload, STATE), bf16),
        compiler_params=params,
        name="pair",
    )(*hold(total, before))
    totals = []
    for shift in range(1, seq_count, 2):
        totals.append(along(pair, shift))

    weight_before, weight_after, pair = lax.optimization_barrier((weight_before, weight_after, pair))
    middle = channels // 2
    upper, lower = weight_before[:middle], weight_after[middle:]
    upper, lower = ring(upper, 1, True), ring(lower, following, True)

    quarter = tokens // RING
    gated = pl.pallas_call(
        gate_kernel,
        in_specs=[near] * (4 + len(totals)),
        out_specs=[near] * RING,
        out_shape=[pltpu.VMEM((channels, quarter), bf16)] * RING,
        compiler_params=params,
        name="gate",
    )(*hold(local, gate_columns, c_own, factor, *totals))

    rows_opposite = ring(gated[2], 2, True)
    rows_near = [ring(gated[s], s, True) for s in (1, following)]

    half = width // 2
    with_tail, without = pltpu.VMEM((SUB + EXTRA, half), bf16), pltpu.VMEM((SUB, half), bf16)
    gain_lines = norm_gain.reshape(-1, SUB)
    begun, begun_squares = pl.pallas_call(
        begin_kernel,
        in_specs=[near] * 6,
        out_specs=[near] * 2,
        scratch_shapes=[pltpu.VMEM((quarter, 2 * channels), bf16)],
        out_shape=[pltpu.VMEM((quarter, width), f32), pltpu.VMEM((PAD, quarter), f32)],
        compiler_params=params,
        name="begin",
    )(*hold(gain_lines, gated[0], rows_opposite, out_weight, upper, lower))
    operands = hold(gain_lines, begun, begun_squares, *rows_near, weight_before, weight_after)
    opposite_first, opposite_second = pl.pallas_call(
        opposite_kernel,
        in_specs=[near] * len(operands),
        out_specs=[near] * 2,
        scratch_shapes=[pltpu.VMEM((SUB, 2 * channels), bf16)],
        out_shape=[with_tail, without],
        compiler_params=params,
        name="opposite",
    )(*operands)
    got_first = ring(opposite_first, 1, False)
    got_second = ring(opposite_second, following, False)
    next_first, next_second, last_first, last_second, own, own_squares = pl.pallas_call(
        project_kernel,
        in_specs=[near] * len(operands),
        out_specs=[near] * 6,
        scratch_shapes=[pltpu.VMEM((3 * SUB, 2 * channels), bf16)],
        out_shape=[with_tail, without, with_tail, without, pltpu.VMEM((SUB, width), f32), pltpu.VMEM((PAD, SUB), f32)],
        compiler_params=params,
        name="project",
    )(*operands)
    sent_second = ring(next_second, 1, False)
    sent_first = ring(last_first, following, False)
    next_sum, last_sum = pl.pallas_call(
        merge_kernel,
        in_specs=[near] * 4,
        out_specs=[near] * 2,
        out_shape=[with_tail, without],
        compiler_params=params,
        name="merge",
    )(*hold(next_first, last_second, got_first, got_second))
    from_before = ring(next_sum, 1, False)
    from_after = ring(last_sum, following, False)

    return pl.pallas_call(
        lambda *refs: finish_kernel(HEAD_COUNT * HEAD_DIM, *refs),
        in_specs=[near] * 6,
        out_specs=pl.BlockSpec((SUB, width), lambda: (0, 0)),
        out_shape=jax.ShapeDtypeStruct((SUB, width), bf16),
        compiler_params=params,
        name="finish",
    )(*hold(own, own_squares, from_before, sent_second, sent_first, from_after))


def solution(mesh):
    in_specs = (
        P(("batch", "seq"), "head"),
        P(("batch", "seq"), "head"),
        P(("batch", "seq"), None),
        P(("batch", "seq"), None),
        P("head", ("batch", "seq")),
        P("head", ("batch", "seq")),
        P("head"),
        P(),
        P("head", None),
    )
    out_specs = P(("batch", "seq", "head"), None)

    return jax.shard_map(body, mesh=mesh, in_specs=in_specs, out_specs=out_specs, check_vma=False)
```
